256 devices in a mesh: lon: 64 (over x, z, core), lat: 4 (over y).
Axes of the slice: x: 4, y: 4, z: 8, core: 2. Of those that a mesh axis runs over, the one named last changes fastest.
Arguments:
- state: float32 [2048, 64, 1024], P('lon', None, 'lat'), may hold values from -6 to 6
Outputs:
- spectrum: float32 [2, 1024, 64, 1024], P(None, 'lon', None, 'lat')
The draws below stay inside these ranges and needn't reach their ends.
All inputs are finite; a program needn't handle non-finite values.
Results may differ from the reference program's by a relative error of at most 0.00011.
Values sent between devices are 32-bit elements; how exact they have to be, the bound alone decides.
No kernel may reach another device: no remote copies, remote signals or barrier semaphores. Data moves between devices by JAX's collectives and lax.ppermute only.
A program may use at most 64 MiB of HBM per device.

```python
import math
import jax
import jax.numpy as jnp

NLON = 2048
FIELDS = 64
NLAT = 1024
MODES = 1024


def steps_of(rng, shape, pieces, least, top_value):
    loudness = 1.0
    for dim, blocks in pieces:
        draws = jax.random.uniform(jax.random.fold_in(jax.random.fold_in(rng, 6), dim), (blocks,), jnp.float32, least / len(pieces), top_value / len(pieces))
        loudness = loudness * jnp.repeat(jnp.exp(draws), shape[dim] // blocks).reshape((-1,) + (1,) * (len(shape) - 1 - dim))
    return loudness


def noise(rng, dims, deviation, limit, shards=(), kind=jnp.bfloat16):
    array = jax.random.normal(rng, dims, jnp.float32) * deviation
    if len(shards) > 0:
        array = steps_of(rng, dims, shards, -0.22, 0.18) * array
    return jnp.clip(array, min=-limit, max=limit).astype(kind)


def setup_inputs(seed: int = 0) -> dict:
    arg_keys = jax.random.split(jax.random.key(seed), 2)
    return {
        "state": noise(arg_keys[0], (NLON, FIELDS, NLAT), 1.0, 6.0, ((0, 64), (2, 4)), jnp.float32),
    }


def reference(state):
    spectrum = jnp.fft.rfft(state, axis=0)[:MODES] * (1.0 / math.sqrt(NLON))
    return jnp.stack([jnp.real(spectrum), jnp.imag(spectrum)]).astype(jnp.float32)
```

```python
import math

import jax
import jax.numpy as jnp
from jax import lax
from jax.experimental import pallas as pl
from jax.experimental.pallas import tpu as pltpu
from jax.sharding import PartitionSpec as P

NLON = 2048
RADIX = 16
INNER = NLON // RADIX
PEERS = 64
HALF = RADIX // 2


def split_bf16(v):
    high = v.astype(jnp.bfloat16)
    low = (v - high.astype(jnp.float32)).astype(jnp.bfloat16)
    return high, low


def phase(rows, cols):
    turn = (rows * cols) % NLON
    turn = jnp.where(turn >= NLON // 2, turn - NLON, turn)
    return turn.astype(jnp.float32) * (2.0 * math.pi / NLON)


def twiddle_matrices(scale):
    shape = (HALF, 2, PEERS, INNER)
    pair = lax.broadcasted_iota(jnp.int32, shape, 0)
    mirror = lax.broadcasted_iota(jnp.int32, shape, 1)
    outer = lax.broadcasted_iota(jnp.int32, shape, 2)
    inner = lax.broadcasted_iota(jnp.int32, shape, 3)
    first = jnp.where(mirror == 0, pair, jnp.where(pair == 0, HALF, RADIX - pair))
    angle = phase(inner, first + RADIX * outer)
    c = jnp.cos(angle) * scale
    s = jnp.sin(angle) * scale
    real_only = pair == 0
    zero = jnp.zeros_like(c)
    plain = mirror == 0
    re_a = jnp.where(real_only, jnp.where(plain, c, zero), c)
    im_a = jnp.where(real_only, jnp.where(plain, -s, zero), -s)
    re_b = jnp.where(real_only, jnp.where(plain, zero, c), jnp.where(plain, s, -s))
    im_b = jnp.where(real_only, jnp.where(plain, zero, -s), jnp.where(plain, c, -c))
    re = jnp.concatenate([re_a, re_b], axis=-1)
    im = jnp.concatenate([im_a, im_b], axis=-1)
    full = jnp.stack([re, im], axis=2)
    full = full.reshape(HALF, 4 * PEERS, 2 * INNER)
    high = lax.reduce_precision(full, 8, 7)
    return high.astype(jnp.bfloat16), (full - high).astype(jnp.bfloat16)


def fft_real16(x):
    def fft_complex8(z):
        def fft4(a):
            (ar, ai), (br, bi), (cr, ci), (dr, di) = a
            sr, si = ar + cr, ai + ci
            tr, ti = ar - cr, ai - ci
            ur, ui = br + dr, bi + di
            vr, vi = br - dr, bi - di
            return [(sr + ur, si + ui), (tr + vi, ti - vr), (sr - ur, si - ui), (tr - vi, ti + vr)]

        even = fft4(z[0::2])
        odd = fft4(z[1::2])
        h = math.sqrt(0.5)
        out = [None] * 8
        for k in range(4):
            er, ei = even[k]
            pr, pi = odd[k]
            if k == 1:
                pr, pi = (pr + pi) * h, (pi - pr) * h
            elif k == 2:
                pr, pi = pi, -pr
            elif k == 3:
                pr, pi = (pi - pr) * h, -(pr + pi) * h
            out[k] = (er + pr, ei + pi)
            out[k + 4] = (er - pr, ei - pi)
        return out

    z = fft_complex8([(x[2 * i], x[2 * i + 1]) for i in range(8)])
    out = [(z[0][0] + z[0][1], None)]
    for k in range(1, 8):
        zr, zi = z[k]
        wr, wi = z[8 - k]
        er, ei = (zr + wr) * 0.5, (zi - wi) * 0.5
        pr, pi = (zi + wi) * 0.5, (wr - zr) * 0.5
        c, s = math.cos(2 * math.pi * k / 16), math.sin(2 * math.pi * k / 16)
        out.append((er + c * pr + s * pi, ei + c * pi - s * pr))
    out.append((z[0][0] - z[0][1], None))
    return out


def relayout_in_kernel(x_ref, o_ref):
    o_ref[...] = jnp.swapaxes(x_ref[...], 0, 1)


def relayout_in(state):
    lon_dev, fields, lat_dev = state.shape
    return pl.pallas_call(
        relayout_in_kernel,
        grid=(fields // 8,),
        in_specs=[pl.BlockSpec((lon_dev, 8, lat_dev), lambda i: (0, i, 0))],
        out_specs=pl.BlockSpec((8, lon_dev, lat_dev), lambda i: (i, 0, 0)),
        out_shape=jax.ShapeDtypeStruct((fields, lon_dev, lat_dev), jnp.float32),
        name="relayout_in",
    )(state)


def fft_kernel(x_ref, wh_ref, wl_ref, o_ref, yh_ref, yl_ref, r_ref):
    width = x_ref.shape[1]

    def butterfly(i, carry):
        rows = 16 if width == 128 else 8
        base = i * rows
        x = [x_ref[pl.ds(n2 * INNER + base, rows), :] for n2 in range(RADIX)]
        y = fft_real16(x)
        for k in range(HALF):
            parts = (y[0][0], y[HALF][0]) if k == 0 else y[k]
            for j, part in enumerate(parts):
                yh_ref[k, pl.ds(j * INNER + base, rows), :] = part
        return carry

    lax.fori_loop(0, INNER // (16 if width == 128 else 8), butterfly, 0)
    for k in range(HALF):
        yh, yl = split_bf16(yh_ref[k])
        wh = wh_ref[k]
        r = jnp.dot(wh, yh, preferred_element_type=jnp.float32)
        r = r + jnp.dot(wh, yl, preferred_element_type=jnp.float32)
        r = r + jnp.dot(wl_ref[k], yh, preferred_element_type=jnp.float32)
        r_ref[0, k] = r[:PEERS]
        r_ref[1, k] = r[PEERS : 2 * PEERS]
        mirror = HALF if k == 0 else RADIX - k
        r_ref[0, mirror] = r[2 * PEERS : 3 * PEERS]
        r_ref[1, mirror] = r[3 * PEERS :]
    for part in range(2):
        for block in range(2):
            o_ref[:, part * RADIX + block * 8 : part * RADIX + block * 8 + 8, :] = jnp.swapaxes(
                r_ref[part, block * 8 : block * 8 + 8], 0, 1
            )


def fft_call(gathered, wh, wl):
    width = gathered.shape[1]
    vmem = pl.BlockSpec(memory_space=pltpu.VMEM)
    return pl.pallas_call(
        fft_kernel,
        in_specs=[vmem, vmem, vmem],
        out_specs=vmem,
        out_shape=jax.ShapeDtypeStruct((PEERS, 2 * RADIX, width), jnp.float32),
        scratch_shapes=[
            pltpu.VMEM((HALF, 2 * INNER, width), jnp.float32),
            pltpu.VMEM((8, 128), jnp.float32),
            pltpu.VMEM((2, RADIX, PEERS, width), jnp.float32),
        ],
        name="fft",
    )(gathered, wh, wl)


def relayout_out_kernel(x_ref, o_ref):
    lat = x_ref.shape[2]
    o_ref[...] = jnp.swapaxes(x_ref[...], 0, 1).reshape(2, RADIX, 8, lat)


def relayout_out(x):
    fields, rows, lat_dev = x.shape
    return pl.pallas_call(
        relayout_out_kernel,
        grid=(fields // 8,),
        in_specs=[pl.BlockSpec((8, rows, lat_dev), lambda i: (i, 0, 0))],
        out_specs=pl.BlockSpec((2, RADIX, 8, lat_dev), lambda i: (0, 0, i, 0)),
        out_shape=jax.ShapeDtypeStruct((2, RADIX, fields, lat_dev), jnp.float32),
        name="relayout_out",
    )(x)


def local(state):
    lon_dev, fields, lat_dev = state.shape
    wh, wl = twiddle_matrices(1.0 / math.sqrt(NLON))
    sent = relayout_in(state)
    gathered = lax.all_to_all(sent, "lon", split_axis=0, concat_axis=0, tiled=True)
    spectrum = fft_call(gathered.reshape(NLON, lat_dev), wh, wl)
    shares = lax.all_to_all(spectrum, "lon", split_axis=0, concat_axis=0, tiled=True)
    return relayout_out(shares)


def solution(mesh):
    return jax.shard_map(
        local,
        mesh=mesh,
        in_specs=(P("lon", None, "lat"),),
        out_specs=P(None, "lon", None, "lat"),
        check_vma=False,
    )
```

```python
import math

import jax
import jax.numpy as jnp
from jax import lax
from jax.experimental import pallas as pl
from jax.experimental.pallas import tpu as pltpu
from jax.sharding import PartitionSpec as P


NLON = 2048
RADIX = 16
INNER = NLON // RADIX
PEERS = 64
HALF = RADIX // 2
NX, NZ, NC = 4, 8, 2
LON = 32
KEPT = 2 * RADIX
FIELDS = 64
LANES = 128
VMEM = pl.BlockSpec(memory_space=pltpu.VMEM)
HBM = pl.BlockSpec(memory_space=pltpu.HBM)
SMEM = pl.BlockSpec(memory_space=pltpu.SMEM)
PARAMS = pltpu.CompilerParams(vmem_limit_bytes=16 * 1024 * 1024)


def f32(*shape):
    return jax.ShapeDtypeStruct(shape, jnp.float32)


def split_bf16(v):
    high = v.astype(jnp.bfloat16)
    low = (v - high.astype(jnp.float32)).astype(jnp.bfloat16)
    return high, low


def phase(rows, cols):
    turn = (rows * cols) % NLON
    turn = jnp.where(turn >= NLON // 2, turn - NLON, turn)
    return turn.astype(jnp.float32) * (2.0 * math.pi / NLON)


def twiddle_matrices(scale):
    shape = (HALF, 2, PEERS, INNER)
    pair = lax.broadcasted_iota(jnp.int32, shape, 0)
    mirror = lax.broadcasted_iota(jnp.int32, shape, 1)
    outer = lax.broadcasted_iota(jnp.int32, shape, 2)
    inner = lax.broadcasted_iota(jnp.int32, shape, 3)
    first = jnp.where(mirror == 0, pair, jnp.where(pair == 0, HALF, RADIX - pair))
    angle = phase(inner, first + RADIX * outer)
    c = jnp.cos(angle) * scale
    s = jnp.sin(angle) * scale
    real_only = pair == 0
    zero = jnp.zeros_like(c)
    plain = mirror == 0
    re_a = jnp.where(real_only, jnp.where(plain, c, zero), c)
    im_a = jnp.where(real_only, jnp.where(plain, -s, zero), -s)
    re_b = jnp.where(real_only, jnp.where(plain, zero, c), jnp.where(plain, s, -s))
    im_b = jnp.where(real_only, jnp.where(plain, zero, -s), jnp.where(plain, c, -c))
    re = jnp.concatenate([re_a, re_b], axis=-1)
    im = jnp.concatenate([im_a, im_b], axis=-1)
    full = jnp.stack([re, im], axis=2)
    full = full.reshape(HALF, 4 * PEERS, 2 * INNER)
    high = lax.reduce_precision(full, 8, 7)
    return high.astype(jnp.bfloat16), (full - high).astype(jnp.bfloat16)


def fft_real16(x):
    def fft_complex8(z):
        def fft4(a):
            (ar, ai), (br, bi), (cr, ci), (dr, di) = a
            sr, si = ar + cr, ai + ci
            tr, ti = ar - cr, ai - ci
            ur, ui = br + dr, bi + di
            vr, vi = br - dr, bi - di
            return [(sr + ur, si + ui), (tr + vi, ti - vr), (sr - ur, si - ui), (tr - vi, ti + vr)]

        even = fft4(z[0::2])
        odd = fft4(z[1::2])
        h = math.sqrt(0.5)
        out = [None] * 8
        for k in range(4):
            er, ei = even[k]
            pr, pi = odd[k]
            if k == 1:
                pr, pi = (pr + pi) * h, (pi - pr) * h
            elif k == 2:
                pr, pi = pi, -pr
            elif k == 3:
                pr, pi = (pi - pr) * h, -(pr + pi) * h
            out[k] = (er + pr, ei + pi)
            out[k + 4] = (er - pr, ei - pi)
        return out

    z = fft_complex8([(x[2 * i], x[2 * i + 1]) for i in range(8)])
    out = [(z[0][0] + z[0][1], None)]
    for k in range(1, 8):
        zr, zi = z[k]
        wr, wi = z[8 - k]
        er, ei = (zr + wr) * 0.5, (zi - wi) * 0.5
        pr, pi = (zi + wi) * 0.5, (wr - zr) * 0.5
        c, s = math.cos(2 * math.pi * k / 16), math.sin(2 * math.pi * k / 16)
        out.append((er + c * pr + s * pi, ei + c * pi - s * pr))
    out.append((z[0][0] - z[0][1], None))
    return out


PAD_R = PEERS + 8


def fft_core(x_ref, wh_ref, wl_ref, y_ref, r_ref):
    def butterfly(i, carry):
        base = pl.multiple_of(i * 8, 8)
        x = [x_ref[pl.ds(n2 * INNER + base, 8), :] for n2 in range(RADIX)]
        y = fft_real16(x)
        for k in range(HALF):
            parts = (y[0][0], y[HALF][0]) if k == 0 else y[k]
            for j, part in enumerate(parts):
                y_ref[k, pl.ds(j * INNER + base, 8), :] = part
        return carry

    lax.fori_loop(0, INNER // 8, butterfly, 0)
    for k in range(HALF):
        yh, yl = split_bf16(y_ref[k])
        wh = wh_ref[k]
        r = jnp.dot(wh, yh, preferred_element_type=jnp.float32)
        r = r + jnp.dot(wh, yl, preferred_element_type=jnp.float32)
        r = r + jnp.dot(wl_ref[k], yh, preferred_element_type=jnp.float32)
        mirror = HALF if k == 0 else RADIX - k
        for q, row in enumerate((k, RADIX + k, mirror, RADIX + mirror)):
            r_ref[pl.ds(row * PAD_R, PEERS), :] = r[q * PEERS : (q + 1) * PEERS]


PIECES = 4


def send_pieces(body, count, buf_ref, o_ref, sem):
    step = count // PIECES
    copies = []
    for piece in range(PIECES):
        lax.fori_loop(piece * step, (piece + 1) * step, body, 0, unroll=4)
        rows = pl.ds(piece * step, step)
        copy = pltpu.make_async_copy(buf_ref.at[rows], o_ref.at[rows], sem.at[piece])
        copy.start()
        copies.append(copy)
    for copy in copies:
        copy.wait()


FFT_SCRATCH = [
    pltpu.VMEM((HALF, 2 * INNER, LANES), jnp.float32),
    pltpu.VMEM((KEPT * PAD_R, LANES), jnp.float32),
]


def mode_rows(r_ref, k1, eight):
    return r_ref[pl.ds(eight * 8 * PAD_R + k1, 8, stride=PAD_R), :]


def fft_a_kernel(x_ref, wh_ref, wl_ref, o_ref, y_ref, r_ref, buf_ref, sem):
    fft_core(x_ref, wh_ref, wl_ref, y_ref, r_ref)

    def peer(k1, carry):
        for eight in range(KEPT // 8):
            buf_ref[k1, eight * 8 : eight * 8 + 8, :] = mode_rows(r_ref, k1, eight)
        return carry

    send_pieces(peer, PEERS, buf_ref, o_ref, sem)


def fft_a(gathered, wh, wl):
    return pl.pallas_call(
        fft_a_kernel,
        in_specs=[VMEM] * 3,
        out_specs=HBM,
        out_shape=f32(PEERS, KEPT, LANES),
        scratch_shapes=FFT_SCRATCH
        + [pltpu.VMEM((PEERS, KEPT, LANES), jnp.float32), pltpu.SemaphoreType.DMA((PIECES,))],
        compiler_params=PARAMS,
        name="fft_a",
    )(gathered, wh, wl)


def fft_p_kernel(pos_ref, *refs):
    g_refs, (wh_ref, wl_ref), o_refs = refs[:8], refs[8:10], refs[10:18]
    x_ref, y_ref, r_ref = refs[18:]
    x, z, c = pos_ref[0], pos_ref[1], pos_ref[2]
    for dx in range(NX):
        for dc in range(NC):
            start = ((x + NX - dx) % NX) * (NLON // NX) + ((c + dc) % NC) * LON
            for zz in range(NZ):
                row = pl.multiple_of(start + zz * NC * LON, LON)
                x_ref[pl.ds(row, LON), :] = g_refs[dx * NC + dc][zz * LON : (zz + 1) * LON, :]
    fft_core(x_ref, wh_ref, wl_ref, y_ref, r_ref)
    for dz in range(NZ):
        target = (z + dz) % NZ
        for xx in range(NX):
            for cc in range(NC):
                k1 = xx * NZ * NC + target * NC + cc
                for eight in range(KEPT // 8):
                    row = (xx * NC + cc) * KEPT + eight * 8
                    o_refs[dz][row : row + 8, :] = mode_rows(r_ref, k1, eight)


def fft_p(pos, blocks, wh, wl):
    return pl.pallas_call(
        fft_p_kernel,
        in_specs=[SMEM] + [VMEM] * 10,
        out_specs=[VMEM] * NZ,
        out_shape=[f32(NX * NC * KEPT, LANES)] * NZ,
        scratch_shapes=[pltpu.VMEM((NLON, LANES), jnp.float32)] + FFT_SCRATCH,
        compiler_params=PARAMS,
        name="fft_p",
    )(pos, *blocks, wh, wl)


def split_z_kernel(pos_ref, s_ref, *refs):
    o_refs, sem = refs[:NZ], refs[NZ]
    z = pos_ref[1]
    copies = []
    for dz in range(NZ):
        field = pl.multiple_of(((z + dz) % NZ) * 8, 8)
        copies.append(
            pltpu.make_async_copy(s_ref.at[:, pl.ds(field, 8), pl.ds(0, LANES)], o_refs[dz], sem.at[dz])
        )
    for copy in copies:
        copy.start()
    for copy in copies:
        copy.wait()


def split_z(pos, state):
    return pl.pallas_call(
        split_z_kernel,
        in_specs=[SMEM, HBM],
        out_specs=[VMEM] * NZ,
        out_shape=[f32(LON, 8, LANES)] * NZ,
        scratch_shapes=[pltpu.SemaphoreType.DMA((NZ,))],
        compiler_params=PARAMS,
        name="split_z",
    )(pos, state)


def spread_x_kernel(pos_ref, *refs):
    b_refs, o_refs = refs[:NZ], refs[NZ:]
    x, z, c = pos_ref[0], pos_ref[1], pos_ref[2]
    for dx in range(NX):
        for dc in range(NC):
            field = ((x + dx) % NX) * NC + (c + dc) % NC
            for dz in range(NZ):
                row = pl.multiple_of(((z + NZ - dz) % NZ) * LON, LON)
                o_refs[dx * NC + dc][pl.ds(row, LON), :] = b_refs[dz][pl.ds(field, LON, stride=8), :]


def spread_x(pos, blocks):
    return pl.pallas_call(
        spread_x_kernel,
        in_specs=[SMEM] + [VMEM] * NZ,
        out_specs=[VMEM] * (NX * NC),
        out_shape=[f32(NZ * LON, LANES)] * (NX * NC),
        compiler_params=PARAMS,
        name="spread_x",
    )(pos, *blocks)


def spread_out_kernel(pos_ref, *refs):
    h_refs, o_refs = refs[:NZ], refs[NZ:]
    x, z, c = pos_ref[0], pos_ref[1], pos_ref[2]
    for dx in range(NX):
        for dc in range(NC):
            source = pl.multiple_of((((x + dx) % NX) * NC + (c + dc) % NC) * KEPT, KEPT)
            for dz in range(NZ):
                row = pl.multiple_of(((z + NZ - dz) % NZ) * KEPT, KEPT)
                o_refs[dx * NC + dc][pl.ds(row, KEPT), :] = h_refs[dz][pl.ds(source, KEPT), :]


def spread_out(pos, blocks):
    return pl.pallas_call(
        spread_out_kernel,
        in_specs=[SMEM] + [VMEM] * NZ,
        out_specs=[VMEM] * (NX * NC),
        out_shape=[f32(NZ * KEPT, LANES)] * (NX * NC),
        compiler_params=PARAMS,
        name="spread_out",
    )(pos, *blocks)


PAD_F = FIELDS + 8


def relayout_a_kernel(s_ref, o_ref, x_ref, buf_ref, sem, out_sem):
    copies = [
        pltpu.make_async_copy(
            s_ref.at[n, :, pl.ds(LANES, LANES)], x_ref.at[pl.ds(n * PAD_F, FIELDS), :], sem.at[n]
        )
        for n in range(LON)
    ]
    for copy in copies:
        copy.start()
    for copy in copies:
        copy.wait()

    def field(f, carry):
        for eight in range(LON // 8):
            buf_ref[f, eight * 8 : eight * 8 + 8, :] = x_ref[pl.ds(eight * 8 * PAD_F + f, 8, stride=PAD_F), :]
        return carry

    send_pieces(field, FIELDS, buf_ref, o_ref, out_sem)


def relayout_a(state):
    return pl.pallas_call(
        relayout_a_kernel,
        in_specs=[HBM],
        out_specs=HBM,
        out_shape=f32(FIELDS, LON, LANES),
        scratch_shapes=[
            pltpu.VMEM((LON * PAD_F, LANES), jnp.float32),
            pltpu.VMEM((FIELDS, LON, LANES), jnp.float32),
            pltpu.SemaphoreType.DMA((LON,)),
            pltpu.SemaphoreType.DMA((PIECES,)),
        ],
        compiler_params=PARAMS,
        name="relayout_a",
    )(state)


PAD_K = KEPT + 8


def store_half(x_ref, buf_ref, o_ref, sem, lane):
    copies = []
    step = KEPT // PIECES
    for piece in range(PIECES):
        for kept in range(piece * step, (piece + 1) * step):
            for eight in range(FIELDS // 8):
                buf_ref[kept, eight * 8 : eight * 8 + 8, :] = x_ref[pl.ds(eight * 8 * PAD_K + kept, 8, stride=PAD_K), :]
        copy = pltpu.make_async_copy(
            buf_ref.at[pl.ds(piece * step, step)],
            o_ref.at[pl.ds(piece * step, step), :, pl.ds(lane, LANES)],
            sem.at[piece],
        )
        copy.start()
        copies.append(copy)
    for copy in copies:
        copy.wait()


STORE_SCRATCH = [
    pltpu.VMEM((FIELDS * PAD_K, LANES), jnp.float32),
    pltpu.VMEM((KEPT, FIELDS, LANES), jnp.float32),
    pltpu.SemaphoreType.DMA((PIECES,)),
]


def store_p_kernel(pos_ref, *refs):
    q_refs, o_ref = refs[:8], refs[8]
    x_ref, buf_ref, sem = refs[9:]
    x, c = pos_ref[0], pos_ref[2]
    for dx in range(NX):
        for dc in range(NC):
            base = ((x + NX - dx) % NX) * NC + (c + dc) % NC
            for zz in range(NZ):
                row = pl.multiple_of((base + zz * NX * NC) * PAD_K, 8)
                x_ref[pl.ds(row, KEPT), :] = q_refs[dx * NC + dc][zz * KEPT : (zz + 1) * KEPT, :]
    store_half(x_ref, buf_ref, o_ref, sem, 0)


def store_p(pos, blocks):
    return pl.pallas_call(
        store_p_kernel,
        in_specs=[SMEM] + [VMEM] * 8,
        out_specs=HBM,
        out_shape=f32(KEPT, FIELDS, 2 * LANES),
        scratch_shapes=STORE_SCRATCH,
        compiler_params=PARAMS,
        name="store_p",
    )(pos, *blocks)


def store_a_kernel(prior_ref, q_ref, o_ref, x_ref, buf_ref, sem):
    del prior_ref

    def field(f, carry):
        x_ref[pl.ds(pl.multiple_of(f * PAD_K, 8), KEPT), :] = q_ref[f]
        return carry

    lax.fori_loop(0, FIELDS, field, 0, unroll=8)
    store_half(x_ref, buf_ref, o_ref, sem, LANES)


def store_a(prior, shares):
    return pl.pallas_call(
        store_a_kernel,
        in_specs=[HBM, VMEM],
        out_specs=HBM,
        out_shape=f32(KEPT, FIELDS, 2 * LANES),
        scratch_shapes=STORE_SCRATCH,
        input_output_aliases={0: 0},
        compiler_params=PARAMS,
        name="store_a",
    )(prior, shares)


def shifts(dx, dz, dc):
    def at(x, z, c):
        return (x % NX) * NZ * NC + (z % NZ) * NC + c % NC

    return [
        (at(x, z, c), at(x + dx, z + dz, c + dc)) for x in range(NX) for z in range(NZ) for c in range(NC)
    ]


Z_ORDER = (4, 3, 5, 2, 6, 1, 7)


def exchange_z(blocks):
    out = [None] * NZ
    out[0] = blocks[0]
    for dz in Z_ORDER:
        out[dz] = lax.ppermute(blocks[dz], "lon", shifts(0, dz, 0))
    return out


def exchange_xc(blocks):
    out = [None] * (NX * NC)
    out[0] = blocks[0]
    for dx in (2, 1, 3, 0):
        for dc in range(NC):
            if dx or dc:
                out[dx * NC + dc] = lax.ppermute(blocks[dx * NC + dc], "lon", shifts(dx, 0, dc))
    return out


def local(state):
    device = lax.axis_index("lon")
    pos = jnp.stack([device // (NZ * NC), (device // NC) % NZ, device % NC]).astype(jnp.int32)
    wh, wl = twiddle_matrices(1.0 / math.sqrt(NLON))
    pieces = split_z(pos, state)
    pieces = exchange_z(pieces)
    sent = relayout_a(state)
    gathered = lax.all_to_all(sent, "lon", split_axis=0, concat_axis=0, tiled=True)
    pieces = spread_x(pos, [b.reshape(LON * 8, LANES) for b in pieces])
    pieces = exchange_xc(pieces)
    pieces = fft_p(pos, pieces, wh, wl)
    pieces = exchange_z(pieces)
    spectrum = fft_a(gathered.reshape(NLON, LANES), wh, wl)
    shares = lax.all_to_all(spectrum, "lon", split_axis=0, concat_axis=0, tiled=True)
    pieces = spread_out(pos, pieces)
    pieces = exchange_xc(pieces)
    out = store_p(pos, pieces)
    out = store_a(out, shares)
    return out.reshape(2, RADIX, FIELDS, 2 * LANES)


def solution(mesh):
    return jax.shard_map(
        local,
        mesh=mesh,
        in_specs=(P("lon", None, "lat"),),
        out_specs=P(None, "lon", None, "lat"),
        check_vma=False,
    )
```

```python
import math

import jax
import jax.numpy as jnp
from jax import lax
from jax.experimental import pallas as pl
from jax.experimental.pallas import tpu as pltpu
from jax.sharding import PartitionSpec as P


NLON = 2048
RADIX = 16
INNER = NLON // RADIX
PEERS = 64
HALF = RADIX // 2
NX, NZ, NC = 4, 8, 2
LON = 32
KEPT = 2 * RADIX
FIELDS = 64
LANES = 128
VMEM = pl.BlockSpec(memory_space=pltpu.VMEM)
HBM = pl.BlockSpec(memory_space=pltpu.HBM)
SMEM = pl.BlockSpec(memory_space=pltpu.SMEM)
PARAMS = pltpu.CompilerParams(vmem_limit_bytes=16 * 1024 * 1024)


def f32(*shape):
    return jax.ShapeDtypeStruct(shape, jnp.float32)


def split_bf16(v):
    high = v.astype(jnp.bfloat16)
    low = (v - high.astype(jnp.float32)).astype(jnp.bfloat16)
    return high, low


def phase(rows, cols):
    turn = (rows * cols) % NLON
    turn = jnp.where(turn >= NLON // 2, turn - NLON, turn)
    return turn.astype(jnp.float32) * (2.0 * math.pi / NLON)


def twiddle_matrices(scale):
    shape = (HALF, 2, PEERS, INNER)
    pair = lax.broadcasted_iota(jnp.int32, shape, 0)
    mirror = lax.broadcasted_iota(jnp.int32, shape, 1)
    outer = lax.broadcasted_iota(jnp.int32, shape, 2)
    inner = lax.broadcasted_iota(jnp.int32, shape, 3)
    first = jnp.where(mirror == 0, pair, jnp.where(pair == 0, HALF, RADIX - pair))
    angle = phase(inner, first + RADIX * outer)
    c = jnp.cos(angle) * scale
    s = jnp.sin(angle) * scale
    real_only = pair == 0
    zero = jnp.zeros_like(c)
    plain = mirror == 0
    re_a = jnp.where(real_only, jnp.where(plain, c, zero), c)
    im_a = jnp.where(real_only, jnp.where(plain, -s, zero), -s)
    re_b = jnp.where(real_only, jnp.where(plain, zero, c), jnp.where(plain, s, -s))
    im_b = jnp.where(real_only, jnp.where(plain, zero, -s), jnp.where(plain, c, -c))
    re = jnp.concatenate([re_a, re_b], axis=-1)
    im = jnp.concatenate([im_a, im_b], axis=-1)
    full = jnp.stack([re, im], axis=2)
    full = full.reshape(HALF, 4 * PEERS, 2 * INNER)
    high = lax.reduce_precision(full, 8, 7)
    return high.astype(jnp.bfloat16), (full - high).astype(jnp.bfloat16)


def fft_real16(x):
    def fft_complex8(z):
        def fft4(a):
            (ar, ai), (br, bi), (cr, ci), (dr, di) = a
            sr, si = ar + cr, ai + ci
            tr, ti = ar - cr, ai - ci
            ur, ui = br + dr, bi + di
            vr, vi = br - dr, bi - di
            return [(sr + ur, si + ui), (tr + vi, ti - vr), (sr - ur, si - ui), (tr - vi, ti + vr)]

        even = fft4(z[0::2])
        odd = fft4(z[1::2])
        h = math.sqrt(0.5)
        out = [None] * 8
        for k in range(4):
            er, ei = even[k]
            pr, pi = odd[k]
            if k == 1:
                pr, pi = (pr + pi) * h, (pi - pr) * h
            elif k == 2:
                pr, pi = pi, -pr
            elif k == 3:
                pr, pi = (pi - pr) * h, -(pr + pi) * h
            out[k] = (er + pr, ei + pi)
            out[k + 4] = (er - pr, ei - pi)
        return out

    z = fft_complex8([(x[2 * i], x[2 * i + 1]) for i in range(8)])
    out = [(z[0][0] + z[0][1], None)]
    for k in range(1, 8):
        zr, zi = z[k]
        wr, wi = z[8 - k]
        er, ei = (zr + wr) * 0.5, (zi - wi) * 0.5
        pr, pi = (zi + wi) * 0.5, (wr - zr) * 0.5
        c, s = math.cos(2 * math.pi * k / 16), math.sin(2 * math.pi * k / 16)
        out.append((er + c * pr + s * pi, ei + c * pi - s * pr))
    out.append((z[0][0] - z[0][1], None))
    return out


PAD_R = PEERS + 8


def fft_core(x_ref, wh_ref, wl_ref, y_ref, r_ref):
    def butterfly(i, carry):
        base = pl.multiple_of(i * 8, 8)
        x = [x_ref[pl.ds(n2 * INNER + base, 8), :] for n2 in range(RADIX)]
        y = fft_real16(x)
        for k in range(HALF):
            parts = (y[0][0], y[HALF][0]) if k == 0 else y[k]
            for j, part in enumerate(parts):
                y_ref[k, pl.ds(j * INNER + base, 8), :] = part
        return carry

    lax.fori_loop(0, INNER // 8, butterfly, 0)
    for k in range(HALF):
        yh, yl = split_bf16(y_ref[k])
        wh = wh_ref[k]
        r = jnp.dot(wh, yh, preferred_element_type=jnp.float32)
        r = r + jnp.dot(wh, yl, preferred_element_type=jnp.float32)
        r = r + jnp.dot(wl_ref[k], yh, preferred_element_type=jnp.float32)
        mirror = HALF if k == 0 else RADIX - k
        for q, row in enumerate((k, RADIX + k, mirror, RADIX + mirror)):
            r_ref[pl.ds(row * PAD_R, PEERS), :] = r[q * PEERS : (q + 1) * PEERS]


PIECES = 4


def send_pieces(body, count, buf_ref, o_ref, sem):
    step = count // PIECES
    copies = []
    for piece in range(PIECES):
        lax.fori_loop(piece * step, (piece + 1) * step, body, 0, unroll=4)
        rows = pl.ds(piece * step, step)
        copy = pltpu.make_async_copy(buf_ref.at[rows], o_ref.at[rows], sem.at[piece])
        copy.start()
        copies.append(copy)
    for copy in copies:
        copy.wait()


FFT_SCRATCH = [
    pltpu.VMEM((HALF, 2 * INNER, LANES), jnp.float32),
    pltpu.VMEM((KEPT * PAD_R, LANES), jnp.float32),
]


def mode_rows(r_ref, k1, eight):
    return r_ref[pl.ds(eight * 8 * PAD_R + k1, 8, stride=PAD_R), :]


def fft_a_kernel(x_ref, wh_ref, wl_ref, o_ref, y_ref, r_ref, buf_ref, sem):
    fft_core(x_ref, wh_ref, wl_ref, y_ref, r_ref)

    def peer(k1, carry):
        for eight in range(KEPT // 8):
            buf_ref[k1, eight * 8 : eight * 8 + 8, :] = mode_rows(r_ref, k1, eight)
        return carry

    send_pieces(peer, PEERS, buf_ref, o_ref, sem)


def fft_a(gathered, wh, wl):
    return pl.pallas_call(
        fft_a_kernel,
        in_specs=[VMEM] * 3,
        out_specs=HBM,
        out_shape=f32(PEERS, KEPT, LANES),
        scratch_shapes=FFT_SCRATCH
        + [pltpu.VMEM((PEERS, KEPT, LANES), jnp.float32), pltpu.SemaphoreType.DMA((PIECES,))],
        compiler_params=PARAMS,
        name="fft_a",
    )(gathered, wh, wl)


def fft_p_kernel(pos_ref, *refs):
    g_refs, (wh_ref, wl_ref), o_refs = refs[:8], refs[8:10], refs[10:18]
    x_ref, y_ref, r_ref = refs[18:]
    x, c = pos_ref[0], pos_ref[2]
    for dx in range(NX):
        for dc in range(NC):
            start = ((x + NX - dx) % NX) * (NLON // NX) + ((c + dc) % NC) * LON
            for zz in range(NZ):
                row = pl.multiple_of(start + zz * NC * LON, LON)
                x_ref[pl.ds(row, LON), :] = g_refs[dx * NC + dc][zz * LON : (zz + 1) * LON, :]
    fft_core(x_ref, wh_ref, wl_ref, y_ref, r_ref)
    for dx in range(NX):
        for dc in range(NC):
            target = ((x + dx) % NX) * NZ * NC + (c + dc) % NC
            for zz in range(NZ):
                for eight in range(KEPT // 8):
                    row = zz * KEPT + eight * 8
                    o_refs[dx * NC + dc][row : row + 8, :] = mode_rows(r_ref, target + zz * NC, eight)


def fft_p(pos, blocks, wh, wl):
    return pl.pallas_call(
        fft_p_kernel,
        in_specs=[SMEM] + [VMEM] * 10,
        out_specs=[VMEM] * (NX * NC),
        out_shape=[f32(NZ * KEPT, LANES)] * (NX * NC),
        scratch_shapes=[pltpu.VMEM((NLON, LANES), jnp.float32)] + FFT_SCRATCH,
        compiler_params=PARAMS,
        name="fft_p",
    )(pos, *blocks, wh, wl)


def split_z_kernel(pos_ref, s_ref, *refs):
    o_refs, sem = refs[:NZ], refs[NZ]
    z = pos_ref[1]
    copies = []
    for dz in range(NZ):
        field = pl.multiple_of(((z + dz) % NZ) * 8, 8)
        copies.append(
            pltpu.make_async_copy(s_ref.at[:, pl.ds(field, 8), pl.ds(0, LANES)], o_refs[dz], sem.at[dz])
        )
    for copy in copies:
        copy.start()
    for copy in copies:
        copy.wait()


def split_z(pos, state):
    return pl.pallas_call(
        split_z_kernel,
        in_specs=[SMEM, HBM],
        out_specs=[VMEM] * NZ,
        out_shape=[f32(LON, 8, LANES)] * NZ,
        scratch_shapes=[pltpu.SemaphoreType.DMA((NZ,))],
        compiler_params=PARAMS,
        name="split_z",
    )(pos, state)


def spread_x_kernel(pos_ref, *refs):
    b_refs, o_refs = refs[:NZ], refs[NZ:]
    x, z, c = pos_ref[0], pos_ref[1], pos_ref[2]
    for dx in range(NX):
        for dc in range(NC):
            field = ((x + dx) % NX) * NC + (c + dc) % NC
            for dz in range(NZ):
                row = pl.multiple_of(((z + NZ - dz) % NZ) * LON, LON)
                o_refs[dx * NC + dc][pl.ds(row, LON), :] = b_refs[dz][pl.ds(field, LON, stride=8), :]


def spread_x(pos, blocks):
    return pl.pallas_call(
        spread_x_kernel,
        in_specs=[SMEM] + [VMEM] * NZ,
        out_specs=[VMEM] * (NX * NC),
        out_shape=[f32(NZ * LON, LANES)] * (NX * NC),
        compiler_params=PARAMS,
        name="spread_x",
    )(pos, *blocks)


def spread_out_kernel(pos_ref, *refs):
    q_refs, o_refs = refs[:8], refs[8:]
    x, z, c = pos_ref[0], pos_ref[1], pos_ref[2]
    for dz in range(NZ):
        source = pl.multiple_of(((z + dz) % NZ) * KEPT, KEPT)
        for dx in range(NX):
            for dc in range(NC):
                row = pl.multiple_of((((x + NX - dx) % NX) * NC + (c + dc) % NC) * KEPT, KEPT)
                o_refs[dz][pl.ds(row, KEPT), :] = q_refs[dx * NC + dc][pl.ds(source, KEPT), :]


def spread_out(pos, blocks):
    return pl.pallas_call(
        spread_out_kernel,
        in_specs=[SMEM] + [VMEM] * (NX * NC),
        out_specs=[VMEM] * NZ,
        out_shape=[f32(NX * NC * KEPT, LANES)] * NZ,
        compiler_params=PARAMS,
        name="spread_out",
    )(pos, *blocks)


PAD_F = FIELDS + 8


def relayout_a_kernel(s_ref, o_ref, x_ref, buf_ref, sem, out_sem):
    copies = [
        pltpu.make_async_copy(
            s_ref.at[n, :, pl.ds(LANES, LANES)], x_ref.at[pl.ds(n * PAD_F, FIELDS), :], sem.at[n]
        )
        for n in range(LON)
    ]
    for copy in copies:
        copy.start()
    for copy in copies:
        copy.wait()

    def field(f, carry):
        for eight in range(LON // 8):
            buf_ref[f, eight * 8 : eight * 8 + 8, :] = x_ref[pl.ds(eight * 8 * PAD_F + f, 8, stride=PAD_F), :]
        return carry

    send_pieces(field, FIELDS, buf_ref, o_ref, out_sem)


def relayout_a(state):
    return pl.pallas_call(
        relayout_a_kernel,
        in_specs=[HBM],
        out_specs=HBM,
        out_shape=f32(FIELDS, LON, LANES),
        scratch_shapes=[
            pltpu.VMEM((LON * PAD_F, LANES), jnp.float32),
            pltpu.VMEM((FIELDS, LON, LANES), jnp.float32),
            pltpu.SemaphoreType.DMA((LON,)),
            pltpu.SemaphoreType.DMA((PIECES,)),
        ],
        compiler_params=PARAMS,
        name="relayout_a",
    )(state)


PAD_K = KEPT + 8


def store_half(x_ref, buf_ref, o_ref, sem, lane):
    copies = []
    step = KEPT // PIECES
    for piece in range(PIECES):
        for kept in range(piece * step, (piece + 1) * step):
            for eight in range(FIELDS // 8):
                buf_ref[kept, eight * 8 : eight * 8 + 8, :] = x_ref[pl.ds(eight * 8 * PAD_K + kept, 8, stride=PAD_K), :]
        copy = pltpu.make_async_copy(
            buf_ref.at[pl.ds(piece * step, step)],
            o_ref.at[pl.ds(piece * step, step), :, pl.ds(lane, LANES)],
            sem.at[piece],
        )
        copy.start()
        copies.append(copy)
    for copy in copies:
        copy.wait()


STORE_SCRATCH = [
    pltpu.VMEM((FIELDS * PAD_K, LANES), jnp.float32),
    pltpu.VMEM((KEPT, FIELDS, LANES), jnp.float32),
    pltpu.SemaphoreType.DMA((PIECES,)),
]


def store_p_kernel(pos_ref, prior_ref, *refs):
    del prior_ref
    h_refs, o_ref = refs[:NZ], refs[NZ]
    x_ref, buf_ref, sem = refs[NZ + 1 :]
    z = pos_ref[1]
    for dz in range(NZ):
        base = ((z + NZ - dz) % NZ) * 8 * PAD_K
        for s in range(8):
            row = pl.multiple_of(base + s * PAD_K, 8)
            x_ref[pl.ds(row, KEPT), :] = h_refs[dz][s * KEPT : (s + 1) * KEPT, :]
    store_half(x_ref, buf_ref, o_ref, sem, 0)


def store_p(pos, prior, blocks):
    return pl.pallas_call(
        store_p_kernel,
        in_specs=[SMEM, HBM] + [VMEM] * NZ,
        out_specs=HBM,
        out_shape=f32(KEPT, FIELDS, 2 * LANES),
        scratch_shapes=STORE_SCRATCH,
        input_output_aliases={1: 0},
        compiler_params=PARAMS,
        name="store_p",
    )(pos, prior, *blocks)


def store_a_kernel(q_ref, o_ref, x_ref, buf_ref, sem):
    def field(f, carry):
        x_ref[pl.ds(pl.multiple_of(f * PAD_K, 8), KEPT), :] = q_ref[f]
        return carry

    lax.fori_loop(0, FIELDS, field, 0, unroll=8)
    store_half(x_ref, buf_ref, o_ref, sem, LANES)


def store_a(shares):
    return pl.pallas_call(
        store_a_kernel,
        in_specs=[VMEM],
        out_specs=HBM,
        out_shape=f32(KEPT, FIELDS, 2 * LANES),
        scratch_shapes=STORE_SCRATCH,
        compiler_params=PARAMS,
        name="store_a",
    )(shares)


def shifts(dx, dz, dc):
    def at(x, z, c):
        return (x % NX) * NZ * NC + (z % NZ) * NC + c % NC

    return [
        (at(x, z, c), at(x + dx, z + dz, c + dc)) for x in range(NX) for z in range(NZ) for c in range(NC)
    ]


Z_FAR = (4, 3, 5)
Z_NEAR = (2, 6, 1, 7)


def exchange_z(blocks):
    out = [None] * NZ
    out[0] = blocks[0]
    for group in (Z_FAR, Z_NEAR):
        for dz in group:
            out[dz] = lax.ppermute(blocks[dz], "lon", shifts(0, dz, 0))
    return out


def exchange_xc(blocks):
    out = [None] * (NX * NC)
    out[0] = blocks[0]
    for dx in (2, 1, 3, 0):
        for dc in range(NC):
            if dx or dc:
                out[dx * NC + dc] = lax.ppermute(blocks[dx * NC + dc], "lon", shifts(dx, 0, dc))
    return out


def local(state):
    device = lax.axis_index("lon")
    pos = jnp.stack([device // (NZ * NC), (device // NC) % NZ, device % NC]).astype(jnp.int32)
    wh, wl = twiddle_matrices(1.0 / math.sqrt(NLON))
    pieces = split_z(pos, state)
    pieces = exchange_z(pieces)
    sent = relayout_a(state)
    gathered = lax.all_to_all(sent, "lon", split_axis=0, concat_axis=0, tiled=True)
    pieces = spread_x(pos, [b.reshape(LON * 8, LANES) for b in pieces])
    pieces = exchange_xc(pieces)
    spectrum = fft_a(gathered.reshape(NLON, LANES), wh, wl)
    shares = lax.all_to_all(spectrum, "lon", split_axis=0, concat_axis=0, tiled=True)
    pieces = fft_p(pos, pieces, wh, wl)
    pieces = exchange_xc(pieces)
    pieces = spread_out(pos, pieces)
    pieces = exchange_z(pieces)
    out = store_a(shares)
    out = store_p(pos, out, pieces)
    return out.reshape(2, RADIX, FIELDS, 2 * LANES)


def solution(mesh):
    return jax.shard_map(
        local,
        mesh=mesh,
        in_specs=(P("lon", None, "lat"),),
        out_specs=P(None, "lon", None, "lat"),
        check_vma=False,
    )
```

```python
import math

import jax
import jax.numpy as jnp
from jax import lax
from jax.experimental import pallas as pl
from jax.experimental.pallas import tpu as pltpu
from jax.sharding import PartitionSpec as P


NLON = 2048
RADIX = 16
INNER = NLON // RADIX
PEERS = 64
HALF = RADIX // 2
NX, NZ, NC = 4, 8, 2
LON = 32
KEPT = 2 * RADIX
FIELDS = 64
LANES = 128
VMEM = pl.BlockSpec(memory_space=pltpu.VMEM)
HBM = pl.BlockSpec(memory_space=pltpu.HBM)
SMEM = pl.BlockSpec(memory_space=pltpu.SMEM)
PARAMS = pltpu.CompilerParams(vmem_limit_bytes=16 * 1024 * 1024)


def f32(*shape):
    return jax.ShapeDtypeStruct(shape, jnp.float32)


def split_bf16(v):
    high = v.astype(jnp.bfloat16)
    low = (v - high.astype(jnp.float32)).astype(jnp.bfloat16)
    return high, low


def phase(rows, cols):
    turn = (rows * cols) % NLON
    turn = jnp.where(turn >= NLON // 2, turn - NLON, turn)
    return turn.astype(jnp.float32) * (2.0 * math.pi / NLON)


def twiddle_matrices(scale):
    shape = (HALF, 2, PEERS, INNER)
    pair = lax.broadcasted_iota(jnp.int32, shape, 0)
    mirror = lax.broadcasted_iota(jnp.int32, shape, 1)
    outer = lax.broadcasted_iota(jnp.int32, shape, 2)
    inner = lax.broadcasted_iota(jnp.int32, shape, 3)
    first = jnp.where(mirror == 0, pair, jnp.where(pair == 0, HALF, RADIX - pair))
    angle = phase(inner, first + RADIX * outer)
    c = jnp.cos(angle) * scale
    s = jnp.sin(angle) * scale
    real_only = pair == 0
    zero = jnp.zeros_like(c)
    plain = mirror == 0
    re_a = jnp.where(real_only, jnp.where(plain, c, zero), c)
    im_a = jnp.where(real_only, jnp.where(plain, -s, zero), -s)
    re_b = jnp.where(real_only, jnp.where(plain, zero, c), jnp.where(plain, s, -s))
    im_b = jnp.where(real_only, jnp.where(plain, zero, -s), jnp.where(plain, c, -c))
    re = jnp.concatenate([re_a, re_b], axis=-1)
    im = jnp.concatenate([im_a, im_b], axis=-1)
    full = jnp.stack([re, im], axis=2)
    full = full.reshape(HALF, 4 * PEERS, 2 * INNER)
    high = lax.reduce_precision(full, 8, 7)
    return high.astype(jnp.bfloat16), (full - high).astype(jnp.bfloat16)


def fft_real16(x):
    def fft_complex8(z):
        def fft4(a):
            (ar, ai), (br, bi), (cr, ci), (dr, di) = a
            sr, si = ar + cr, ai + ci
            tr, ti = ar - cr, ai - ci
            ur, ui = br + dr, bi + di
            vr, vi = br - dr, bi - di
            return [(sr + ur, si + ui), (tr + vi, ti - vr), (sr - ur, si - ui), (tr - vi, ti + vr)]

        even = fft4(z[0::2])
        odd = fft4(z[1::2])
        h = math.sqrt(0.5)
        out = [None] * 8
        for k in range(4):
            er, ei = even[k]
            pr, pi = odd[k]
            if k == 1:
                pr, pi = (pr + pi) * h, (pi - pr) * h
            elif k == 2:
                pr, pi = pi, -pr
            elif k == 3:
                pr, pi = (pi - pr) * h, -(pr + pi) * h
            out[k] = (er + pr, ei + pi)
            out[k + 4] = (er - pr, ei - pi)
        return out

    z = fft_complex8([(x[2 * i], x[2 * i + 1]) for i in range(8)])
    out = [(z[0][0] + z[0][1], None)]
    for k in range(1, 8):
        zr, zi = z[k]
        wr, wi = z[8 - k]
        er, ei = (zr + wr) * 0.5, (zi - wi) * 0.5
        pr, pi = (zi + wi) * 0.5, (wr - zr) * 0.5
        c, s = math.cos(2 * math.pi * k / 16), math.sin(2 * math.pi * k / 16)
        out.append((er + c * pr + s * pi, ei + c * pi - s * pr))
    out.append((z[0][0] - z[0][1], None))
    return out


PAD_R = PEERS + 8


def fft_core(x_ref, wh_ref, wl_ref, y_ref, r_ref):
    def butterfly(i, carry):
        base = pl.multiple_of(i * 8, 8)
        x = [x_ref[pl.ds(n2 * INNER + base, 8), :] for n2 in range(RADIX)]
        y = fft_real16(x)
        for k in range(HALF):
            parts = (y[0][0], y[HALF][0]) if k == 0 else y[k]
            for j, part in enumerate(parts):
                y_ref[k, pl.ds(j * INNER + base, 8), :] = part
        return carry

    lax.fori_loop(0, INNER // 8, butterfly, 0)
    for k in range(HALF):
        yh, yl = split_bf16(y_ref[k])
        wh = wh_ref[k]
        r = jnp.dot(wh, yh, preferred_element_type=jnp.float32)
        r = r + jnp.dot(wh, yl, preferred_element_type=jnp.float32)
        r = r + jnp.dot(wl_ref[k], yh, preferred_element_type=jnp.float32)
        mirror = HALF if k == 0 else RADIX - k
        for q, row in enumerate((k, RADIX + k, mirror, RADIX + mirror)):
            r_ref[pl.ds(row * PAD_R, PEERS), :] = r[q * PEERS : (q + 1) * PEERS]


PIECES = 4


def send_pieces(body, count, buf_ref, o_ref, sem):
    step = count // PIECES
    copies = []
    for piece in range(PIECES):
        lax.fori_loop(piece * step, (piece + 1) * step, body, 0, unroll=4)
        rows = pl.ds(piece * step, step)
        copy = pltpu.make_async_copy(buf_ref.at[rows], o_ref.at[rows], sem.at[piece])
        copy.start()
        copies.append(copy)
    for copy in copies:
        copy.wait()


FFT_SCRATCH = [
    pltpu.VMEM((HALF, 2 * INNER, LANES), jnp.float32),
    pltpu.VMEM((KEPT * PAD_R, LANES), jnp.float32),
]


def mode_rows(r_ref, k1, eight):
    return r_ref[pl.ds(eight * 8 * PAD_R + k1, 8, stride=PAD_R), :]


def fft_a_kernel(x_ref, wh_ref, wl_ref, o_ref, y_ref, r_ref, buf_ref, sem):
    fft_core(x_ref, wh_ref, wl_ref, y_ref, r_ref)

    def peer(k1, carry):
        for eight in range(KEPT // 8):
            buf_ref[k1, eight * 8 : eight * 8 + 8, :] = mode_rows(r_ref, k1, eight)
        return carry

    send_pieces(peer, PEERS, buf_ref, o_ref, sem)


def fft_a(gathered, wh, wl):
    return pl.pallas_call(
        fft_a_kernel,
        in_specs=[VMEM] * 3,
        out_specs=HBM,
        out_shape=f32(PEERS, KEPT, LANES),
        scratch_shapes=FFT_SCRATCH
        + [pltpu.VMEM((PEERS, KEPT, LANES), jnp.float32), pltpu.SemaphoreType.DMA((PIECES,))],
        compiler_params=PARAMS,
        name="fft_a",
    )(gathered, wh, wl)


def fft_p_kernel(pos_ref, *refs):
    g_refs, (wh_ref, wl_ref), o_refs = refs[:8], refs[8:10], refs[10:18]
    x_ref, y_ref, r_ref = refs[18:]
    x, z, c = pos_ref[0], pos_ref[1], pos_ref[2]
    for dx in range(NX):
        for dc in range(NC):
            start = ((x + NX - dx) % NX) * (NLON // NX) + ((c + dc) % NC) * LON
            for zz in range(NZ):
                row = pl.multiple_of(start + zz * NC * LON, LON)
                x_ref[pl.ds(row, LON), :] = g_refs[dx * NC + dc][zz * LON : (zz + 1) * LON, :]
    fft_core(x_ref, wh_ref, wl_ref, y_ref, r_ref)
    for dz in range(NZ):
        target = (z + dz) % NZ
        for xx in range(NX):
            for cc in range(NC):
                k1 = xx * NZ * NC + target * NC + cc
                for eight in range(KEPT // 8):
                    row = (xx * NC + cc) * KEPT + eight * 8
                    o_refs[dz][row : row + 8, :] = mode_rows(r_ref, k1, eight)


def fft_p(pos, blocks, wh, wl):
    return pl.pallas_call(
        fft_p_kernel,
        in_specs=[SMEM] + [VMEM] * 10,
        out_specs=[VMEM] * NZ,
        out_shape=[f32(NX * NC * KEPT, LANES)] * NZ,
        scratch_shapes=[pltpu.VMEM((NLON, LANES), jnp.float32)] + FFT_SCRATCH,
        compiler_params=PARAMS,
        name="fft_p",
    )(pos, *blocks, wh, wl)


def split_z_kernel(pos_ref, s_ref, *refs):
    o_refs, sem = refs[:NZ], refs[NZ]
    z = pos_ref[1]
    copies = []
    for dz in range(NZ):
        field = pl.multiple_of(((z + dz) % NZ) * 8, 8)
        copies.append(
            pltpu.make_async_copy(s_ref.at[:, pl.ds(field, 8), pl.ds(0, LANES)], o_refs[dz], sem.at[dz])
        )
    for copy in copies:
        copy.start()
    for copy in copies:
        copy.wait()


def split_z(pos, state):
    return pl.pallas_call(
        split_z_kernel,
        in_specs=[SMEM, HBM],
        out_specs=[VMEM] * NZ,
        out_shape=[f32(LON, 8, LANES)] * NZ,
        scratch_shapes=[pltpu.SemaphoreType.DMA((NZ,))],
        compiler_params=PARAMS,
        name="split_z",
    )(pos, state)


def spread_x_kernel(pos_ref, *refs):
    b_refs, o_refs = refs[:NZ], refs[NZ:]
    x, z, c = pos_ref[0], pos_ref[1], pos_ref[2]
    for dx in range(NX):
        for dc in range(NC):
            field = ((x + dx) % NX) * NC + (c + dc) % NC
            for dz in range(NZ):
                row = pl.multiple_of(((z + NZ - dz) % NZ) * LON, LON)
                o_refs[dx * NC + dc][pl.ds(row, LON), :] = b_refs[dz][pl.ds(field, LON, stride=8), :]


def spread_x(pos, blocks):
    return pl.pallas_call(
        spread_x_kernel,
        in_specs=[SMEM] + [VMEM] * NZ,
        out_specs=[VMEM] * (NX * NC),
        out_shape=[f32(NZ * LON, LANES)] * (NX * NC),
        compiler_params=PARAMS,
        name="spread_x",
    )(pos, *blocks)


def spread_out_kernel(pos_ref, *refs):
    h_refs, o_refs = refs[:NZ], refs[NZ:]
    x, z, c = pos_ref[0], pos_ref[1], pos_ref[2]
    for dx in range(NX):
        for dc in range(NC):
            source = pl.multiple_of((((x + dx) % NX) * NC + (c + dc) % NC) * KEPT, KEPT)
            for dz in range(NZ):
                row = pl.multiple_of(((z + NZ - dz) % NZ) * KEPT, KEPT)
                o_refs[dx * NC + dc][pl.ds(row, KEPT), :] = h_refs[dz][pl.ds(source, KEPT), :]


def spread_out(pos, blocks):
    return pl.pallas_call(
        spread_out_kernel,
        in_specs=[SMEM] + [VMEM] * NZ,
        out_specs=[VMEM] * (NX * NC),
        out_shape=[f32(NZ * KEPT, LANES)] * (NX * NC),
        compiler_params=PARAMS,
        name="spread_out",
    )(pos, *blocks)


PAD_F = FIELDS + 8


def relayout_a_kernel(s_ref, o_ref, x_ref, buf_ref, sem, out_sem):
    copies = [
        pltpu.make_async_copy(
            s_ref.at[n, :, pl.ds(LANES, LANES)], x_ref.at[pl.ds(n * PAD_F, FIELDS), :], sem.at[n]
        )
        for n in range(LON)
    ]
    for copy in copies:
        copy.start()
    for copy in copies:
        copy.wait()

    def field(f, carry):
        for eight in range(LON // 8):
            buf_ref[f, eight * 8 : eight * 8 + 8, :] = x_ref[pl.ds(eight * 8 * PAD_F + f, 8, stride=PAD_F), :]
        return carry

    send_pieces(field, FIELDS, buf_ref, o_ref, out_sem)


def relayout_a(state):
    return pl.pallas_call(
        relayout_a_kernel,
        in_specs=[HBM],
        out_specs=HBM,
        out_shape=f32(FIELDS, LON, LANES),
        scratch_shapes=[
            pltpu.VMEM((LON * PAD_F, LANES), jnp.float32),
            pltpu.VMEM((FIELDS, LON, LANES), jnp.float32),
            pltpu.SemaphoreType.DMA((LON,)),
            pltpu.SemaphoreType.DMA((PIECES,)),
        ],
        compiler_params=PARAMS,
        name="relayout_a",
    )(state)


PAD_K = KEPT + 8


def store_half(x_ref, buf_ref, o_ref, sem, lane):
    copies = []
    step = KEPT // PIECES
    for piece in range(PIECES):
        for kept in range(piece * step, (piece + 1) * step):
            for eight in range(FIELDS // 8):
                buf_ref[kept, eight * 8 : eight * 8 + 8, :] = x_ref[pl.ds(eight * 8 * PAD_K + kept, 8, stride=PAD_K), :]
        copy = pltpu.make_async_copy(
            buf_ref.at[pl.ds(piece * step, step)],
            o_ref.at[pl.ds(piece * step, step), :, pl.ds(lane, LANES)],
            sem.at[piece],
        )
        copy.start()
        copies.append(copy)
    for copy in copies:
        copy.wait()


STORE_SCRATCH = [
    pltpu.VMEM((FIELDS * PAD_K, LANES), jnp.float32),
    pltpu.VMEM((KEPT, FIELDS, LANES), jnp.float32),
    pltpu.SemaphoreType.DMA((PIECES,)),
]


def store_p_kernel(pos_ref, *refs):
    q_refs, o_ref = refs[:8], refs[8]
    x_ref, buf_ref, sem = refs[9:]
    x, c = pos_ref[0], pos_ref[2]
    for dx in range(NX):
        for dc in range(NC):
            base = ((x + NX - dx) % NX) * NC + (c + dc) % NC
            for zz in range(NZ):
                row = pl.multiple_of((base + zz * NX * NC) * PAD_K, 8)
                x_ref[pl.ds(row, KEPT), :] = q_refs[dx * NC + dc][zz * KEPT : (zz + 1) * KEPT, :]
    store_half(x_ref, buf_ref, o_ref, sem, 0)


def store_p(pos, blocks):
    return pl.pallas_call(
        store_p_kernel,
        in_specs=[SMEM] + [VMEM] * 8,
        out_specs=HBM,
        out_shape=f32(KEPT, FIELDS, 2 * LANES),
        scratch_shapes=STORE_SCRATCH,
        compiler_params=PARAMS,
        name="store_p",
    )(pos, *blocks)


def store_a_kernel(prior_ref, q_ref, o_ref, x_ref, buf_ref, sem):
    del prior_ref

    def field(f, carry):
        x_ref[pl.ds(pl.multiple_of(f * PAD_K, 8), KEPT), :] = q_ref[f]
        return carry

    lax.fori_loop(0, FIELDS, field, 0, unroll=8)
    store_half(x_ref, buf_ref, o_ref, sem, LANES)


def store_a(prior, shares):
    return pl.pallas_call(
        store_a_kernel,
        in_specs=[HBM, VMEM],
        out_specs=HBM,
        out_shape=f32(KEPT, FIELDS, 2 * LANES),
        scratch_shapes=STORE_SCRATCH,
        input_output_aliases={0: 0},
        compiler_params=PARAMS,
        name="store_a",
    )(prior, shares)


def shifts(dx, dz, dc):
    def at(x, z, c):
        return (x % NX) * NZ * NC + (z % NZ) * NC + c % NC

    return [
        (at(x, z, c), at(x + dx, z + dz, c + dc)) for x in range(NX) for z in range(NZ) for c in range(NC)
    ]


Z_ORDER = (4, 3, 5, 2, 6, 1, 7)


def exchange_z(blocks):
    out = [None] * NZ
    out[0] = blocks[0]
    for dz in Z_ORDER:
        out[dz] = lax.ppermute(blocks[dz], "lon", shifts(0, dz, 0))
    return out


X_ORDER = ((2, 0), (2, 1), (1, 0), (3, 0), (1, 1), (3, 1), (0, 1))


def exchange_xc(blocks):
    out = [None] * (NX * NC)
    out[0] = blocks[0]
    for dx, dc in X_ORDER:
        out[dx * NC + dc] = lax.ppermute(blocks[dx * NC + dc], "lon", shifts(dx, 0, dc))
    return out


def local(state):
    device = lax.axis_index("lon")
    pos = jnp.stack([device // (NZ * NC), (device // NC) % NZ, device % NC]).astype(jnp.int32)
    wh, wl = twiddle_matrices(1.0 / math.sqrt(NLON))
    pieces = split_z(pos, state)
    pieces = exchange_z(pieces)
    sent = relayout_a(state)
    gathered = lax.all_to_all(sent, "lon", split_axis=0, concat_axis=0, tiled=True)
    pieces = spread_x(pos, [b.reshape(LON * 8, LANES) for b in pieces])
    pieces = exchange_xc(pieces)
    pieces = fft_p(pos, pieces, wh, wl)
    pieces = exchange_z(pieces)
    spectrum = fft_a(gathered.reshape(NLON, LANES), wh, wl)
    shares = lax.all_to_all(spectrum, "lon", split_axis=0, concat_axis=0, tiled=True)
    pieces = spread_out(pos, pieces)
    pieces = exchange_xc(pieces)
    out = store_p(pos, pieces)
    out = store_a(out, shares)
    return out.reshape(2, RADIX, FIELDS, 2 * LANES)


def solution(mesh):
    return jax.shard_map(
        local,
        mesh=mesh,
        in_specs=(P("lon", None, "lat"),),
        out_specs=P(None, "lon", None, "lat"),
        check_vma=False,
    )
```

```python
import math

import jax
import jax.numpy as jnp
from jax import lax
from jax.experimental import pallas as pl
from jax.experimental.pallas import tpu as pltpu
from jax.sharding import PartitionSpec as P


NLON = 2048
RADIX = 16
INNER = NLON // RADIX
PEERS = 64
HALF = RADIX // 2
NX, NZ, NC = 4, 8, 2
LON = 32
KEPT = 2 * RADIX
FIELDS = 64
LANES = 128
VMEM = pl.BlockSpec(memory_space=pltpu.VMEM)
HBM = pl.BlockSpec(memory_space=pltpu.HBM)
SMEM = pl.BlockSpec(memory_space=pltpu.SMEM)
PARAMS = pltpu.CompilerParams(vmem_limit_bytes=16 * 1024 * 1024)


def f32(*shape):
    return jax.ShapeDtypeStruct(shape, jnp.float32)


def split_bf16(v):
    high = v.astype(jnp.bfloat16)
    low = (v - high.astype(jnp.float32)).astype(jnp.bfloat16)
    return high, low


def phase(rows, cols):
    turn = (rows * cols) % NLON
    turn = jnp.where(turn >= NLON // 2, turn - NLON, turn)
    return turn.astype(jnp.float32) * (2.0 * math.pi / NLON)


def twiddle_matrices(scale):
    shape = (HALF, 2, PEERS, INNER)
    pair = lax.broadcasted_iota(jnp.int32, shape, 0)
    mirror = lax.broadcasted_iota(jnp.int32, shape, 1)
    outer = lax.broadcasted_iota(jnp.int32, shape, 2)
    inner = lax.broadcasted_iota(jnp.int32, shape, 3)
    first = jnp.where(mirror == 0, pair, jnp.where(pair == 0, HALF, RADIX - pair))
    angle = phase(inner, first + RADIX * outer)
    c = jnp.cos(angle) * scale
    s = jnp.sin(angle) * scale
    real_only = pair == 0
    zero = jnp.zeros_like(c)
    plain = mirror == 0
    re_a = jnp.where(real_only, jnp.where(plain, c, zero), c)
    im_a = jnp.where(real_only, jnp.where(plain, -s, zero), -s)
    re_b = jnp.where(real_only, jnp.where(plain, zero, c), jnp.where(plain, s, -s))
    im_b = jnp.where(real_only, jnp.where(plain, zero, -s), jnp.where(plain, c, -c))
    re = jnp.concatenate([re_a, re_b], axis=-1)
    im = jnp.concatenate([im_a, im_b], axis=-1)
    full = jnp.stack([re, im], axis=2)
    full = full.reshape(HALF, 4 * PEERS, 2 * INNER)
    high = lax.reduce_precision(full, 8, 7)
    return high.astype(jnp.bfloat16), (full - high).astype(jnp.bfloat16)


def fft_real16(x):
    def fft_complex8(z):
        def fft4(a):
            (ar, ai), (br, bi), (cr, ci), (dr, di) = a
            sr, si = ar + cr, ai + ci
            tr, ti = ar - cr, ai - ci
            ur, ui = br + dr, bi + di
            vr, vi = br - dr, bi - di
            return [(sr + ur, si + ui), (tr + vi, ti - vr), (sr - ur, si - ui), (tr - vi, ti + vr)]

        even = fft4(z[0::2])
        odd = fft4(z[1::2])
        h = math.sqrt(0.5)
        out = [None] * 8
        for k in range(4):
            er, ei = even[k]
            pr, pi = odd[k]
            if k == 1:
                pr, pi = (pr + pi) * h, (pi - pr) * h
            elif k == 2:
                pr, pi = pi, -pr
            elif k == 3:
                pr, pi = (pi - pr) * h, -(pr + pi) * h
            out[k] = (er + pr, ei + pi)
            out[k + 4] = (er - pr, ei - pi)
        return out

    z = fft_complex8([(x[2 * i], x[2 * i + 1]) for i in range(8)])
    out = [(z[0][0] + z[0][1], None)]
    for k in range(1, 8):
        zr, zi = z[k]
        wr, wi = z[8 - k]
        er, ei = (zr + wr) * 0.5, (zi - wi) * 0.5
        pr, pi = (zi + wi) * 0.5, (wr - zr) * 0.5
        c, s = math.cos(2 * math.pi * k / 16), math.sin(2 * math.pi * k / 16)
        out.append((er + c * pr + s * pi, ei + c * pi - s * pr))
    out.append((z[0][0] - z[0][1], None))
    return out


PAD_R = PEERS + 8


def fft_core(x_ref, wh_ref, wl_ref, y_ref, r_ref):
    def butterfly(i, carry):
        base = pl.multiple_of(i * 8, 8)
        x = [x_ref[pl.ds(n2 * INNER + base, 8), :] for n2 in range(RADIX)]
        y = fft_real16(x)
        for k in range(HALF):
            parts = (y[0][0], y[HALF][0]) if k == 0 else y[k]
            for j, part in enumerate(parts):
                y_ref[k, pl.ds(j * INNER + base, 8), :] = part
        return carry

    lax.fori_loop(0, INNER // 8, butterfly, 0)
    for k in range(HALF):
        yh, yl = split_bf16(y_ref[k])
        wh = wh_ref[k]
        r = jnp.dot(wh, yh, preferred_element_type=jnp.float32)
        r = r + jnp.dot(wh, yl, preferred_element_type=jnp.float32)
        r = r + jnp.dot(wl_ref[k], yh, preferred_element_type=jnp.float32)
        mirror = HALF if k == 0 else RADIX - k
        for q, row in enumerate((k, RADIX + k, mirror, RADIX + mirror)):
            r_ref[pl.ds(row * PAD_R, PEERS), :] = r[q * PEERS : (q + 1) * PEERS]


PIECES = 4


def send_pieces(body, count, buf_ref, o_ref, sem):
    step = count // PIECES
    copies = []
    for piece in range(PIECES):
        lax.fori_loop(piece * step, (piece + 1) * step, body, 0, unroll=4)
        rows = pl.ds(piece * step, step)
        copy = pltpu.make_async_copy(buf_ref.at[rows], o_ref.at[rows], sem.at[piece])
        copy.start()
        copies.append(copy)
    for copy in copies:
        copy.wait()


FFT_SCRATCH = [
    pltpu.VMEM((HALF, 2 * INNER, LANES), jnp.float32),
    pltpu.VMEM((KEPT * PAD_R, LANES), jnp.float32),
]


def mode_rows(r_ref, k1, eight):
    return r_ref[pl.ds(eight * 8 * PAD_R + k1, 8, stride=PAD_R), :]


def fft_a_kernel(x_ref, wh_ref, wl_ref, o_ref, y_ref, r_ref, buf_ref, sem):
    fft_core(x_ref, wh_ref, wl_ref, y_ref, r_ref)

    def peer(k1, carry):
        for eight in range(KEPT // 8):
            buf_ref[k1, eight * 8 : eight * 8 + 8, :] = mode_rows(r_ref, k1, eight)
        return carry

    send_pieces(peer, PEERS, buf_ref, o_ref, sem)


def fft_a(gathered, wh, wl):
    return pl.pallas_call(
        fft_a_kernel,
        in_specs=[VMEM] * 3,
        out_specs=HBM,
        out_shape=pltpu.HBM((PEERS, KEPT, LANES), jnp.float32),
        scratch_shapes=FFT_SCRATCH
        + [pltpu.VMEM((PEERS, KEPT, LANES), jnp.float32), pltpu.SemaphoreType.DMA((PIECES,))],
        compiler_params=PARAMS,
        name="fft_a",
    )(gathered, wh, wl)


def fft_p_kernel(pos_ref, *refs):
    g_refs, (wh_ref, wl_ref), o_refs = refs[:8], refs[8:10], refs[10:18]
    x_ref, y_ref, r_ref = refs[18:]
    x, z, c = pos_ref[0], pos_ref[1], pos_ref[2]
    for dx in range(NX):
        for dc in range(NC):
            start = ((x + NX - dx) % NX) * (NLON // NX) + ((c + dc) % NC) * LON
            for zz in range(NZ):
                row = pl.multiple_of(start + zz * NC * LON, LON)
                x_ref[pl.ds(row, LON), :] = g_refs[dx * NC + dc][zz * LON : (zz + 1) * LON, :]
    fft_core(x_ref, wh_ref, wl_ref, y_ref, r_ref)
    for dz in range(NZ):
        target = (z + dz) % NZ
        for xx in range(NX):
            for cc in range(NC):
                k1 = xx * NZ * NC + target * NC + cc
                for eight in range(KEPT // 8):
                    row = (xx * NC + cc) * KEPT + eight * 8
                    o_refs[dz][row : row + 8, :] = mode_rows(r_ref, k1, eight)


def fft_p(pos, blocks, wh, wl):
    return pl.pallas_call(
        fft_p_kernel,
        in_specs=[SMEM] + [VMEM] * 10,
        out_specs=[VMEM] * NZ,
        out_shape=[f32(NX * NC * KEPT, LANES)] * NZ,
        scratch_shapes=[pltpu.VMEM((NLON, LANES), jnp.float32)] + FFT_SCRATCH,
        compiler_params=PARAMS,
        name="fft_p",
    )(pos, *blocks, wh, wl)


def split_z_kernel(pos_ref, s_ref, *refs):
    o_refs, sem = refs[:NZ], refs[NZ]
    z = pos_ref[1]
    copies = []
    for dz in range(NZ):
        field = pl.multiple_of(((z + dz) % NZ) * 8, 8)
        copies.append(
            pltpu.make_async_copy(s_ref.at[:, pl.ds(field, 8), pl.ds(0, LANES)], o_refs[dz], sem.at[dz])
        )
    for copy in copies:
        copy.start()
    for copy in copies:
        copy.wait()


def split_z(pos, state):
    return pl.pallas_call(
        split_z_kernel,
        in_specs=[SMEM, HBM],
        out_specs=[VMEM] * NZ,
        out_shape=[f32(LON, 8, LANES)] * NZ,
        scratch_shapes=[pltpu.SemaphoreType.DMA((NZ,))],
        compiler_params=PARAMS,
        name="split_z",
    )(pos, state)


def spread_x_kernel(pos_ref, *refs):
    b_refs, o_refs = refs[:NZ], refs[NZ:]
    x, z, c = pos_ref[0], pos_ref[1], pos_ref[2]
    for dx in range(NX):
        for dc in range(NC):
            field = ((x + dx) % NX) * NC + (c + dc) % NC
            for dz in range(NZ):
                row = pl.multiple_of(((z + NZ - dz) % NZ) * LON, LON)
                o_refs[dx * NC + dc][pl.ds(row, LON), :] = b_refs[dz][pl.ds(field, LON, stride=8), :]


def spread_x(pos, blocks):
    return pl.pallas_call(
        spread_x_kernel,
        in_specs=[SMEM] + [VMEM] * NZ,
        out_specs=[VMEM] * (NX * NC),
        out_shape=[f32(NZ * LON, LANES)] * (NX * NC),
        compiler_params=PARAMS,
        name="spread_x",
    )(pos, *blocks)


def spread_out_kernel(pos_ref, *refs):
    h_refs, o_refs = refs[:NZ], refs[NZ:]
    x, z, c = pos_ref[0], pos_ref[1], pos_ref[2]
    for dx in range(NX):
        for dc in range(NC):
            source = pl.multiple_of((((x + dx) % NX) * NC + (c + dc) % NC) * KEPT, KEPT)
            for dz in range(NZ):
                row = pl.multiple_of(((z + NZ - dz) % NZ) * KEPT, KEPT)
                o_refs[dx * NC + dc][pl.ds(row, KEPT), :] = h_refs[dz][pl.ds(source, KEPT), :]


def spread_out(pos, blocks):
    return pl.pallas_call(
        spread_out_kernel,
        in_specs=[SMEM] + [VMEM] * NZ,
        out_specs=[VMEM] * (NX * NC),
        out_shape=[f32(NZ * KEPT, LANES)] * (NX * NC),
        compiler_params=PARAMS,
        name="spread_out",
    )(pos, *blocks)


PAD_F = FIELDS + 8


def relayout_a_kernel(s_ref, o_ref, x_ref, buf_ref, sem, out_sem):
    copies = [
        pltpu.make_async_copy(
            s_ref.at[n, :, pl.ds(LANES, LANES)], x_ref.at[pl.ds(n * PAD_F, FIELDS), :], sem.at[n]
        )
        for n in range(LON)
    ]
    for copy in copies:
        copy.start()
    for copy in copies:
        copy.wait()

    def field(f, carry):
        for eight in range(LON // 8):
            buf_ref[f, eight * 8 : eight * 8 + 8, :] = x_ref[pl.ds(eight * 8 * PAD_F + f, 8, stride=PAD_F), :]
        return carry

    send_pieces(field, FIELDS, buf_ref, o_ref, out_sem)


def relayout_a(state):
    return pl.pallas_call(
        relayout_a_kernel,
        in_specs=[HBM],
        out_specs=HBM,
        out_shape=f32(FIELDS, LON, LANES),
        scratch_shapes=[
            pltpu.VMEM((LON * PAD_F, LANES), jnp.float32),
            pltpu.VMEM((FIELDS, LON, LANES), jnp.float32),
            pltpu.SemaphoreType.DMA((LON,)),
            pltpu.SemaphoreType.DMA((PIECES,)),
        ],
        compiler_params=PARAMS,
        name="relayout_a",
    )(state)


PAD_K = KEPT + 8


def store_half(x_ref, buf_ref, o_ref, sem, lane):
    copies = []
    step = KEPT // PIECES
    for piece in range(PIECES):
        for kept in range(piece * step, (piece + 1) * step):
            for eight in range(FIELDS // 8):
                buf_ref[kept, eight * 8 : eight * 8 + 8, :] = x_ref[pl.ds(eight * 8 * PAD_K + kept, 8, stride=PAD_K), :]
        copy = pltpu.make_async_copy(
            buf_ref.at[pl.ds(piece * step, step)],
            o_ref.at[pl.ds(piece * step, step), :, pl.ds(lane, LANES)],
            sem.at[piece],
        )
        copy.start()
        copies.append(copy)
    for copy in copies:
        copy.wait()


STORE_SCRATCH = [
    pltpu.VMEM((FIELDS * PAD_K, LANES), jnp.float32),
    pltpu.VMEM((KEPT, FIELDS, LANES), jnp.float32),
    pltpu.SemaphoreType.DMA((PIECES,)),
]


def store_p_kernel(pos_ref, prior_ref, *refs):
    del prior_ref
    q_refs, o_ref = refs[:8], refs[8]
    x_ref, buf_ref, sem = refs[9:]
    x, c = pos_ref[0], pos_ref[2]
    for dx in range(NX):
        for dc in range(NC):
            base = ((x + NX - dx) % NX) * NC + (c + dc) % NC
            for zz in range(NZ):
                row = pl.multiple_of((base + zz * NX * NC) * PAD_K, 8)
                x_ref[pl.ds(row, KEPT), :] = q_refs[dx * NC + dc][zz * KEPT : (zz + 1) * KEPT, :]
    store_half(x_ref, buf_ref, o_ref, sem, 0)


def store_p(pos, prior, blocks):
    return pl.pallas_call(
        store_p_kernel,
        in_specs=[SMEM, HBM] + [VMEM] * 8,
        out_specs=HBM,
        out_shape=f32(KEPT, FIELDS, 2 * LANES),
        scratch_shapes=STORE_SCRATCH,
        input_output_aliases={1: 0},
        compiler_params=PARAMS,
        name="store_p",
    )(pos, prior, *blocks)


def store_a_kernel(q_ref, o_ref, x_ref, buf_ref, sem):
    def field(f, carry):
        x_ref[pl.ds(pl.multiple_of(f * PAD_K, 8), KEPT), :] = q_ref[f]
        return carry

    lax.fori_loop(0, FIELDS, field, 0, unroll=8)
    store_half(x_ref, buf_ref, o_ref, sem, LANES)


def store_a(shares):
    return pl.pallas_call(
        store_a_kernel,
        in_specs=[VMEM],
        out_specs=HBM,
        out_shape=f32(KEPT, FIELDS, 2 * LANES),
        scratch_shapes=STORE_SCRATCH,
        compiler_params=PARAMS,
        name="store_a",
    )(shares)


def shifts(dx, dz, dc):
    def at(x, z, c):
        return (x % NX) * NZ * NC + (z % NZ) * NC + c % NC

    return [
        (at(x, z, c), at(x + dx, z + dz, c + dc)) for x in range(NX) for z in range(NZ) for c in range(NC)
    ]


Z_ORDER = (1, 7, 4, 3, 5, 2, 6)


def exchange_z(blocks):
    out = [None] * NZ
    out[0] = blocks[0]
    for dz in Z_ORDER:
        out[dz] = lax.ppermute(blocks[dz], "lon", shifts(0, dz, 0))
    return out


X_ORDER = ((2, 0), (2, 1), (1, 0), (3, 0), (1, 1), (3, 1), (0, 1))


def exchange_xc(blocks):
    out = [None] * (NX * NC)
    out[0] = blocks[0]
    for dx, dc in X_ORDER:
        out[dx * NC + dc] = lax.ppermute(blocks[dx * NC + dc], "lon", shifts(dx, 0, dc))
    return out


def local(state):
    device = lax.axis_index("lon")
    pos = jnp.stack([device // (NZ * NC), (device // NC) % NZ, device % NC]).astype(jnp.int32)
    wh, wl = twiddle_matrices(1.0 / math.sqrt(NLON))
    pieces = split_z(pos, pltpu.with_memory_space_constraint(state, pltpu.HBM))
    pieces = exchange_z(pieces)
    sent = relayout_a(pltpu.with_memory_space_constraint(state, pltpu.HBM))
    gathered = lax.all_to_all(sent, "lon", split_axis=0, concat_axis=0, tiled=True)
    pieces = spread_x(pos, [b.reshape(LON * 8, LANES) for b in pieces])
    pieces = exchange_xc(pieces)
    pieces = fft_p(pos, pieces, wh, wl)
    pieces = exchange_z(pieces)
    spectrum = fft_a(gathered.reshape(NLON, LANES), wh, wl)
    shares = lax.all_to_all(spectrum, "lon", split_axis=0, concat_axis=0, tiled=True)
    pieces = spread_out(pos, pieces)
    pieces = exchange_xc(pieces)
    out = store_a(shares)
    out = store_p(pos, out, pieces)
    return out.reshape(2, RADIX, FIELDS, 2 * LANES)


def solution(mesh):
    return jax.shard_map(
        local,
        mesh=mesh,
        in_specs=(P("lon", None, "lat"),),
        out_specs=P(None, "lon", None, "lat"),
        check_vma=False,
    )
```

```python
import math

import jax
import jax.numpy as jnp
from jax import lax
from jax.experimental import pallas as pl
from jax.experimental.pallas import tpu as pltpu
from jax.sharding import PartitionSpec as P


NLON = 2048
RADIX = 16
INNER = NLON // RADIX
PEERS = 64
HALF = RADIX // 2
NX, NZ, NC = 4, 8, 2
LON = 32
KEPT = 2 * RADIX
FIELDS = 64
LANES = 128
VMEM = pl.BlockSpec(memory_space=pltpu.VMEM)
HBM = pl.BlockSpec(memory_space=pltpu.HBM)
SMEM = pl.BlockSpec(memory_space=pltpu.SMEM)
PARAMS = pltpu.CompilerParams(vmem_limit_bytes=16 * 1024 * 1024)


def f32(*shape):
    return jax.ShapeDtypeStruct(shape, jnp.float32)


def split_bf16(v):
    high = v.astype(jnp.bfloat16)
    low = (v - high.astype(jnp.float32)).astype(jnp.bfloat16)
    return high, low


def phase(rows, cols):
    turn = (rows * cols) % NLON
    turn = jnp.where(turn >= NLON // 2, turn - NLON, turn)
    return turn.astype(jnp.float32) * (2.0 * math.pi / NLON)


def twiddle_matrices(scale):
    shape = (HALF, 2, PEERS, INNER)
    pair = lax.broadcasted_iota(jnp.int32, shape, 0)
    mirror = lax.broadcasted_iota(jnp.int32, shape, 1)
    outer = lax.broadcasted_iota(jnp.int32, shape, 2)
    inner = lax.broadcasted_iota(jnp.int32, shape, 3)
    first = jnp.where(mirror == 0, pair, jnp.where(pair == 0, HALF, RADIX - pair))
    angle = phase(inner, first + RADIX * outer)
    c = jnp.cos(angle) * scale
    s = jnp.sin(angle) * scale
    real_only = pair == 0
    zero = jnp.zeros_like(c)
    plain = mirror == 0
    re_a = jnp.where(real_only, jnp.where(plain, c, zero), c)
    im_a = jnp.where(real_only, jnp.where(plain, -s, zero), -s)
    re_b = jnp.where(real_only, jnp.where(plain, zero, c), jnp.where(plain, s, -s))
    im_b = jnp.where(real_only, jnp.where(plain, zero, -s), jnp.where(plain, c, -c))
    re = jnp.concatenate([re_a, re_b], axis=-1)
    im = jnp.concatenate([im_a, im_b], axis=-1)
    full = jnp.stack([re, im], axis=2)
    full = full.reshape(HALF, 4 * PEERS, 2 * INNER)
    high = lax.reduce_precision(full, 8, 7)
    return high.astype(jnp.bfloat16), (full - high).astype(jnp.bfloat16)


def fft_real16(x):
    def fft_complex8(z):
        def fft4(a):
            (ar, ai), (br, bi), (cr, ci), (dr, di) = a
            sr, si = ar + cr, ai + ci
            tr, ti = ar - cr, ai - ci
            ur, ui = br + dr, bi + di
            vr, vi = br - dr, bi - di
            return [(sr + ur, si + ui), (tr + vi, ti - vr), (sr - ur, si - ui), (tr - vi, ti + vr)]

        even = fft4(z[0::2])
        odd = fft4(z[1::2])
        h = math.sqrt(0.5)
        out = [None] * 8
        for k in range(4):
            er, ei = even[k]
            pr, pi = odd[k]
            if k == 1:
                pr, pi = (pr + pi) * h, (pi - pr) * h
            elif k == 2:
                pr, pi = pi, -pr
            elif k == 3:
                pr, pi = (pi - pr) * h, -(pr + pi) * h
            out[k] = (er + pr, ei + pi)
            out[k + 4] = (er - pr, ei - pi)
        return out

    z = fft_complex8([(x[2 * i], x[2 * i + 1]) for i in range(8)])
    out = [(z[0][0] + z[0][1], None)]
    for k in range(1, 8):
        zr, zi = z[k]
        wr, wi = z[8 - k]
        er, ei = (zr + wr) * 0.5, (zi - wi) * 0.5
        pr, pi = (zi + wi) * 0.5, (wr - zr) * 0.5
        c, s = math.cos(2 * math.pi * k / 16), math.sin(2 * math.pi * k / 16)
        out.append((er + c * pr + s * pi, ei + c * pi - s * pr))
    out.append((z[0][0] - z[0][1], None))
    return out


PAD_R = PEERS + 8


def natural_row(n2, base):
    return n2 * INNER + base


def grouped_row(n2, base):
    return ((n2 % 4) * 4 + base // LON) * INNER + (n2 // 4) * LON + base % LON


def fft_core(x_ref, wh_ref, wl_ref, y_ref, r_ref, row_of):
    def butterfly(i, carry):
        base = pl.multiple_of(i * 8, 8)
        x = [x_ref[pl.ds(pl.multiple_of(row_of(n2, base), 8), 8), :] for n2 in range(RADIX)]
        y = fft_real16(x)
        for k in range(HALF):
            parts = (y[0][0], y[HALF][0]) if k == 0 else y[k]
            for j, part in enumerate(parts):
                y_ref[k, pl.ds(j * INNER + base, 8), :] = part
        return carry

    lax.fori_loop(0, INNER // 8, butterfly, 0)
    for k in range(HALF):
        yh, yl = split_bf16(y_ref[k])
        wh = wh_ref[k]
        r = jnp.dot(wh, yh, preferred_element_type=jnp.float32)
        r = r + jnp.dot(wh, yl, preferred_element_type=jnp.float32)
        r = r + jnp.dot(wl_ref[k], yh, preferred_element_type=jnp.float32)
        mirror = HALF if k == 0 else RADIX - k
        for q, row in enumerate((k, RADIX + k, mirror, RADIX + mirror)):
            r_ref[pl.ds(row * PAD_R, PEERS), :] = r[q * PEERS : (q + 1) * PEERS]


PIECES = 4


def send_pieces(body, count, buf_ref, o_ref, sem):
    step = count // PIECES
    copies = []
    for piece in range(PIECES):
        lax.fori_loop(piece * step, (piece + 1) * step, body, 0, unroll=4)
        rows = pl.ds(piece * step, step)
        copy = pltpu.make_async_copy(buf_ref.at[rows], o_ref.at[rows], sem.at[piece])
        copy.start()
        copies.append(copy)
    for copy in copies:
        copy.wait()


FFT_SCRATCH = [
    pltpu.VMEM((HALF, 2 * INNER, LANES), jnp.float32),
    pltpu.VMEM((KEPT * PAD_R, LANES), jnp.float32),
]


def mode_rows(r_ref, k1, eight):
    return r_ref[pl.ds(eight * 8 * PAD_R + k1, 8, stride=PAD_R), :]


def fft_a_kernel(x_ref, wh_ref, wl_ref, o_ref, y_ref, r_ref, buf_ref, sem):
    fft_core(x_ref, wh_ref, wl_ref, y_ref, r_ref, grouped_row)

    def peer(k1, carry):
        for eight in range(KEPT // 8):
            buf_ref[k1, eight * 8 : eight * 8 + 8, :] = mode_rows(r_ref, k1, eight)
        return carry

    send_pieces(peer, PEERS, buf_ref, o_ref, sem)


def fft_a(gathered, wh, wl):
    return pl.pallas_call(
        fft_a_kernel,
        in_specs=[VMEM] * 3,
        out_specs=HBM,
        out_shape=pltpu.HBM((PEERS, KEPT, LANES), jnp.float32),
        scratch_shapes=FFT_SCRATCH
        + [pltpu.VMEM((PEERS, KEPT, LANES), jnp.float32), pltpu.SemaphoreType.DMA((PIECES,))],
        compiler_params=PARAMS,
        name="fft_a",
    )(gathered, wh, wl)


def fft_p_kernel(pos_ref, *refs):
    g_refs, (wh_ref, wl_ref), o_refs = refs[:8], refs[8:10], refs[10:18]
    x_ref, y_ref, r_ref = refs[18:]
    x, z, c = pos_ref[0], pos_ref[1], pos_ref[2]
    for dx in range(NX):
        for dc in range(NC):
            start = ((x + NX - dx) % NX) * (NLON // NX) + ((c + dc) % NC) * LON
            for zz in range(NZ):
                row = pl.multiple_of(start + zz * NC * LON, LON)
                x_ref[pl.ds(row, LON), :] = g_refs[dx * NC + dc][zz * LON : (zz + 1) * LON, :]
    fft_core(x_ref, wh_ref, wl_ref, y_ref, r_ref, natural_row)
    for dz in range(NZ):
        target = (z + dz) % NZ
        for xx in range(NX):
            for cc in range(NC):
                k1 = xx * NZ * NC + target * NC + cc
                for eight in range(KEPT // 8):
                    row = (xx * NC + cc) * KEPT + eight * 8
                    o_refs[dz][row : row + 8, :] = mode_rows(r_ref, k1, eight)


def fft_p(pos, blocks, wh, wl):
    return pl.pallas_call(
        fft_p_kernel,
        in_specs=[SMEM] + [VMEM] * 10,
        out_specs=[VMEM] * NZ,
        out_shape=[f32(NX * NC * KEPT, LANES)] * NZ,
        scratch_shapes=[pltpu.VMEM((NLON, LANES), jnp.float32)] + FFT_SCRATCH,
        compiler_params=PARAMS,
        name="fft_p",
    )(pos, *blocks, wh, wl)


def split_z_kernel(pos_ref, s_ref, *refs):
    o_refs, sem = refs[:NZ], refs[NZ]
    z = pos_ref[1]
    copies = []
    for dz in range(NZ):
        field = pl.multiple_of(((z + dz) % NZ) * 8, 8)
        copies.append(
            pltpu.make_async_copy(s_ref.at[:, pl.ds(field, 8), pl.ds(0, LANES)], o_refs[dz], sem.at[dz])
        )
    for copy in copies:
        copy.start()
    for copy in copies:
        copy.wait()


def split_z(pos, state):
    return pl.pallas_call(
        split_z_kernel,
        in_specs=[SMEM, HBM],
        out_specs=[VMEM] * NZ,
        out_shape=[f32(LON, 8, LANES)] * NZ,
        scratch_shapes=[pltpu.SemaphoreType.DMA((NZ,))],
        compiler_params=PARAMS,
        name="split_z",
    )(pos, state)


def spread_x_kernel(pos_ref, *refs):
    b_refs, o_refs = refs[:NZ], refs[NZ:]
    x, z, c = pos_ref[0], pos_ref[1], pos_ref[2]
    for dx in range(NX):
        for dc in range(NC):
            field = ((x + dx) % NX) * NC + (c + dc) % NC
            for dz in range(NZ):
                row = pl.multiple_of(((z + NZ - dz) % NZ) * LON, LON)
                o_refs[dx * NC + dc][pl.ds(row, LON), :] = b_refs[dz][pl.ds(field, LON, stride=8), :]


def spread_x(pos, blocks):
    return pl.pallas_call(
        spread_x_kernel,
        in_specs=[SMEM] + [VMEM] * NZ,
        out_specs=[VMEM] * (NX * NC),
        out_shape=[f32(NZ * LON, LANES)] * (NX * NC),
        compiler_params=PARAMS,
        name="spread_x",
    )(pos, *blocks)


def spread_out_kernel(pos_ref, *refs):
    h_refs, o_refs = refs[:NZ], refs[NZ:]
    x, z, c = pos_ref[0], pos_ref[1], pos_ref[2]
    for dx in range(NX):
        for dc in range(NC):
            source = pl.multiple_of((((x + dx) % NX) * NC + (c + dc) % NC) * KEPT, KEPT)
            for dz in range(NZ):
                row = pl.multiple_of(((z + NZ - dz) % NZ) * KEPT, KEPT)
                o_refs[dx * NC + dc][pl.ds(row, KEPT), :] = h_refs[dz][pl.ds(source, KEPT), :]


def spread_out(pos, blocks):
    return pl.pallas_call(
        spread_out_kernel,
        in_specs=[SMEM] + [VMEM] * NZ,
        out_specs=[VMEM] * (NX * NC),
        out_shape=[f32(NZ * KEPT, LANES)] * (NX * NC),
        compiler_params=PARAMS,
        name="spread_out",
    )(pos, *blocks)


GROUP = NZ * NC


def split_a_kernel(pos_ref, s_ref, *refs):
    o_refs, sem = refs[:NX], refs[NX]
    x = pos_ref[0]
    copies = []
    for dx in range(NX):
        field = pl.multiple_of(((x + dx) % NX) * GROUP, GROUP)
        copies.append(
            pltpu.make_async_copy(s_ref.at[:, pl.ds(field, GROUP), pl.ds(LANES, LANES)], o_refs[dx], sem.at[dx])
        )
    for copy in copies:
        copy.start()
    for copy in copies:
        copy.wait()


def split_a(pos, state):
    return pl.pallas_call(
        split_a_kernel,
        in_specs=[SMEM, HBM],
        out_specs=[VMEM] * NX,
        out_shape=[f32(LON, GROUP, LANES)] * NX,
        scratch_shapes=[pltpu.SemaphoreType.DMA((NX,))],
        compiler_params=PARAMS,
        name="split_a",
    )(pos, state)


def spread_a_kernel(pos_ref, *refs):
    b_refs, o_ref, buf_ref, sem = refs[:NX], refs[NX], refs[NX + 1], refs[NX + 2]
    x = pos_ref[0]

    def field(f, carry):
        for dx in range(NX):
            row = pl.multiple_of(((x + NX - dx) % NX) * LON, LON)
            buf_ref[f, pl.ds(row, LON), :] = b_refs[dx][pl.ds(f, LON, stride=GROUP), :]
        return carry

    send_pieces(field, GROUP, buf_ref, o_ref, sem)


def spread_a(pos, blocks):
    return pl.pallas_call(
        spread_a_kernel,
        in_specs=[SMEM] + [VMEM] * NX,
        out_specs=HBM,
        out_shape=pltpu.HBM((GROUP, NX * LON, LANES), jnp.float32),
        scratch_shapes=[
            pltpu.VMEM((GROUP, NX * LON, LANES), jnp.float32),
            pltpu.SemaphoreType.DMA((PIECES,)),
        ],
        compiler_params=PARAMS,
        name="spread_a",
    )(pos, *blocks)


PAD_K = KEPT + 8


def store_half(x_ref, buf_ref, o_ref, sem, lane):
    copies = []
    step = KEPT // PIECES
    for piece in range(PIECES):
        for kept in range(piece * step, (piece + 1) * step):
            for eight in range(FIELDS // 8):
                buf_ref[kept, eight * 8 : eight * 8 + 8, :] = x_ref[pl.ds(eight * 8 * PAD_K + kept, 8, stride=PAD_K), :]
        copy = pltpu.make_async_copy(
            buf_ref.at[pl.ds(piece * step, step)],
            o_ref.at[pl.ds(piece * step, step), :, pl.ds(lane, LANES)],
            sem.at[piece],
        )
        copy.start()
        copies.append(copy)
    for copy in copies:
        copy.wait()


STORE_SCRATCH = [
    pltpu.VMEM((FIELDS * PAD_K, LANES), jnp.float32),
    pltpu.VMEM((KEPT, FIELDS, LANES), jnp.float32),
    pltpu.SemaphoreType.DMA((PIECES,)),
]


def store_p_kernel(pos_ref, prior_ref, *refs):
    del prior_ref
    q_refs, o_ref = refs[:8], refs[8]
    x_ref, buf_ref, sem = refs[9:]
    x, c = pos_ref[0], pos_ref[2]
    for dx in range(NX):
        for dc in range(NC):
            base = ((x + NX - dx) % NX) * NC + (c + dc) % NC
            for zz in range(NZ):
                row = pl.multiple_of((base + zz * NX * NC) * PAD_K, 8)
                x_ref[pl.ds(row, KEPT), :] = q_refs[dx * NC + dc][zz * KEPT : (zz + 1) * KEPT, :]
    store_half(x_ref, buf_ref, o_ref, sem, 0)


def store_p(pos, prior, blocks):
    return pl.pallas_call(
        store_p_kernel,
        in_specs=[SMEM, HBM] + [VMEM] * 8,
        out_specs=HBM,
        out_shape=f32(KEPT, FIELDS, 2 * LANES),
        scratch_shapes=STORE_SCRATCH,
        input_output_aliases={1: 0},
        compiler_params=PARAMS,
        name="store_p",
    )(pos, prior, *blocks)


def store_a_kernel(q_ref, o_ref, x_ref, buf_ref, sem):
    def field(f, carry):
        x_ref[pl.ds(pl.multiple_of(f * PAD_K, 8), KEPT), :] = q_ref[f]
        return carry

    lax.fori_loop(0, FIELDS, field, 0, unroll=8)
    store_half(x_ref, buf_ref, o_ref, sem, LANES)


def store_a(shares):
    return pl.pallas_call(
        store_a_kernel,
        in_specs=[VMEM],
        out_specs=HBM,
        out_shape=f32(KEPT, FIELDS, 2 * LANES),
        scratch_shapes=STORE_SCRATCH,
        compiler_params=PARAMS,
        name="store_a",
    )(shares)


def shifts(dx, dz, dc):
    def at(x, z, c):
        return (x % NX) * NZ * NC + (z % NZ) * NC + c % NC

    return [
        (at(x, z, c), at(x + dx, z + dz, c + dc)) for x in range(NX) for z in range(NZ) for c in range(NC)
    ]


Z_ORDER = (1, 7, 4, 3, 5, 2, 6)


def exchange_z(blocks):
    out = [None] * NZ
    out[0] = blocks[0]
    for dz in Z_ORDER:
        out[dz] = lax.ppermute(blocks[dz], "lon", shifts(0, dz, 0))
    return out


AX_ORDER = (2, 1, 3)
GROUPS = [[x * GROUP + g for g in range(GROUP)] for x in range(NX)]


def exchange_x(blocks):
    out = [None] * NX
    out[0] = blocks[0]
    for dx in AX_ORDER:
        out[dx] = lax.ppermute(blocks[dx], "lon", shifts(dx, 0, 0))
    return out


X_ORDER = ((2, 0), (2, 1), (1, 0), (3, 0), (1, 1), (3, 1), (0, 1))


def exchange_xc(blocks):
    out = [None] * (NX * NC)
    out[0] = blocks[0]
    for dx, dc in X_ORDER:
        out[dx * NC + dc] = lax.ppermute(blocks[dx * NC + dc], "lon", shifts(dx, 0, dc))
    return out


def local(state):
    device = lax.axis_index("lon")
    pos = jnp.stack([device // (NZ * NC), (device // NC) % NZ, device % NC]).astype(jnp.int32)
    wh, wl = twiddle_matrices(1.0 / math.sqrt(NLON))
    pieces = split_z(pos, pltpu.with_memory_space_constraint(state, pltpu.HBM))
    pieces = exchange_z(pieces)
    parts = split_a(pos, pltpu.with_memory_space_constraint(state, pltpu.HBM))
    parts = exchange_x(parts)
    sent = spread_a(pos, [b.reshape(LON * GROUP, LANES) for b in parts])
    gathered = lax.all_to_all(
        sent, "lon", split_axis=0, concat_axis=0, axis_index_groups=GROUPS, tiled=True
    )
    pieces = spread_x(pos, [b.reshape(LON * 8, LANES) for b in pieces])
    pieces = exchange_xc(pieces)
    pieces = fft_p(pos, pieces, wh, wl)
    pieces = exchange_z(pieces)
    spectrum = fft_a(gathered.reshape(NLON, LANES), wh, wl)
    shares = lax.all_to_all(spectrum, "lon", split_axis=0, concat_axis=0, tiled=True)
    pieces = spread_out(pos, pieces)
    pieces = exchange_xc(pieces)
    out = store_a(shares)
    out = store_p(pos, out, pieces)
    return out.reshape(2, RADIX, FIELDS, 2 * LANES)


def solution(mesh):
    return jax.shard_map(
        local,
        mesh=mesh,
        in_specs=(P("lon", None, "lat"),),
        out_specs=P(None, "lon", None, "lat"),
        check_vma=False,
    )
```

```python
import math

import jax
import jax.numpy as jnp
from jax import lax
from jax.experimental import pallas as pl
from jax.experimental.pallas import tpu as pltpu
from jax.sharding import PartitionSpec as P


NLON = 2048
RADIX = 16
INNER = NLON // RADIX
PEERS = 64
HALF = RADIX // 2
NX, NZ, NC = 4, 8, 2
LON = 32
KEPT = 2 * RADIX
FIELDS = 64
LANES = 128
VMEM = pl.BlockSpec(memory_space=pltpu.VMEM)
HBM = pl.BlockSpec(memory_space=pltpu.HBM)
SMEM = pl.BlockSpec(memory_space=pltpu.SMEM)
PARAMS = pltpu.CompilerParams(vmem_limit_bytes=16 * 1024 * 1024)


def f32(*shape):
    return jax.ShapeDtypeStruct(shape, jnp.float32)


def vmem(*shape):
    return pltpu.VMEM(shape, jnp.float32)


def split_bf16(v):
    high = v.astype(jnp.bfloat16)
    low = (v - high.astype(jnp.float32)).astype(jnp.bfloat16)
    return high, low


def phase(rows, cols):
    turn = (rows * cols) % NLON
    turn = jnp.where(turn >= NLON // 2, turn - NLON, turn)
    return turn.astype(jnp.float32) * (2.0 * math.pi / NLON)


def twiddle_matrices(scale):
    shape = (HALF, 2, PEERS, INNER)
    pair = lax.broadcasted_iota(jnp.int32, shape, 0)
    mirror = lax.broadcasted_iota(jnp.int32, shape, 1)
    outer = lax.broadcasted_iota(jnp.int32, shape, 2)
    inner = lax.broadcasted_iota(jnp.int32, shape, 3)
    first = jnp.where(mirror == 0, pair, jnp.where(pair == 0, HALF, RADIX - pair))
    angle = phase(inner, first + RADIX * outer)
    c = jnp.cos(angle) * scale
    s = jnp.sin(angle) * scale
    real_only = pair == 0
    zero = jnp.zeros_like(c)
    plain = mirror == 0
    re_a = jnp.where(real_only, jnp.where(plain, c, zero), c)
    im_a = jnp.where(real_only, jnp.where(plain, -s, zero), -s)
    re_b = jnp.where(real_only, jnp.where(plain, zero, c), jnp.where(plain, s, -s))
    im_b = jnp.where(real_only, jnp.where(plain, zero, -s), jnp.where(plain, c, -c))
    re = jnp.concatenate([re_a, re_b], axis=-1)
    im = jnp.concatenate([im_a, im_b], axis=-1)
    full = jnp.stack([re, im], axis=2)
    full = full.reshape(HALF, 4 * PEERS, 2 * INNER)
    high = lax.reduce_precision(full, 8, 7)
    high, low = high.astype(jnp.bfloat16), (full - high).astype(jnp.bfloat16)
    return jnp.concatenate([high, low], axis=-1)


def fft_real16(x):
    def fft_complex8(z):
        def fft4(a):
            (ar, ai), (br, bi), (cr, ci), (dr, di) = a
            sr, si = ar + cr, ai + ci
            tr, ti = ar - cr, ai - ci
            ur, ui = br + dr, bi + di
            vr, vi = br - dr, bi - di
            return [(sr + ur, si + ui), (tr + vi, ti - vr), (sr - ur, si - ui), (tr - vi, ti + vr)]

        even = fft4(z[0::2])
        odd = fft4(z[1::2])
        h = math.sqrt(0.5)
        out = [None] * 8
        for k in range(4):
            er, ei = even[k]
            pr, pi = odd[k]
            if k == 1:
                pr, pi = (pr + pi) * h, (pi - pr) * h
            elif k == 2:
                pr, pi = pi, -pr
            elif k == 3:
                pr, pi = (pi - pr) * h, -(pr + pi) * h
            out[k] = (er + pr, ei + pi)
            out[k + 4] = (er - pr, ei - pi)
        return out

    z = fft_complex8([(x[2 * i], x[2 * i + 1]) for i in range(8)])
    out = [(z[0][0] + z[0][1], None)]
    for k in range(1, 8):
        zr, zi = z[k]
        wr, wi = z[8 - k]
        er, ei = (zr + wr) * 0.5, (zi - wi) * 0.5
        pr, pi = (zi + wi) * 0.5, (wr - zr) * 0.5
        c, s = math.cos(2 * math.pi * k / 16), math.sin(2 * math.pi * k / 16)
        out.append((er + c * pr + s * pi, ei + c * pi - s * pr))
    out.append((z[0][0] - z[0][1], None))
    return out


PAD_R = PEERS + 8


def natural_row(n2, base):
    return n2 * INNER + base


def grouped_row(n2, base):
    return ((n2 % 4) * 4 + base // LON) * INNER + (n2 // 4) * LON + base % LON


def fft_core(x_ref, w_ref, y_ref, r_ref, row_of, loads):
    def butterfly(i, carry):
        base = pl.multiple_of(i * 8, 8)
        x = [x_ref[pl.ds(pl.multiple_of(row_of(n2, base), 8), 8), :] for n2 in range(RADIX)]
        y = fft_real16(x)
        for k in range(HALF):
            parts = (y[0][0], y[HALF][0]) if k == 0 else y[k]
            for j, part in enumerate(parts):
                y_ref[k, pl.ds(j * INNER + base, 8), :] = part
        return carry

    lax.fori_loop(0, INNER // 8, butterfly, 0)
    for k in range(HALF):
        yh, yl = split_bf16(y_ref[k])
        loads[k].wait()
        high, both = w_ref[k, :, : 2 * INNER], w_ref[k]
        r = jnp.dot(
            jnp.concatenate([high, both], axis=1),
            jnp.concatenate([yl, yh, yh], axis=0),
            preferred_element_type=jnp.float32,
        )
        mirror = HALF if k == 0 else RADIX - k
        for q, row in enumerate((k, RADIX + k, mirror, RADIX + mirror)):
            r_ref[pl.ds(row * PAD_R, PEERS), :] = r[q * PEERS : (q + 1) * PEERS]


PIECES = 4


def send_pieces(body, count, buf_ref, o_ref, sem):
    step = count // PIECES
    copies = []
    for piece in range(PIECES):
        lax.fori_loop(piece * step, (piece + 1) * step, body, 0, unroll=4)
        rows = pl.ds(piece * step, step)
        copy = pltpu.make_async_copy(buf_ref.at[rows], o_ref.at[rows], sem.at[piece])
        copy.start()
        copies.append(copy)
    for copy in copies:
        copy.wait()


def load_matrices(w_hbm, w_ref, sem):
    loads = [pltpu.make_async_copy(w_hbm.at[k], w_ref.at[k], sem.at[k]) for k in range(HALF)]
    for load in loads:
        load.start()
    return loads


FFT_SCRATCH = [
    pltpu.VMEM((HALF, 4 * PEERS, 4 * INNER), jnp.bfloat16),
    pltpu.SemaphoreType.DMA((HALF,)),
    pltpu.VMEM((HALF, 2 * INNER, LANES), jnp.float32),
    pltpu.VMEM((KEPT * PAD_R, LANES), jnp.float32),
]


def mode_rows(r_ref, k1, eight):
    return r_ref[pl.ds(eight * 8 * PAD_R + k1, 8, stride=PAD_R), :]


def fft_a_kernel(x_ref, w_hbm, o_ref, w_ref, w_sem, y_ref, r_ref, buf_ref, sem):
    loads = load_matrices(w_hbm, w_ref, w_sem)
    fft_core(x_ref, w_ref, y_ref, r_ref, grouped_row, loads)

    def peer(k1, carry):
        for eight in range(KEPT // 8):
            buf_ref[k1, eight * 8 : eight * 8 + 8, :] = mode_rows(r_ref, k1, eight)
        return carry

    send_pieces(peer, PEERS, buf_ref, o_ref, sem)


def fft_a(gathered, w):
    return pl.pallas_call(
        fft_a_kernel,
        in_specs=[VMEM, HBM],
        out_specs=HBM,
        out_shape=pltpu.HBM((PEERS, KEPT, LANES), jnp.float32),
        scratch_shapes=FFT_SCRATCH
        + [pltpu.VMEM((PEERS, KEPT, LANES), jnp.float32), pltpu.SemaphoreType.DMA((PIECES,))],
        compiler_params=PARAMS,
        name="fft_a",
    )(gathered, pltpu.with_memory_space_constraint(w, pltpu.HBM))


def fft_p_kernel(pos_ref, *refs):
    g_refs, w_hbm, o_refs = refs[:8], refs[8], refs[9:17]
    x_ref, w_ref, w_sem, y_ref, r_ref = refs[17:]
    loads = load_matrices(w_hbm, w_ref, w_sem)
    x, z, c = pos_ref[0], pos_ref[1], pos_ref[2]
    for dx in range(NX):
        for dc in range(NC):
            start = ((x + NX - dx) % NX) * (NLON // NX) + ((c + dc) % NC) * LON
            for zz in range(NZ):
                row = pl.multiple_of(start + zz * NC * LON, LON)
                x_ref[pl.ds(row, LON), :] = g_refs[dx * NC + dc][zz * LON : (zz + 1) * LON, :]
    fft_core(x_ref, w_ref, y_ref, r_ref, natural_row, loads)
    for dz in range(NZ):
        target = (z + dz) % NZ
        for xx in range(NX):
            for cc in range(NC):
                k1 = xx * NZ * NC + target * NC + cc
                for eight in range(KEPT // 8):
                    row = (xx * NC + cc) * KEPT + eight * 8
                    o_refs[dz][row : row + 8, :] = mode_rows(r_ref, k1, eight)


def fft_p(pos, blocks, w):
    return pl.pallas_call(
        fft_p_kernel,
        in_specs=[SMEM] + [VMEM] * 8 + [HBM],
        out_specs=[VMEM] * NZ,
        out_shape=[vmem(NX * NC * KEPT, LANES)] * NZ,
        scratch_shapes=[pltpu.VMEM((NLON, LANES), jnp.float32)] + FFT_SCRATCH,
        compiler_params=PARAMS,
        name="fft_p",
    )(pos, *blocks, pltpu.with_memory_space_constraint(w, pltpu.HBM))


GROUP = NZ * NC


def split_kernel(pos_ref, s_ref, *refs):
    o_refs, sem = refs[: NZ + NX], refs[NZ + NX]
    x, z = pos_ref[0], pos_ref[1]
    copies = []
    for dz in range(NZ):
        field = pl.multiple_of(((z + dz) % NZ) * 8, 8)
        source = s_ref.at[:, pl.ds(field, 8), pl.ds(0, LANES)]
        copies.append(pltpu.make_async_copy(source, o_refs[dz], sem.at[dz]))
    for dx in range(NX):
        field = pl.multiple_of(((x + dx) % NX) * GROUP, GROUP)
        source = s_ref.at[:, pl.ds(field, GROUP), pl.ds(LANES, LANES)]
        copies.append(pltpu.make_async_copy(source, o_refs[NZ + dx], sem.at[NZ + dx]))
    for copy in copies:
        copy.start()
    for copy in copies:
        copy.wait()


def split(pos, state):
    out = pl.pallas_call(
        split_kernel,
        in_specs=[SMEM, HBM],
        out_specs=[VMEM] * (NZ + NX),
        out_shape=[vmem(LON, 8, LANES)] * NZ + [vmem(LON, GROUP, LANES)] * NX,
        scratch_shapes=[pltpu.SemaphoreType.DMA((NZ + NX,))],
        compiler_params=PARAMS,
        name="split",
    )(pos, pltpu.with_memory_space_constraint(state, pltpu.HBM))
    return out[:NZ], out[NZ:]


def spread_x_kernel(pos_ref, *refs):
    b_refs, o_refs = refs[:NZ], refs[NZ:]
    x, z, c = pos_ref[0], pos_ref[1], pos_ref[2]
    for dx in range(NX):
        for dc in range(NC):
            field = ((x + dx) % NX) * NC + (c + dc) % NC
            for dz in range(NZ):
                row = pl.multiple_of(((z + NZ - dz) % NZ) * LON, LON)
                o_refs[dx * NC + dc][pl.ds(row, LON), :] = b_refs[dz][pl.ds(field, LON, stride=8), :]


def spread_x(pos, blocks):
    return pl.pallas_call(
        spread_x_kernel,
        in_specs=[SMEM] + [VMEM] * NZ,
        out_specs=[VMEM] * (NX * NC),
        out_shape=[vmem(NZ * LON, LANES)] * (NX * NC),
        compiler_params=PARAMS,
        name="spread_x",
    )(pos, *blocks)


def spread_out_kernel(pos_ref, *refs):
    h_refs, o_refs = refs[:NZ], refs[NZ:]
    x, z, c = pos_ref[0], pos_ref[1], pos_ref[2]
    for dx in range(NX):
        for dc in range(NC):
            source = pl.multiple_of((((x + dx) % NX) * NC + (c + dc) % NC) * KEPT, KEPT)
            for dz in range(NZ):
                row = pl.multiple_of(((z + NZ - dz) % NZ) * KEPT, KEPT)
                o_refs[dx * NC + dc][pl.ds(row, KEPT), :] = h_refs[dz][pl.ds(source, KEPT), :]


def spread_out(pos, blocks):
    return pl.pallas_call(
        spread_out_kernel,
        in_specs=[SMEM] + [VMEM] * NZ,
        out_specs=[VMEM] * (NX * NC),
        out_shape=[vmem(NZ * KEPT, LANES)] * (NX * NC),
        compiler_params=PARAMS,
        name="spread_out",
    )(pos, *blocks)


def spread_a_kernel(pos_ref, *refs):
    b_refs, o_ref, buf_ref, sem = refs[:NX], refs[NX], refs[NX + 1], refs[NX + 2]
    x = pos_ref[0]

    def field(f, carry):
        for dx in range(NX):
            row = pl.multiple_of(((x + NX - dx) % NX) * LON, LON)
            buf_ref[f, pl.ds(row, LON), :] = b_refs[dx][pl.ds(f, LON, stride=GROUP), :]
        return carry

    send_pieces(field, GROUP, buf_ref, o_ref, sem)


def spread_a(pos, blocks):
    return pl.pallas_call(
        spread_a_kernel,
        in_specs=[SMEM] + [VMEM] * NX,
        out_specs=HBM,
        out_shape=pltpu.HBM((GROUP, NX * LON, LANES), jnp.float32),
        scratch_shapes=[
            pltpu.VMEM((GROUP, NX * LON, LANES), jnp.float32),
            pltpu.SemaphoreType.DMA((PIECES,)),
        ],
        compiler_params=PARAMS,
        name="spread_a",
    )(pos, *blocks)


PAD_K = KEPT + 8


def store_half(x_ref, buf_ref, o_ref, sem, lane):
    copies = []
    step = KEPT // PIECES
    for piece in range(PIECES):
        for kept in range(piece * step, (piece + 1) * step):
            for eight in range(FIELDS // 8):
                buf_ref[kept, eight * 8 : eight * 8 + 8, :] = x_ref[pl.ds(eight * 8 * PAD_K + kept, 8, stride=PAD_K), :]
        copy = pltpu.make_async_copy(
            buf_ref.at[pl.ds(piece * step, step)],
            o_ref.at[pl.ds(piece * step, step), :, pl.ds(lane, LANES)],
            sem.at[piece],
        )
        copy.start()
        copies.append(copy)
    for copy in copies:
        copy.wait()


STORE_SCRATCH = [
    pltpu.VMEM((FIELDS * PAD_K, LANES), jnp.float32),
    pltpu.VMEM((KEPT, FIELDS, LANES), jnp.float32),
    pltpu.SemaphoreType.DMA((PIECES,)),
]


def store_p_kernel(pos_ref, prior_ref, *refs):
    del prior_ref
    q_refs, o_ref = refs[:8], refs[8]
    x_ref, buf_ref, sem = refs[9:]
    x, c = pos_ref[0], pos_ref[2]
    for dx in range(NX):
        for dc in range(NC):
            base = ((x + NX - dx) % NX) * NC + (c + dc) % NC
            for zz in range(NZ):
                row = pl.multiple_of((base + zz * NX * NC) * PAD_K, 8)
                x_ref[pl.ds(row, KEPT), :] = q_refs[dx * NC + dc][zz * KEPT : (zz + 1) * KEPT, :]
    store_half(x_ref, buf_ref, o_ref, sem, 0)


def store_p(pos, prior, blocks):
    return pl.pallas_call(
        store_p_kernel,
        in_specs=[SMEM, HBM] + [VMEM] * 8,
        out_specs=HBM,
        out_shape=f32(KEPT, FIELDS, 2 * LANES),
        scratch_shapes=STORE_SCRATCH,
        input_output_aliases={1: 0},
        compiler_params=PARAMS,
        name="store_p",
    )(pos, prior, *blocks)


def store_a_kernel(q_ref, o_ref, x_ref, buf_ref, sem):
    def field(f, carry):
        x_ref[pl.ds(pl.multiple_of(f * PAD_K, 8), KEPT), :] = q_ref[f]
        return carry

    lax.fori_loop(0, FIELDS, field, 0, unroll=8)
    store_half(x_ref, buf_ref, o_ref, sem, LANES)


def store_a(shares):
    return pl.pallas_call(
        store_a_kernel,
        in_specs=[VMEM],
        out_specs=HBM,
        out_shape=f32(KEPT, FIELDS, 2 * LANES),
        scratch_shapes=STORE_SCRATCH,
        compiler_params=PARAMS,
        name="store_a",
    )(shares)


def shifts(dx, dz, dc):
    def at(x, z, c):
        return (x % NX) * NZ * NC + (z % NZ) * NC + c % NC

    return [
        (at(x, z, c), at(x + dx, z + dz, c + dc)) for x in range(NX) for z in range(NZ) for c in range(NC)
    ]


Z_ORDER = (1, 7, 4, 3, 5, 2, 6)


def exchange_z(blocks):
    out = [None] * NZ
    out[0] = blocks[0]
    for dz in Z_ORDER:
        out[dz] = lax.ppermute(blocks[dz], "lon", shifts(0, dz, 0))
    return out


AX_ORDER = (2, 1, 3)
GROUPS = [[x * GROUP + g for g in range(GROUP)] for x in range(NX)]


def exchange_x(blocks):
    out = [None] * NX
    out[0] = blocks[0]
    for dx in AX_ORDER:
        out[dx] = lax.ppermute(blocks[dx], "lon", shifts(dx, 0, 0))
    return out


X_ORDER = ((2, 0), (2, 1), (1, 0), (3, 0), (1, 1), (3, 1), (0, 1))


def exchange_xc(blocks):
    out = [None] * (NX * NC)
    out[0] = blocks[0]
    for dx, dc in X_ORDER:
        out[dx * NC + dc] = lax.ppermute(blocks[dx * NC + dc], "lon", shifts(dx, 0, dc))
    return out


def local(state):
    device = lax.axis_index("lon")
    pos = jnp.stack([device // (NZ * NC), (device // NC) % NZ, device % NC]).astype(jnp.int32)
    w = twiddle_matrices(1.0 / math.sqrt(NLON))
    pieces, parts = split(pos, state)
    pieces = exchange_z(pieces)
    parts = exchange_x(parts)
    sent = spread_a(pos, [b.reshape(LON * GROUP, LANES) for b in parts])
    gathered = lax.all_to_all(
        sent, "lon", split_axis=0, concat_axis=0, axis_index_groups=GROUPS, tiled=True
    )
    pieces = spread_x(pos, [b.reshape(LON * 8, LANES) for b in pieces])
    pieces = exchange_xc(pieces)
    pieces = fft_p(pos, pieces, w)
    pieces = exchange_z(pieces)
    spectrum = fft_a(gathered.reshape(NLON, LANES), w)
    shares = lax.all_to_all(spectrum, "lon", split_axis=0, concat_axis=0, tiled=True)
    pieces = spread_out(pos, pieces)
    pieces = exchange_xc(pieces)
    out = store_a(shares)
    out = store_p(pos, out, pieces)
    return out.reshape(2, RADIX, FIELDS, 2 * LANES)


def solution(mesh):
    return jax.shard_map(
        local,
        mesh=mesh,
        in_specs=(P("lon", None, "lat"),),
        out_specs=P(None, "lon", None, "lat"),
        check_vma=False,
    )
```

```python
import math

import jax
import jax.numpy as jnp
from jax import lax
from jax.experimental import pallas as pl
from jax.experimental.pallas import tpu as pltpu
from jax.sharding import PartitionSpec as P


NLON = 2048
RADIX = 16
INNER = NLON // RADIX
PEERS = 64
HALF = RADIX // 2
NX, NZ, NC = 4, 8, 2
LON = 32
KEPT = 2 * RADIX
FIELDS = 64
LANES = 128
VMEM = pl.BlockSpec(memory_space=pltpu.VMEM)
HBM = pl.BlockSpec(memory_space=pltpu.HBM)
SMEM = pl.BlockSpec(memory_space=pltpu.SMEM)
PARAMS = pltpu.CompilerParams(vmem_limit_bytes=16 * 1024 * 1024)


def f32(*shape):
    return jax.ShapeDtypeStruct(shape, jnp.float32)


def vmem(*shape):
    return pltpu.VMEM(shape, jnp.float32)


def split_bf16(v):
    high = v.astype(jnp.bfloat16)
    low = (v - high.astype(jnp.float32)).astype(jnp.bfloat16)
    return high, low


def phase(rows, cols):
    turn = (rows * cols) % NLON
    turn = jnp.where(turn >= NLON // 2, turn - NLON, turn)
    return turn.astype(jnp.float32) * (2.0 * math.pi / NLON)


def twiddle_matrices(scale):
    shape = (HALF, 2, PEERS, INNER)
    pair = lax.broadcasted_iota(jnp.int32, shape, 0)
    mirror = lax.broadcasted_iota(jnp.int32, shape, 1)
    outer = lax.broadcasted_iota(jnp.int32, shape, 2)
    inner = lax.broadcasted_iota(jnp.int32, shape, 3)
    first = jnp.where(mirror == 0, pair, jnp.where(pair == 0, HALF, RADIX - pair))
    angle = phase(inner, first + RADIX * outer)
    c = jnp.cos(angle) * scale
    s = jnp.sin(angle) * scale
    real_only = pair == 0
    zero = jnp.zeros_like(c)
    plain = mirror == 0
    re_a = jnp.where(real_only, jnp.where(plain, c, zero), c)
    im_a = jnp.where(real_only, jnp.where(plain, -s, zero), -s)
    re_b = jnp.where(real_only, jnp.where(plain, zero, c), jnp.where(plain, s, -s))
    im_b = jnp.where(real_only, jnp.where(plain, zero, -s), jnp.where(plain, c, -c))
    re = jnp.concatenate([re_a, re_b], axis=-1)
    im = jnp.concatenate([im_a, im_b], axis=-1)
    full = jnp.stack([re, im], axis=2)
    full = full.reshape(HALF, 4 * PEERS, 2 * INNER)
    high = lax.reduce_precision(full, 8, 7)
    high, low = high.astype(jnp.bfloat16), (full - high).astype(jnp.bfloat16)
    return high, low


def fft_real16(x):
    def fft_complex8(z):
        def fft4(a):
            (ar, ai), (br, bi), (cr, ci), (dr, di) = a
            sr, si = ar + cr, ai + ci
            tr, ti = ar - cr, ai - ci
            ur, ui = br + dr, bi + di
            vr, vi = br - dr, bi - di
            return [(sr + ur, si + ui), (tr + vi, ti - vr), (sr - ur, si - ui), (tr - vi, ti + vr)]

        even = fft4(z[0::2])
        odd = fft4(z[1::2])
        h = math.sqrt(0.5)
        out = [None] * 8
        for k in range(4):
            er, ei = even[k]
            pr, pi = odd[k]
            if k == 1:
                pr, pi = (pr + pi) * h, (pi - pr) * h
            elif k == 2:
                pr, pi = pi, -pr
            elif k == 3:
                pr, pi = (pi - pr) * h, -(pr + pi) * h
            out[k] = (er + pr, ei + pi)
            out[k + 4] = (er - pr, ei - pi)
        return out

    z = fft_complex8([(x[2 * i], x[2 * i + 1]) for i in range(8)])
    out = [(z[0][0] + z[0][1], None)]
    for k in range(1, 8):
        zr, zi = z[k]
        wr, wi = z[8 - k]
        er, ei = (zr + wr) * 0.5, (zi - wi) * 0.5
        pr, pi = (zi + wi) * 0.5, (wr - zr) * 0.5
        c, s = math.cos(2 * math.pi * k / 16), math.sin(2 * math.pi * k / 16)
        out.append((er + c * pr + s * pi, ei + c * pi - s * pr))
    out.append((z[0][0] - z[0][1], None))
    return out


PAD_R = PEERS + 8


def natural_row(n2, base):
    return n2 * INNER + base


def grouped_row(n2, base):
    return ((n2 % 4) * 4 + base // LON) * INNER + (n2 // 4) * LON + base % LON


def fft_core(x_ref, wh_ref, wl_ref, y_ref, r_ref, row_of):
    def butterfly(i, carry):
        base = pl.multiple_of(i * 8, 8)
        x = [x_ref[pl.ds(pl.multiple_of(row_of(n2, base), 8), 8), :] for n2 in range(RADIX)]
        y = fft_real16(x)
        for k in range(HALF):
            parts = (y[0][0], y[HALF][0]) if k == 0 else y[k]
            for j, part in enumerate(parts):
                y_ref[k, pl.ds(j * INNER + base, 8), :] = part
        return carry

    lax.fori_loop(0, INNER // 8, butterfly, 0, unroll=4)
    for k in range(HALF):
        yh, yl = split_bf16(y_ref[k])
        two = jnp.dot(wh_ref[k], jnp.concatenate([yh, yl], axis=1), preferred_element_type=jnp.float32)
        r = two[:, :LANES] + two[:, LANES:]
        r = r + jnp.dot(wl_ref[k], yh, preferred_element_type=jnp.float32)
        mirror = HALF if k == 0 else RADIX - k
        for q, row in enumerate((k, RADIX + k, mirror, RADIX + mirror)):
            r_ref[pl.ds(row * PAD_R, PEERS), :] = r[q * PEERS : (q + 1) * PEERS]


PIECES = 4


def send_pieces(body, count, buf_ref, o_ref, sem):
    step = count // PIECES
    copies = []
    for piece in range(PIECES):
        lax.fori_loop(piece * step, (piece + 1) * step, body, 0, unroll=4)
        rows = pl.ds(piece * step, step)
        copy = pltpu.make_async_copy(buf_ref.at[rows], o_ref.at[rows], sem.at[piece])
        copy.start()
        copies.append(copy)
    for copy in copies:
        copy.wait()


FFT_SCRATCH = [
    pltpu.VMEM((HALF, 2 * INNER, LANES), jnp.float32),
    pltpu.VMEM((KEPT * PAD_R, LANES), jnp.float32),
]


def mode_rows(r_ref, k1, eight):
    return r_ref[pl.ds(eight * 8 * PAD_R + k1, 8, stride=PAD_R), :]


def fft_a_kernel(x_ref, wh_ref, wl_ref, o_ref, y_ref, r_ref, buf_ref, sem):
    fft_core(x_ref, wh_ref, wl_ref, y_ref, r_ref, grouped_row)

    def peer(k1, carry):
        for eight in range(KEPT // 8):
            buf_ref[k1, eight * 8 : eight * 8 + 8, :] = mode_rows(r_ref, k1, eight)
        return carry

    send_pieces(peer, PEERS, buf_ref, o_ref, sem)


def fft_a(gathered, wh, wl):
    return pl.pallas_call(
        fft_a_kernel,
        in_specs=[VMEM] * 3,
        out_specs=HBM,
        out_shape=pltpu.HBM((PEERS, KEPT, LANES), jnp.float32),
        scratch_shapes=FFT_SCRATCH
        + [pltpu.VMEM((PEERS, KEPT, LANES), jnp.float32), pltpu.SemaphoreType.DMA((PIECES,))],
        compiler_params=PARAMS,
        name="fft_a",
    )(gathered, wh, wl)


def fft_p_kernel(pos_ref, *refs):
    g_refs, (wh_ref, wl_ref) = refs[:8], refs[8:10]
    stay_ref, far_ref, send_refs, swap_ref = refs[10], refs[11], refs[12:15], refs[15]
    x_ref, y_ref, r_ref = refs[16:]
    x, z, c = pos_ref[0], pos_ref[1], pos_ref[2]
    for dx in range(NX):
        for dc in range(NC):
            xx, core = (x + NX - dx) % NX, (c + dc) % NC
            for piece in range(NZ):
                zz, cc = piece_source(z, core, piece)
                row = pl.multiple_of(xx * (NLON // NX) + zz * (NC * LON) + cc * LON, LON)
                x_ref[pl.ds(row, LON), :] = g_refs[dx * NC + dc][piece * LON : (piece + 1) * LON, :]
    fft_core(x_ref, wh_ref, wl_ref, y_ref, r_ref, natural_row)
    way = 1 - 2 * c
    places = [(stay_ref, 0, z), (far_ref, 0, z + NZ // 2)]
    places += [(swap_ref, i, z - way * k) for i, k in enumerate(STEPS)]
    places += [(send_refs[i], 0, z + way * k) for i, k in enumerate(STEPS)]
    for ref, slot, place in places:
        target = (place + NZ) % NZ
        for xx in range(NX):
            for cc in range(NC):
                for eight in range(KEPT // 8):
                    row = slot * BLOCK + (xx * NC + cc) * KEPT + eight * 8
                    ref[row : row + 8, :] = mode_rows(r_ref, xx * NZ * NC + target * NC + cc, eight)


def fft_p(pos, blocks, wh, wl):
    return pl.pallas_call(
        fft_p_kernel,
        in_specs=[SMEM] + [VMEM] * 10,
        out_specs=[VMEM] * 6,
        out_shape=[vmem(BLOCK, LANES)] * 2 + [vmem(2 * BLOCK, LANES)] * 3 + [vmem(3 * BLOCK, LANES)],
        scratch_shapes=[pltpu.VMEM((NLON, LANES), jnp.float32)] + FFT_SCRATCH,
        compiler_params=PARAMS,
        name="fft_p",
    )(pos, *blocks, wh, wl)


GROUP = NZ * NC


STEPS = (1, 2, 3)


def split_kernel(pos_ref, s_ref, *refs):
    stay_ref, far_ref, send_refs, swap_ref = refs[0], refs[1], refs[2:5], refs[5]
    part_refs, sem = refs[6 : 6 + NX], refs[6 + NX]
    x, z, c = pos_ref[0], pos_ref[1], pos_ref[2]
    way = 1 - 2 * c
    places = [(stay_ref, 0, z), (far_ref, 0, z + NZ // 2)]
    places += [(swap_ref, i, z - way * k) for i, k in enumerate(STEPS)]
    places += [(send_refs[i], 0, z + way * k) for i, k in enumerate(STEPS)]
    copies = []
    for ref, slot, target in places:
        field = pl.multiple_of(((target + NZ) % NZ) * 8, 8)
        source = s_ref.at[:, pl.ds(field, 8), pl.ds(0, LANES)]
        copies.append(pltpu.make_async_copy(source, ref.at[pl.ds(slot * LON, LON)], sem.at[len(copies)]))
    for dx in range(NX):
        field = pl.multiple_of(((x + dx) % NX) * GROUP, GROUP)
        source = s_ref.at[:, pl.ds(field, GROUP), pl.ds(LANES, LANES)]
        copies.append(pltpu.make_async_copy(source, part_refs[dx], sem.at[len(copies)]))
    for copy in copies:
        copy.start()
    for copy in copies:
        copy.wait()


def split(pos, state):
    out = pl.pallas_call(
        split_kernel,
        in_specs=[SMEM, HBM],
        out_specs=[VMEM] * (6 + NX),
        out_shape=[vmem(LON, 8, LANES)] * 2
        + [vmem(2 * LON, 8, LANES)] * 3
        + [vmem(3 * LON, 8, LANES)]
        + [vmem(LON, GROUP, LANES)] * NX,
        scratch_shapes=[pltpu.SemaphoreType.DMA((NZ + NX,))],
        compiler_params=PARAMS,
        name="split",
    )(pos, pltpu.with_memory_space_constraint(state, pltpu.HBM))
    return [v.reshape(-1, LANES) for v in out[:6]], out[6:]


BLOCK = 256


def merge_kernel(swap_ref, *refs):
    o_refs, sem = refs[3:6], refs[6]
    copies = [
        pltpu.make_async_copy(swap_ref.at[pl.ds(i * BLOCK, BLOCK)], o_refs[i].at[pl.ds(BLOCK, BLOCK)], sem.at[i])
        for i in range(3)
    ]
    for copy in copies:
        copy.start()
    for copy in copies:
        copy.wait()


def merge(swap, sends):
    anywhere = pl.BlockSpec(memory_space=pl.ANY)
    return pl.pallas_call(
        merge_kernel,
        in_specs=[anywhere] * 4,
        out_specs=[anywhere] * 3,
        out_shape=[f32(2 * BLOCK, LANES)] * 3,
        scratch_shapes=[pltpu.SemaphoreType.DMA((3,))],
        input_output_aliases={1: 0, 2: 1, 3: 2},
        compiler_params=PARAMS,
        name="merge",
    )(swap, *sends)


def piece_of(refs, piece):
    if piece < 2:
        return refs[piece], 0
    return refs[1 + piece // 2], (piece % 2) * BLOCK


def piece_source(z, core, piece):
    if piece == 0:
        return z, core
    if piece == 1:
        return (z + NZ // 2) % NZ, core
    way = 1 - 2 * core
    return (z - way * (piece // 2) + NZ) % NZ, core if piece % 2 == 0 else 1 - core


def spread_x_kernel(pos_ref, *refs):
    b_refs, o_refs = refs[:5], refs[5:]
    x, c = pos_ref[0], pos_ref[2]
    for dx in range(NX):
        for dc in range(NC):
            field = ((x + dx) % NX) * NC + (c + dc) % NC
            for piece in range(NZ):
                ref, row = piece_of(b_refs, piece)
                o_refs[dx * NC + dc][piece * LON : (piece + 1) * LON, :] = ref[pl.ds(row + field, LON, stride=8), :]


def spread_x(pos, blocks):
    return pl.pallas_call(
        spread_x_kernel,
        in_specs=[SMEM] + [VMEM] * 5,
        out_specs=[VMEM] * (NX * NC),
        out_shape=[vmem(NZ * LON, LANES)] * (NX * NC),
        compiler_params=PARAMS,
        name="spread_x",
    )(pos, *blocks)


def spread_out_kernel(pos_ref, *refs):
    h_refs, o_refs = refs[:5], refs[5:]
    x, c = pos_ref[0], pos_ref[2]
    for dx in range(NX):
        for dc in range(NC):
            source = (((x + dx) % NX) * NC + (c + dc) % NC) * KEPT
            for piece in range(NZ):
                ref, row = piece_of(h_refs, piece)
                start = pl.multiple_of(source + row, KEPT)
                o_refs[dx * NC + dc][piece * KEPT : (piece + 1) * KEPT, :] = ref[pl.ds(start, KEPT), :]


def spread_out(pos, blocks):
    return pl.pallas_call(
        spread_out_kernel,
        in_specs=[SMEM] + [VMEM] * 5,
        out_specs=[VMEM] * (NX * NC),
        out_shape=[vmem(NZ * KEPT, LANES)] * (NX * NC),
        compiler_params=PARAMS,
        name="spread_out",
    )(pos, *blocks)


def spread_a_kernel(pos_ref, *refs):
    b_refs, o_ref, buf_ref, sem = refs[:NX], refs[NX], refs[NX + 1], refs[NX + 2]
    x = pos_ref[0]

    def field(f, carry):
        for dx in range(NX):
            row = pl.multiple_of(((x + NX - dx) % NX) * LON, LON)
            buf_ref[f, pl.ds(row, LON), :] = b_refs[dx][pl.ds(f, LON, stride=GROUP), :]
        return carry

    send_pieces(field, GROUP, buf_ref, o_ref, sem)


def spread_a(pos, blocks):
    return pl.pallas_call(
        spread_a_kernel,
        in_specs=[SMEM] + [VMEM] * NX,
        out_specs=HBM,
        out_shape=pltpu.HBM((GROUP, NX * LON, LANES), jnp.float32),
        scratch_shapes=[
            pltpu.VMEM((GROUP, NX * LON, LANES), jnp.float32),
            pltpu.SemaphoreType.DMA((PIECES,)),
        ],
        compiler_params=PARAMS,
        name="spread_a",
    )(pos, *blocks)


PAD_K = KEPT + 8


def store_half(x_ref, buf_ref, o_ref, sem, lane):
    copies = []
    step = KEPT // PIECES
    for piece in range(PIECES):
        for kept in range(piece * step, (piece + 1) * step):
            for eight in range(FIELDS // 8):
                buf_ref[kept, eight * 8 : eight * 8 + 8, :] = x_ref[pl.ds(eight * 8 * PAD_K + kept, 8, stride=PAD_K), :]
        copy = pltpu.make_async_copy(
            buf_ref.at[pl.ds(piece * step, step)],
            o_ref.at[pl.ds(piece * step, step), :, pl.ds(lane, LANES)],
            sem.at[piece],
        )
        copy.start()
        copies.append(copy)
    for copy in copies:
        copy.wait()


STORE_SCRATCH = [
    pltpu.VMEM((FIELDS * PAD_K, LANES), jnp.float32),
    pltpu.VMEM((KEPT, FIELDS, LANES), jnp.float32),
    pltpu.SemaphoreType.DMA((PIECES,)),
]


def store_p_kernel(pos_ref, prior_ref, *refs):
    del prior_ref
    q_refs, o_ref = refs[:8], refs[8]
    x_ref, buf_ref, sem = refs[9:]
    x, z, c = pos_ref[0], pos_ref[1], pos_ref[2]
    for dx in range(NX):
        for dc in range(NC):
            xx, core = (x + NX - dx) % NX, (c + dc) % NC
            for piece in range(NZ):
                zz, cc = piece_source(z, core, piece)
                row = pl.multiple_of((zz * NX * NC + xx * NC + cc) * PAD_K, 8)
                x_ref[pl.ds(row, KEPT), :] = q_refs[dx * NC + dc][piece * KEPT : (piece + 1) * KEPT, :]
    store_half(x_ref, buf_ref, o_ref, sem, 0)


def store_p(pos, prior, blocks):
    return pl.pallas_call(
        store_p_kernel,
        in_specs=[SMEM, HBM] + [VMEM] * 8,
        out_specs=HBM,
        out_shape=f32(KEPT, FIELDS, 2 * LANES),
        scratch_shapes=STORE_SCRATCH,
        input_output_aliases={1: 0},
        compiler_params=PARAMS,
        name="store_p",
    )(pos, prior, *blocks)


def store_a_kernel(q_ref, o_ref, x_ref, buf_ref, sem):
    def field(f, carry):
        x_ref[pl.ds(pl.multiple_of(f * PAD_K, 8), KEPT), :] = q_ref[f]
        return carry

    lax.fori_loop(0, FIELDS, field, 0, unroll=8)
    store_half(x_ref, buf_ref, o_ref, sem, LANES)


def store_a(shares):
    return pl.pallas_call(
        store_a_kernel,
        in_specs=[VMEM],
        out_specs=HBM,
        out_shape=f32(KEPT, FIELDS, 2 * LANES),
        scratch_shapes=STORE_SCRATCH,
        compiler_params=PARAMS,
        name="store_a",
    )(shares)


def shifts(dx, dz, dc):
    def at(x, z, c):
        return (x % NX) * NZ * NC + (z % NZ) * NC + c % NC

    return [
        (at(x, z, c), at(x + dx, z + dz, c + dc)) for x in range(NX) for z in range(NZ) for c in range(NC)
    ]


def two_ways(k):
    return [
        pair
        for c in range(NC)
        for pair in shifts(0, k if c == 0 else NZ - k, 0)
        if pair[0] % NC == c
    ]


Z_ORDER = (1, 3, 2)


def exchange_z(blocks):
    stay, far, sends, swap = blocks[0], blocks[1], blocks[2:5], blocks[5]
    swap = lax.ppermute(swap, "lon", shifts(0, 0, 1))
    far = lax.ppermute(far, "lon", shifts(0, NZ // 2, 0))
    sends = merge(swap, sends)
    got = [None] * 3
    for k in Z_ORDER:
        got[k - 1] = lax.ppermute(sends[k - 1], "lon", two_ways(k))
    return [stay, far, *got]


AX_ORDER = (2, 1, 3)
GROUPS = [[x * GROUP + g for g in range(GROUP)] for x in range(NX)]


def exchange_x(blocks):
    out = [None] * NX
    out[0] = blocks[0]
    for dx in AX_ORDER:
        out[dx] = lax.ppermute(blocks[dx], "lon", shifts(dx, 0, 0))
    return out


X_ORDER = ((2, 0), (2, 1), (1, 0), (3, 0), (1, 1), (3, 1), (0, 1))


def exchange_xc(blocks):
    out = [None] * (NX * NC)
    out[0] = blocks[0]
    for dx, dc in X_ORDER:
        out[dx * NC + dc] = lax.ppermute(blocks[dx * NC + dc], "lon", shifts(dx, 0, dc))
    return out


def local(state):
    device = lax.axis_index("lon")
    pos = jnp.stack([device // (NZ * NC), (device // NC) % NZ, device % NC]).astype(jnp.int32)
    wh, wl = twiddle_matrices(1.0 / math.sqrt(NLON))
    pieces, parts = split(pos, state)
    pieces = exchange_z(pieces)
    parts = exchange_x(parts)
    sent = spread_a(pos, [b.reshape(LON * GROUP, LANES) for b in parts])
    gathered = lax.all_to_all(
        sent, "lon", split_axis=0, concat_axis=0, axis_index_groups=GROUPS, tiled=True
    )
    pieces = spread_x(pos, pieces)
    pieces = exchange_xc(pieces)
    pieces = fft_p(pos, pieces, wh, wl)
    pieces = exchange_z(pieces)
    spectrum = fft_a(gathered.reshape(NLON, LANES), wh, wl)
    shares = lax.all_to_all(spectrum, "lon", split_axis=0, concat_axis=0, tiled=True)
    pieces = spread_out(pos, pieces)
    pieces = exchange_xc(pieces)
    out = store_a(shares)
    out = store_p(pos, out, pieces)
    return out.reshape(2, RADIX, FIELDS, 2 * LANES)


def solution(mesh):
    return jax.shard_map(
        local,
        mesh=mesh,
        in_specs=(P("lon", None, "lat"),),
        out_specs=P(None, "lon", None, "lat"),
        check_vma=False,
    )
```

```python
import math

import jax
import jax.numpy as jnp
from jax import lax
from jax.experimental import pallas as pl
from jax.experimental.pallas import tpu as pltpu
from jax.sharding import PartitionSpec as P


NLON = 2048
RADIX = 16
INNER = NLON // RADIX
PEERS = 64
HALF = RADIX // 2
NX, NZ, NC = 4, 8, 2
LON = 32
KEPT = 2 * RADIX
FIELDS = 64
LANES = 128
VMEM = pl.BlockSpec(memory_space=pltpu.VMEM)
HBM = pl.BlockSpec(memory_space=pltpu.HBM)
SMEM = pl.BlockSpec(memory_space=pltpu.SMEM)
PARAMS = pltpu.CompilerParams(vmem_limit_bytes=16 * 1024 * 1024)


def f32(*shape):
    return jax.ShapeDtypeStruct(shape, jnp.float32)


def vmem(*shape):
    return pltpu.VMEM(shape, jnp.float32)


def split_bf16(v):
    high = v.astype(jnp.bfloat16)
    low = (v - high.astype(jnp.float32)).astype(jnp.bfloat16)
    return high, low


def phase(rows, cols):
    turn = (rows * cols) % NLON
    turn = jnp.where(turn >= NLON // 2, turn - NLON, turn)
    return turn.astype(jnp.float32) * (2.0 * math.pi / NLON)


def twiddle_matrices(scale):
    shape = (HALF, 2, PEERS, INNER)
    pair = lax.broadcasted_iota(jnp.int32, shape, 0)
    mirror = lax.broadcasted_iota(jnp.int32, shape, 1)
    outer = lax.broadcasted_iota(jnp.int32, shape, 2)
    inner = lax.broadcasted_iota(jnp.int32, shape, 3)
    first = jnp.where(mirror == 0, pair, jnp.where(pair == 0, HALF, RADIX - pair))
    angle = phase(inner, first + RADIX * outer)
    c = jnp.cos(angle) * scale
    s = jnp.sin(angle) * scale
    real_only = pair == 0
    zero = jnp.zeros_like(c)
    plain = mirror == 0
    re_a = jnp.where(real_only, jnp.where(plain, c, zero), c)
    im_a = jnp.where(real_only, jnp.where(plain, -s, zero), -s)
    re_b = jnp.where(real_only, jnp.where(plain, zero, c), jnp.where(plain, s, -s))
    im_b = jnp.where(real_only, jnp.where(plain, zero, -s), jnp.where(plain, c, -c))
    re = jnp.concatenate([re_a, re_b], axis=-1)
    im = jnp.concatenate([im_a, im_b], axis=-1)
    full = jnp.stack([re, im], axis=2)
    full = full.reshape(HALF, 4 * PEERS, 2 * INNER)
    high = lax.reduce_precision(full, 8, 7)
    high, low = high.astype(jnp.bfloat16), (full - high).astype(jnp.bfloat16)
    return high, low


def fft_real16(x):
    def fft_complex8(z):
        def fft4(a):
            (ar, ai), (br, bi), (cr, ci), (dr, di) = a
            sr, si = ar + cr, ai + ci
            tr, ti = ar - cr, ai - ci
            ur, ui = br + dr, bi + di
            vr, vi = br - dr, bi - di
            return [(sr + ur, si + ui), (tr + vi, ti - vr), (sr - ur, si - ui), (tr - vi, ti + vr)]

        even = fft4(z[0::2])
        odd = fft4(z[1::2])
        h = math.sqrt(0.5)
        out = [None] * 8
        for k in range(4):
            er, ei = even[k]
            pr, pi = odd[k]
            if k == 1:
                pr, pi = (pr + pi) * h, (pi - pr) * h
            elif k == 2:
                pr, pi = pi, -pr
            elif k == 3:
                pr, pi = (pi - pr) * h, -(pr + pi) * h
            out[k] = (er + pr, ei + pi)
            out[k + 4] = (er - pr, ei - pi)
        return out

    z = fft_complex8([(x[2 * i], x[2 * i + 1]) for i in range(8)])
    out = [(z[0][0] + z[0][1], None)]
    for k in range(1, 8):
        zr, zi = z[k]
        wr, wi = z[8 - k]
        er, ei = (zr + wr) * 0.5, (zi - wi) * 0.5
        pr, pi = (zi + wi) * 0.5, (wr - zr) * 0.5
        c, s = math.cos(2 * math.pi * k / 16), math.sin(2 * math.pi * k / 16)
        out.append((er + c * pr + s * pi, ei + c * pi - s * pr))
    out.append((z[0][0] - z[0][1], None))
    return out


PAD_R = PEERS + 8


def natural_row(n2, base):
    return n2 * INNER + base


def grouped_row(n2, base):
    return ((n2 % 4) * 4 + base // LON) * INNER + (n2 // 4) * LON + base % LON


def fft_core(x_ref, wh_ref, wl_ref, y_ref, r_ref, row_of):
    def butterfly(i, carry):
        base = pl.multiple_of(i * 8, 8)
        x = [x_ref[pl.ds(pl.multiple_of(row_of(n2, base), 8), 8), :] for n2 in range(RADIX)]
        y = fft_real16(x)
        for k in range(HALF):
            parts = (y[0][0], y[HALF][0]) if k == 0 else y[k]
            for j, part in enumerate(parts):
                y_ref[k, pl.ds(j * INNER + base, 8), :] = part
        return carry

    lax.fori_loop(0, INNER // 8, butterfly, 0, unroll=4)
    for k in range(HALF):
        yh, yl = split_bf16(y_ref[k])
        two = jnp.dot(wh_ref[k], jnp.concatenate([yh, yl], axis=1), preferred_element_type=jnp.float32)
        r = two[:, :LANES] + two[:, LANES:]
        r = r + jnp.dot(wl_ref[k], yh, preferred_element_type=jnp.float32)
        mirror = HALF if k == 0 else RADIX - k
        for q, row in enumerate((k, RADIX + k, mirror, RADIX + mirror)):
            r_ref[pl.ds(row * PAD_R, PEERS), :] = r[q * PEERS : (q + 1) * PEERS]


PIECES = 4


def send_pieces(body, count, buf_ref, o_ref, sem):
    step = count // PIECES
    copies = []
    for piece in range(PIECES):
        lax.fori_loop(piece * step, (piece + 1) * step, body, 0, unroll=4)
        rows = pl.ds(piece * step, step)
        copy = pltpu.make_async_copy(buf_ref.at[rows], o_ref.at[rows], sem.at[piece])
        copy.start()
        copies.append(copy)
    for copy in copies:
        copy.wait()


FFT_SCRATCH = [
    pltpu.VMEM((HALF, 2 * INNER, LANES), jnp.float32),
    pltpu.VMEM((KEPT * PAD_R, LANES), jnp.float32),
]


def mode_rows(r_ref, k1, eight):
    return r_ref[pl.ds(eight * 8 * PAD_R + k1, 8, stride=PAD_R), :]


def fft_a_kernel(x_ref, wh_ref, wl_ref, o_ref, y_ref, r_ref, buf_ref, sem):
    fft_core(x_ref, wh_ref, wl_ref, y_ref, r_ref, grouped_row)

    def peer(k1, carry):
        for eight in range(KEPT // 8):
            buf_ref[k1, eight * 8 : eight * 8 + 8, :] = mode_rows(r_ref, k1, eight)
        return carry

    send_pieces(peer, PEERS, buf_ref, o_ref, sem)


def fft_a(gathered, wh, wl):
    return pl.pallas_call(
        fft_a_kernel,
        in_specs=[VMEM] * 3,
        out_specs=HBM,
        out_shape=pltpu.HBM((PEERS, KEPT, LANES), jnp.float32),
        scratch_shapes=FFT_SCRATCH
        + [pltpu.VMEM((PEERS, KEPT, LANES), jnp.float32), pltpu.SemaphoreType.DMA((PIECES,))],
        compiler_params=PARAMS,
        name="fft_a",
    )(gathered, wh, wl)


def fft_p_kernel(pos_ref, *refs):
    g_refs, (wh_ref, wl_ref) = refs[:8], refs[8:10]
    stay_ref, far_ref, send_refs, swap_ref = refs[10], refs[11], refs[12:15], refs[15]
    x_ref, y_ref, r_ref = refs[16:]
    x, z, c = pos_ref[0], pos_ref[1], pos_ref[2]
    for dx in range(NX):
        for dc in range(NC):
            xx, core = (x + NX - dx) % NX, (c + dc) % NC
            for piece in range(NZ):
                zz, cc = piece_source(z, core, piece)
                row = pl.multiple_of(xx * (NLON // NX) + zz * (NC * LON) + cc * LON, LON)
                x_ref[pl.ds(row, LON), :] = g_refs[dx * NC + dc][piece * LON : (piece + 1) * LON, :]
    fft_core(x_ref, wh_ref, wl_ref, y_ref, r_ref, natural_row)
    way = 1 - 2 * c
    places = [(stay_ref, 0, z), (far_ref, 0, z + NZ // 2)]
    places += [(swap_ref, i, z - way * k) for i, k in enumerate(STEPS)]
    places += [(send_refs[i], 0, z + way * k) for i, k in enumerate(STEPS)]
    for ref, slot, place in places:
        target = (place + NZ) % NZ
        for xx in range(NX):
            for cc in range(NC):
                for eight in range(KEPT // 8):
                    row = slot * BLOCK + (xx * NC + cc) * KEPT + eight * 8
                    ref[row : row + 8, :] = mode_rows(r_ref, xx * NZ * NC + target * NC + cc, eight)


def fft_p(pos, blocks, wh, wl):
    return pl.pallas_call(
        fft_p_kernel,
        in_specs=[SMEM] + [VMEM] * 10,
        out_specs=[VMEM] * 6,
        out_shape=[vmem(BLOCK, LANES)] * 2 + [vmem(2 * BLOCK, LANES)] * 3 + [vmem(3 * BLOCK, LANES)],
        scratch_shapes=[pltpu.VMEM((NLON, LANES), jnp.float32)] + FFT_SCRATCH,
        compiler_params=PARAMS,
        name="fft_p",
    )(pos, *blocks, wh, wl)


GROUP = NZ * NC


STEPS = (1, 2, 3)


def split_kernel(pos_ref, s_ref, *refs):
    stay_ref, far_ref, send_refs, swap_ref = refs[0], refs[1], refs[2:5], refs[5]
    part_refs, sem = refs[6 : 6 + NX], refs[6 + NX]
    x, z, c = pos_ref[0], pos_ref[1], pos_ref[2]
    way = 1 - 2 * c
    places = [(stay_ref, 0, z), (far_ref, 0, z + NZ // 2)]
    places += [(swap_ref, i, z - way * k) for i, k in enumerate(STEPS)]
    places += [(send_refs[i], 0, z + way * k) for i, k in enumerate(STEPS)]
    copies = []
    for ref, slot, target in places:
        field = pl.multiple_of(((target + NZ) % NZ) * 8, 8)
        source = s_ref.at[:, pl.ds(field, 8), pl.ds(0, LANES)]
        copies.append(pltpu.make_async_copy(source, ref.at[pl.ds(slot * LON, LON)], sem.at[len(copies)]))
    for dx in range(NX):
        field = pl.multiple_of(((x + dx) % NX) * GROUP, GROUP)
        source = s_ref.at[:, pl.ds(field, GROUP), pl.ds(LANES, LANES)]
        copies.append(pltpu.make_async_copy(source, part_refs[dx], sem.at[len(copies)]))
    for copy in copies:
        copy.start()
    for copy in copies:
        copy.wait()


def split(pos, state):
    out = pl.pallas_call(
        split_kernel,
        in_specs=[SMEM, HBM],
        out_specs=[VMEM] * (6 + NX),
        out_shape=[vmem(LON, 8, LANES)] * 2
        + [vmem(2 * LON, 8, LANES)] * 3
        + [vmem(3 * LON, 8, LANES)]
        + [vmem(LON, GROUP, LANES)] * NX,
        scratch_shapes=[pltpu.SemaphoreType.DMA((NZ + NX,))],
        compiler_params=PARAMS,
        name="split",
    )(pos, pltpu.with_memory_space_constraint(state, pltpu.HBM))
    return [v.reshape(-1, LANES) for v in out[:6]], out[6:]


BLOCK = 256


def merge_kernel(swap_ref, *refs):
    o_refs, sem = refs[3:6], refs[6]
    copies = [
        pltpu.make_async_copy(swap_ref.at[pl.ds(i * BLOCK, BLOCK)], o_refs[i].at[pl.ds(BLOCK, BLOCK)], sem.at[i])
        for i in range(3)
    ]
    for copy in copies:
        copy.start()
    for copy in copies:
        copy.wait()


def merge(swap, sends):
    anywhere = pl.BlockSpec(memory_space=pl.ANY)
    return pl.pallas_call(
        merge_kernel,
        in_specs=[anywhere] * 4,
        out_specs=[anywhere] * 3,
        out_shape=[f32(2 * BLOCK, LANES)] * 3,
        scratch_shapes=[pltpu.SemaphoreType.DMA((3,))],
        input_output_aliases={1: 0, 2: 1, 3: 2},
        compiler_params=PARAMS,
        name="merge",
    )(swap, *sends)


def piece_of(refs, piece):
    if piece < 2:
        return refs[piece], 0
    return refs[1 + piece // 2], (piece % 2) * BLOCK


def piece_source(z, core, piece):
    if piece == 0:
        return z, core
    if piece == 1:
        return (z + NZ // 2) % NZ, core
    way = 1 - 2 * core
    return (z - way * (piece // 2) + NZ) % NZ, core if piece % 2 == 0 else 1 - core


def spread_x_kernel(pos_ref, *refs):
    b_refs, o_refs = refs[:5], refs[5:]
    x, c = pos_ref[0], pos_ref[2]
    for dx in range(NX):
        for dc in range(NC):
            field = ((x + dx) % NX) * NC + (c + dc) % NC
            for piece in range(NZ):
                ref, row = piece_of(b_refs, piece)
                o_refs[dx * NC + dc][piece * LON : (piece + 1) * LON, :] = ref[pl.ds(row + field, LON, stride=8), :]


def spread_x(pos, blocks):
    return pl.pallas_call(
        spread_x_kernel,
        in_specs=[SMEM] + [VMEM] * 5,
        out_specs=[VMEM] * (NX * NC),
        out_shape=[vmem(NZ * LON, LANES)] * (NX * NC),
        compiler_params=PARAMS,
        name="spread_x",
    )(pos, *blocks)


def spread_out_kernel(pos_ref, *refs):
    h_refs, o_refs = refs[:5], refs[5:]
    x, c = pos_ref[0], pos_ref[2]
    for dx in range(NX):
        for dc in range(NC):
            source = (((x + dx) % NX) * NC + (c + dc) % NC) * KEPT
            for piece in range(NZ):
                ref, row = piece_of(h_refs, piece)
                start = pl.multiple_of(source + row, KEPT)
                o_refs[dx * NC + dc][piece * KEPT : (piece + 1) * KEPT, :] = ref[pl.ds(start, KEPT), :]


def spread_out(pos, blocks):
    return pl.pallas_call(
        spread_out_kernel,
        in_specs=[SMEM] + [VMEM] * 5,
        out_specs=[VMEM] * (NX * NC),
        out_shape=[vmem(NZ * KEPT, LANES)] * (NX * NC),
        compiler_params=PARAMS,
        name="spread_out",
    )(pos, *blocks)


def spread_a_kernel(pos_ref, *refs):
    b_refs, o_ref, buf_ref, sem = refs[:NX], refs[NX], refs[NX + 1], refs[NX + 2]
    x = pos_ref[0]

    def field(f, carry):
        for dx in range(NX):
            row = pl.multiple_of(((x + NX - dx) % NX) * LON, LON)
            buf_ref[f, pl.ds(row, LON), :] = b_refs[dx][pl.ds(f, LON, stride=GROUP), :]
        return carry

    send_pieces(field, GROUP, buf_ref, o_ref, sem)


def spread_a(pos, blocks):
    return pl.pallas_call(
        spread_a_kernel,
        in_specs=[SMEM] + [VMEM] * NX,
        out_specs=HBM,
        out_shape=pltpu.HBM((GROUP, NX * LON, LANES), jnp.float32),
        scratch_shapes=[
            pltpu.VMEM((GROUP, NX * LON, LANES), jnp.float32),
            pltpu.SemaphoreType.DMA((PIECES,)),
        ],
        compiler_params=PARAMS,
        name="spread_a",
    )(pos, *blocks)


PAD_K = KEPT + 8


def store_half(x_ref, buf_ref, o_ref, sem, lane):
    copies = []
    step = KEPT // PIECES
    for piece in range(PIECES):
        for kept in range(piece * step, (piece + 1) * step):
            for eight in range(FIELDS // 8):
                buf_ref[kept, eight * 8 : eight * 8 + 8, :] = x_ref[pl.ds(eight * 8 * PAD_K + kept, 8, stride=PAD_K), :]
        copy = pltpu.make_async_copy(
            buf_ref.at[pl.ds(piece * step, step)],
            o_ref.at[pl.ds(piece * step, step), :, pl.ds(lane, LANES)],
            sem.at[piece],
        )
        copy.start()
        copies.append(copy)
    for copy in copies:
        copy.wait()


STORE_SCRATCH = [
    pltpu.VMEM((FIELDS * PAD_K, LANES), jnp.float32),
    pltpu.VMEM((KEPT, FIELDS, LANES), jnp.float32),
    pltpu.SemaphoreType.DMA((PIECES,)),
]


def store_p_kernel(pos_ref, prior_ref, *refs):
    del prior_ref
    q_refs, o_ref = refs[:8], refs[8]
    x_ref, buf_ref, sem = refs[9:]
    x, z, c = pos_ref[0], pos_ref[1], pos_ref[2]
    for dx in range(NX):
        for dc in range(NC):
            xx, core = (x + NX - dx) % NX, (c + dc) % NC
            for piece in range(NZ):
                zz, cc = piece_source(z, core, piece)
                row = pl.multiple_of((zz * NX * NC + xx * NC + cc) * PAD_K, 8)
                x_ref[pl.ds(row, KEPT), :] = q_refs[dx * NC + dc][piece * KEPT : (piece + 1) * KEPT, :]
    store_half(x_ref, buf_ref, o_ref, sem, 0)


def store_p(pos, prior, blocks):
    return pl.pallas_call(
        store_p_kernel,
        in_specs=[SMEM, HBM] + [VMEM] * 8,
        out_specs=HBM,
        out_shape=f32(KEPT, FIELDS, 2 * LANES),
        scratch_shapes=STORE_SCRATCH,
        input_output_aliases={1: 0},
        compiler_params=PARAMS,
        name="store_p",
    )(pos, prior, *blocks)


def store_a_kernel(q_ref, o_ref, x_ref, buf_ref, sem):
    def field(f, carry):
        x_ref[pl.ds(pl.multiple_of(f * PAD_K, 8), KEPT), :] = q_ref[f]
        return carry

    lax.fori_loop(0, FIELDS, field, 0, unroll=8)
    store_half(x_ref, buf_ref, o_ref, sem, LANES)


def store_a(shares):
    return pl.pallas_call(
        store_a_kernel,
        in_specs=[VMEM],
        out_specs=HBM,
        out_shape=f32(KEPT, FIELDS, 2 * LANES),
        scratch_shapes=STORE_SCRATCH,
        compiler_params=PARAMS,
        name="store_a",
    )(shares)


def shifts(dx, dz, dc):
    def at(x, z, c):
        return (x % NX) * NZ * NC + (z % NZ) * NC + c % NC

    return [
        (at(x, z, c), at(x + dx, z + dz, c + dc)) for x in range(NX) for z in range(NZ) for c in range(NC)
    ]


def two_ways(k):
    return [
        pair
        for c in range(NC)
        for pair in shifts(0, k if c == 0 else NZ - k, 0)
        if pair[0] % NC == c
    ]


Z_IN = (1, 3, 4, 2)
Z_OUT = (4, 3, 1, 2)


def exchange_z(blocks, order):
    stay, far, sends, swap = blocks[0], blocks[1], blocks[2:5], blocks[5]
    swap = lax.ppermute(swap, "lon", shifts(0, 0, 1))
    sends = merge(swap, sends)
    got = {}
    for k in order:
        block = far if k == NZ // 2 else sends[k - 1]
        got[k] = lax.ppermute(block, "lon", two_ways(k))
    return [stay, got[NZ // 2], *(got[k] for k in STEPS)]


AX_ORDER = (2, 1, 3)
GROUPS = [[x * GROUP + g for g in range(GROUP)] for x in range(NX)]


def exchange_x(blocks):
    out = [None] * NX
    out[0] = blocks[0]
    for dx in AX_ORDER:
        out[dx] = lax.ppermute(blocks[dx], "lon", shifts(dx, 0, 0))
    return out


X_ORDER = ((2, 0), (2, 1), (1, 0), (3, 0), (1, 1), (3, 1), (0, 1))


def exchange_xc(blocks):
    out = [None] * (NX * NC)
    out[0] = blocks[0]
    for dx, dc in X_ORDER:
        out[dx * NC + dc] = lax.ppermute(blocks[dx * NC + dc], "lon", shifts(dx, 0, dc))
    return out


def local(state):
    device = lax.axis_index("lon")
    pos = jnp.stack([device // (NZ * NC), (device // NC) % NZ, device % NC]).astype(jnp.int32)
    wh, wl = twiddle_matrices(1.0 / math.sqrt(NLON))
    pieces, parts = split(pos, state)
    pieces = exchange_z(pieces, Z_IN)
    parts = exchange_x(parts)
    sent = spread_a(pos, [b.reshape(LON * GROUP, LANES) for b in parts])
    gathered = lax.all_to_all(
        sent, "lon", split_axis=0, concat_axis=0, axis_index_groups=GROUPS, tiled=True
    )
    pieces = spread_x(pos, pieces)
    pieces = exchange_xc(pieces)
    pieces = fft_p(pos, pieces, wh, wl)
    pieces = exchange_z(pieces, Z_OUT)
    spectrum = fft_a(gathered.reshape(NLON, LANES), wh, wl)
    shares = lax.all_to_all(spectrum, "lon", split_axis=0, concat_axis=0, tiled=True)
    pieces = spread_out(pos, pieces)
    pieces = exchange_xc(pieces)
    out = store_a(shares)
    out = store_p(pos, out, pieces)
    return out.reshape(2, RADIX, FIELDS, 2 * LANES)


def solution(mesh):
    return jax.shard_map(
        local,
        mesh=mesh,
        in_specs=(P("lon", None, "lat"),),
        out_specs=P(None, "lon", None, "lat"),
        check_vma=False,
    )
```

```python
import math

import jax
import jax.numpy as jnp
from jax import lax
from jax.experimental import pallas as pl
from jax.experimental.pallas import tpu as pltpu
from jax.sharding import PartitionSpec as P


NLON = 2048
RADIX = 16
INNER = NLON // RADIX
PEERS = 64
HALF = RADIX // 2
NX, NZ, NC = 4, 8, 2
LON = 32
KEPT = 2 * RADIX
FIELDS = 64
LANES = 128
VMEM = pl.BlockSpec(memory_space=pltpu.VMEM)
HBM = pl.BlockSpec(memory_space=pltpu.HBM)
SMEM = pl.BlockSpec(memory_space=pltpu.SMEM)
PARAMS = pltpu.CompilerParams(vmem_limit_bytes=16 * 1024 * 1024)


def f32(*shape):
    return jax.ShapeDtypeStruct(shape, jnp.float32)


def vmem(*shape):
    return pltpu.VMEM(shape, jnp.float32)


def split_bf16(v):
    high = v.astype(jnp.bfloat16)
    low = (v - high.astype(jnp.float32)).astype(jnp.bfloat16)
    return high, low


def phase(rows, cols):
    turn = (rows * cols) % NLON
    turn = jnp.where(turn >= NLON // 2, turn - NLON, turn)
    return turn.astype(jnp.float32) * (2.0 * math.pi / NLON)


def twiddle_matrices(scale):
    shape = (HALF, 2, PEERS, INNER)
    pair = lax.broadcasted_iota(jnp.int32, shape, 0)
    mirror = lax.broadcasted_iota(jnp.int32, shape, 1)
    outer = lax.broadcasted_iota(jnp.int32, shape, 2)
    inner = lax.broadcasted_iota(jnp.int32, shape, 3)
    first = jnp.where(mirror == 0, pair, jnp.where(pair == 0, HALF, RADIX - pair))
    angle = phase(inner, first + RADIX * outer)
    c = jnp.cos(angle) * scale
    s = jnp.sin(angle) * scale
    real_only = pair == 0
    zero = jnp.zeros_like(c)
    plain = mirror == 0
    re_a = jnp.where(real_only, jnp.where(plain, c, zero), c)
    im_a = jnp.where(real_only, jnp.where(plain, -s, zero), -s)
    re_b = jnp.where(real_only, jnp.where(plain, zero, c), jnp.where(plain, s, -s))
    im_b = jnp.where(real_only, jnp.where(plain, zero, -s), jnp.where(plain, c, -c))
    re = jnp.concatenate([re_a, re_b], axis=-1)
    im = jnp.concatenate([im_a, im_b], axis=-1)
    full = jnp.stack([re, im], axis=2)
    full = full.reshape(HALF, 4 * PEERS, 2 * INNER)
    high = lax.reduce_precision(full, 8, 7)
    high, low = high.astype(jnp.bfloat16), (full - high).astype(jnp.bfloat16)
    return high, low


def fft_real16(x):
    def fft_complex8(z):
        def fft4(a):
            (ar, ai), (br, bi), (cr, ci), (dr, di) = a
            sr, si = ar + cr, ai + ci
            tr, ti = ar - cr, ai - ci
            ur, ui = br + dr, bi + di
            vr, vi = br - dr, bi - di
            return [(sr + ur, si + ui), (tr + vi, ti - vr), (sr - ur, si - ui), (tr - vi, ti + vr)]

        even = fft4(z[0::2])
        odd = fft4(z[1::2])
        h = math.sqrt(0.5)
        out = [None] * 8
        for k in range(4):
            er, ei = even[k]
            pr, pi = odd[k]
            if k == 1:
                pr, pi = (pr + pi) * h, (pi - pr) * h
            elif k == 2:
                pr, pi = pi, -pr
            elif k == 3:
                pr, pi = (pi - pr) * h, -(pr + pi) * h
            out[k] = (er + pr, ei + pi)
            out[k + 4] = (er - pr, ei - pi)
        return out

    z = fft_complex8([(x[2 * i], x[2 * i + 1]) for i in range(8)])
    out = [(z[0][0] + z[0][1], None)]
    for k in range(1, 8):
        zr, zi = z[k]
        wr, wi = z[8 - k]
        er, ei = (zr + wr) * 0.5, (zi - wi) * 0.5
        pr, pi = (zi + wi) * 0.5, (wr - zr) * 0.5
        c, s = math.cos(2 * math.pi * k / 16), math.sin(2 * math.pi * k / 16)
        out.append((er + c * pr + s * pi, ei + c * pi - s * pr))
    out.append((z[0][0] - z[0][1], None))
    return out


PAD_R = PEERS + 8


def natural_row(n2, base):
    return n2 * INNER + base


def grouped_row(n2, base):
    return ((n2 % 4) * 4 + base // LON) * INNER + (n2 // 4) * LON + base % LON


def fft_core(x_ref, wh_ref, wl_ref, y_ref, r_ref, row_of):
    def butterfly(i, carry):
        base = pl.multiple_of(i * 8, 8)
        x = [x_ref[pl.ds(pl.multiple_of(row_of(n2, base), 8), 8), :] for n2 in range(RADIX)]
        y = fft_real16(x)
        for k in range(HALF):
            parts = (y[0][0], y[HALF][0]) if k == 0 else y[k]
            for j, part in enumerate(parts):
                y_ref[k, pl.ds(j * INNER + base, 8), :] = part
        return carry

    lax.fori_loop(0, INNER // 8, butterfly, 0, unroll=4)
    for k in range(HALF):
        yh, yl = split_bf16(y_ref[k])
        two = jnp.dot(wh_ref[k], jnp.concatenate([yh, yl], axis=1), preferred_element_type=jnp.float32)
        r = two[:, :LANES] + two[:, LANES:]
        r = r + jnp.dot(wl_ref[k], yh, preferred_element_type=jnp.float32)
        mirror = HALF if k == 0 else RADIX - k
        for q, row in enumerate((k, RADIX + k, mirror, RADIX + mirror)):
            r_ref[pl.ds(row * PAD_R, PEERS), :] = r[q * PEERS : (q + 1) * PEERS]


PIECES = 4


def send_pieces(body, count, buf_ref, o_ref, sem):
    step = count // PIECES
    copies = []
    for piece in range(PIECES):
        lax.fori_loop(piece * step, (piece + 1) * step, body, 0, unroll=4)
        rows = pl.ds(piece * step, step)
        copy = pltpu.make_async_copy(buf_ref.at[rows], o_ref.at[rows], sem.at[piece])
        copy.start()
        copies.append(copy)
    for copy in copies:
        copy.wait()


FFT_SCRATCH = [
    pltpu.VMEM((HALF, 2 * INNER, LANES), jnp.float32),
    pltpu.VMEM((KEPT * PAD_R, LANES), jnp.float32),
]


def mode_rows(r_ref, k1, eight):
    return r_ref[pl.ds(eight * 8 * PAD_R + k1, 8, stride=PAD_R), :]


def fft_a_kernel(x_ref, wh_ref, wl_ref, o_ref, y_ref, r_ref, buf_ref, sem):
    fft_core(x_ref, wh_ref, wl_ref, y_ref, r_ref, grouped_row)

    def peer(k1, carry):
        for eight in range(KEPT // 8):
            buf_ref[k1, eight * 8 : eight * 8 + 8, :] = mode_rows(r_ref, k1, eight)
        return carry

    send_pieces(peer, PEERS, buf_ref, o_ref, sem)


def fft_a(gathered, wh, wl):
    return pl.pallas_call(
        fft_a_kernel,
        in_specs=[VMEM] * 3,
        out_specs=HBM,
        out_shape=pltpu.HBM((PEERS, KEPT, LANES), jnp.float32),
        scratch_shapes=FFT_SCRATCH
        + [pltpu.VMEM((PEERS, KEPT, LANES), jnp.float32), pltpu.SemaphoreType.DMA((PIECES,))],
        compiler_params=PARAMS,
        name="fft_a",
    )(gathered, wh, wl)


def fft_p_kernel(pos_ref, *refs):
    g_refs, (wh_ref, wl_ref), o_refs = refs[:8], refs[8:10], refs[10:18]
    x_ref, y_ref, r_ref = refs[18:]
    x, z, c = pos_ref[0], pos_ref[1], pos_ref[2]
    for dx in range(NX):
        for dc in range(NC):
            xx, core = (x + NX - dx) % NX, (c + dc) % NC
            for piece in range(NZ):
                zz, cc = piece_source(z, core, piece)
                row = pl.multiple_of(xx * (NLON // NX) + zz * (NC * LON) + cc * LON, LON)
                x_ref[pl.ds(row, LON), :] = g_refs[dx * NC + dc][piece * LON : (piece + 1) * LON, :]
    fft_core(x_ref, wh_ref, wl_ref, y_ref, r_ref, natural_row)
    for dz in range(NZ):
        target = (z + dz) % NZ
        for xx in range(NX):
            for cc in range(NC):
                k1 = xx * NZ * NC + target * NC + cc
                for eight in range(KEPT // 8):
                    row = (xx * NC + cc) * KEPT + eight * 8
                    o_refs[dz][row : row + 8, :] = mode_rows(r_ref, k1, eight)


def fft_p(pos, blocks, wh, wl):
    return pl.pallas_call(
        fft_p_kernel,
        in_specs=[SMEM] + [VMEM] * 10,
        out_specs=[VMEM] * NZ,
        out_shape=[vmem(NX * NC * KEPT, LANES)] * NZ,
        scratch_shapes=[pltpu.VMEM((NLON, LANES), jnp.float32)] + FFT_SCRATCH,
        compiler_params=PARAMS,
        name="fft_p",
    )(pos, *blocks, wh, wl)


GROUP = NZ * NC


STEPS = (1, 2, 3)


def start_and_wait(pairs, sem):
    copies = [pltpu.make_async_copy(source, target, sem.at[i]) for i, (source, target) in enumerate(pairs)]
    for copy in copies:
        copy.start()
    for copy in copies:
        copy.wait()


def fields_of(s_ref, target):
    field = pl.multiple_of(((target + NZ) % NZ) * 8, 8)
    return s_ref.at[:, pl.ds(field, 8), pl.ds(0, LANES)]


def split_swap_kernel(pos_ref, s_ref, swap_ref, sem):
    z, way = pos_ref[1], 1 - 2 * pos_ref[2]
    pairs = [(fields_of(s_ref, z - way * k), swap_ref.at[pl.ds(i * LON, LON)]) for i, k in enumerate(STEPS)]
    start_and_wait(pairs, sem)


def split_swap(pos, state):
    return pl.pallas_call(
        split_swap_kernel,
        in_specs=[SMEM, HBM],
        out_specs=VMEM,
        out_shape=vmem(3 * LON, 8, LANES),
        scratch_shapes=[pltpu.SemaphoreType.DMA((3,))],
        compiler_params=PARAMS,
        name="split_swap",
    )(pos, pltpu.with_memory_space_constraint(state, pltpu.HBM)).reshape(-1, LANES)


def split_rest_kernel(pos_ref, s_ref, *refs):
    stay_ref, far_ref, send_refs, part_refs, sem = refs[0], refs[1], refs[2:5], refs[5 : 5 + NX], refs[5 + NX]
    x, z, way = pos_ref[0], pos_ref[1], 1 - 2 * pos_ref[2]
    pairs = [(fields_of(s_ref, z + way * k), send_refs[i].at[pl.ds(0, LON)]) for i, k in enumerate(STEPS)]
    pairs += [(fields_of(s_ref, z + NZ // 2), far_ref), (fields_of(s_ref, z), stay_ref)]
    for dx in range(NX):
        field = pl.multiple_of(((x + dx) % NX) * GROUP, GROUP)
        pairs.append((s_ref.at[:, pl.ds(field, GROUP), pl.ds(LANES, LANES)], part_refs[dx]))
    start_and_wait(pairs, sem)


def split_rest(pos, state):
    out = pl.pallas_call(
        split_rest_kernel,
        in_specs=[SMEM, HBM],
        out_specs=[VMEM] * (5 + NX),
        out_shape=[vmem(LON, 8, LANES)] * 2 + [vmem(2 * LON, 8, LANES)] * 3 + [vmem(LON, GROUP, LANES)] * NX,
        scratch_shapes=[pltpu.SemaphoreType.DMA((5 + NX,))],
        compiler_params=PARAMS,
        name="split_rest",
    )(pos, pltpu.with_memory_space_constraint(state, pltpu.HBM))
    return [v.reshape(-1, LANES) for v in out[:5]], out[5:]


BLOCK = 256


def merge_kernel(swap_ref, *refs):
    o_refs, sem = refs[3:6], refs[6]
    copies = [
        pltpu.make_async_copy(swap_ref.at[pl.ds(i * BLOCK, BLOCK)], o_refs[i].at[pl.ds(BLOCK, BLOCK)], sem.at[i])
        for i in range(3)
    ]
    for copy in copies:
        copy.start()
    for copy in copies:
        copy.wait()


def merge(swap, sends):
    anywhere = pl.BlockSpec(memory_space=pl.ANY)
    return pl.pallas_call(
        merge_kernel,
        in_specs=[anywhere] * 4,
        out_specs=[anywhere] * 3,
        out_shape=[f32(2 * BLOCK, LANES)] * 3,
        scratch_shapes=[pltpu.SemaphoreType.DMA((3,))],
        input_output_aliases={1: 0, 2: 1, 3: 2},
        compiler_params=PARAMS,
        name="merge",
    )(swap, *sends)


def piece_of(refs, piece):
    if piece < 2:
        return refs[piece], 0
    return refs[1 + piece // 2], (piece % 2) * BLOCK


def piece_source(z, core, piece):
    if piece == 0:
        return z, core
    if piece == 1:
        return (z + NZ // 2) % NZ, core
    way = 1 - 2 * core
    return (z - way * (piece // 2) + NZ) % NZ, core if piece % 2 == 0 else 1 - core


def spread_x_kernel(pos_ref, *refs):
    b_refs, o_refs = refs[:5], refs[5:]
    x, c = pos_ref[0], pos_ref[2]
    for dx in range(NX):
        for dc in range(NC):
            field = ((x + dx) % NX) * NC + (c + dc) % NC
            for piece in range(NZ):
                ref, row = piece_of(b_refs, piece)
                o_refs[dx * NC + dc][piece * LON : (piece + 1) * LON, :] = ref[pl.ds(row + field, LON, stride=8), :]


def spread_x(pos, blocks):
    return pl.pallas_call(
        spread_x_kernel,
        in_specs=[SMEM] + [VMEM] * 5,
        out_specs=[VMEM] * (NX * NC),
        out_shape=[vmem(NZ * LON, LANES)] * (NX * NC),
        compiler_params=PARAMS,
        name="spread_x",
    )(pos, *blocks)


def spread_out_kernel(pos_ref, *refs):
    h_refs, o_refs = refs[:NZ], refs[NZ:]
    x, z, c = pos_ref[0], pos_ref[1], pos_ref[2]
    for dx in range(NX):
        for dc in range(NC):
            source = pl.multiple_of((((x + dx) % NX) * NC + (c + dc) % NC) * KEPT, KEPT)
            for dz in range(NZ):
                row = pl.multiple_of(((z + NZ - dz) % NZ) * KEPT, KEPT)
                o_refs[dx * NC + dc][pl.ds(row, KEPT), :] = h_refs[dz][pl.ds(source, KEPT), :]


def spread_out(pos, blocks):
    return pl.pallas_call(
        spread_out_kernel,
        in_specs=[SMEM] + [VMEM] * NZ,
        out_specs=[VMEM] * (NX * NC),
        out_shape=[vmem(NZ * KEPT, LANES)] * (NX * NC),
        compiler_params=PARAMS,
        name="spread_out",
    )(pos, *blocks)


def spread_a_kernel(pos_ref, *refs):
    b_refs, o_ref, buf_ref, sem = refs[:NX], refs[NX], refs[NX + 1], refs[NX + 2]
    x = pos_ref[0]

    def field(f, carry):
        for dx in range(NX):
            row = pl.multiple_of(((x + NX - dx) % NX) * LON, LON)
            buf_ref[f, pl.ds(row, LON), :] = b_refs[dx][pl.ds(f, LON, stride=GROUP), :]
        return carry

    send_pieces(field, GROUP, buf_ref, o_ref, sem)


def spread_a(pos, blocks):
    return pl.pallas_call(
        spread_a_kernel,
        in_specs=[SMEM] + [VMEM] * NX,
        out_specs=HBM,
        out_shape=pltpu.HBM((GROUP, NX * LON, LANES), jnp.float32),
        scratch_shapes=[
            pltpu.VMEM((GROUP, NX * LON, LANES), jnp.float32),
            pltpu.SemaphoreType.DMA((PIECES,)),
        ],
        compiler_params=PARAMS,
        name="spread_a",
    )(pos, *blocks)


PAD_K = KEPT + 8


def store_half(x_ref, buf_ref, o_ref, sem, lane):
    copies = []
    step = KEPT // PIECES
    for piece in range(PIECES):
        for kept in range(piece * step, (piece + 1) * step):
            for eight in range(FIELDS // 8):
                buf_ref[kept, eight * 8 : eight * 8 + 8, :] = x_ref[pl.ds(eight * 8 * PAD_K + kept, 8, stride=PAD_K), :]
        copy = pltpu.make_async_copy(
            buf_ref.at[pl.ds(piece * step, step)],
            o_ref.at[pl.ds(piece * step, step), :, pl.ds(lane, LANES)],
            sem.at[piece],
        )
        copy.start()
        copies.append(copy)
    for copy in copies:
        copy.wait()


STORE_SCRATCH = [
    pltpu.VMEM((FIELDS * PAD_K, LANES), jnp.float32),
    pltpu.VMEM((KEPT, FIELDS, LANES), jnp.float32),
    pltpu.SemaphoreType.DMA((PIECES,)),
]


def store_p_kernel(pos_ref, prior_ref, *refs):
    del prior_ref
    q_refs, o_ref = refs[:8], refs[8]
    x_ref, buf_ref, sem = refs[9:]
    x, c = pos_ref[0], pos_ref[2]
    for dx in range(NX):
        for dc in range(NC):
            base = ((x + NX - dx) % NX) * NC + (c + dc) % NC
            for zz in range(NZ):
                row = pl.multiple_of((base + zz * NX * NC) * PAD_K, 8)
                x_ref[pl.ds(row, KEPT), :] = q_refs[dx * NC + dc][zz * KEPT : (zz + 1) * KEPT, :]
    store_half(x_ref, buf_ref, o_ref, sem, 0)


def store_p(pos, prior, blocks):
    return pl.pallas_call(
        store_p_kernel,
        in_specs=[SMEM, HBM] + [VMEM] * 8,
        out_specs=HBM,
        out_shape=f32(KEPT, FIELDS, 2 * LANES),
        scratch_shapes=STORE_SCRATCH,
        input_output_aliases={1: 0},
        compiler_params=PARAMS,
        name="store_p",
    )(pos, prior, *blocks)


def store_a_kernel(q_ref, o_ref, x_ref, buf_ref, sem):
    def field(f, carry):
        x_ref[pl.ds(pl.multiple_of(f * PAD_K, 8), KEPT), :] = q_ref[f]
        return carry

    lax.fori_loop(0, FIELDS, field, 0, unroll=8)
    store_half(x_ref, buf_ref, o_ref, sem, LANES)


def store_a(shares):
    return pl.pallas_call(
        store_a_kernel,
        in_specs=[VMEM],
        out_specs=HBM,
        out_shape=f32(KEPT, FIELDS, 2 * LANES),
        scratch_shapes=STORE_SCRATCH,
        compiler_params=PARAMS,
        name="store_a",
    )(shares)


def shifts(dx, dz, dc):
    def at(x, z, c):
        return (x % NX) * NZ * NC + (z % NZ) * NC + c % NC

    return [
        (at(x, z, c), at(x + dx, z + dz, c + dc)) for x in range(NX) for z in range(NZ) for c in range(NC)
    ]


def two_ways(k):
    return [
        pair
        for c in range(NC)
        for pair in shifts(0, k if c == 0 else NZ - k, 0)
        if pair[0] % NC == c
    ]


Z_IN = (3, 4, 2, 1)
Z_OUT = (1, 7, 4, 3, 5, 2, 6)


def exchange_z_in(blocks, swap):
    stay, far, sends = blocks[0], blocks[1], blocks[2:5]
    sends = merge(swap, sends)
    got = {}
    for k in Z_IN:
        block = far if k == NZ // 2 else sends[k - 1]
        got[k] = lax.ppermute(block, "lon", two_ways(k))
    return [stay, got[NZ // 2], *(got[k] for k in STEPS)]


def exchange_z_out(blocks):
    out = [None] * NZ
    out[0] = blocks[0]
    for dz in Z_OUT:
        out[dz] = lax.ppermute(blocks[dz], "lon", shifts(0, dz, 0))
    return out


AX_ORDER = (2, 1, 3)
GROUPS = [[x * GROUP + g for g in range(GROUP)] for x in range(NX)]


def exchange_x(blocks):
    out = [None] * NX
    out[0] = blocks[0]
    for dx in AX_ORDER:
        out[dx] = lax.ppermute(blocks[dx], "lon", shifts(dx, 0, 0))
    return out


X_ORDER = ((2, 0), (2, 1), (1, 0), (3, 0), (1, 1), (3, 1), (0, 1))


def exchange_xc(blocks):
    out = [None] * (NX * NC)
    out[0] = blocks[0]
    for dx, dc in X_ORDER:
        out[dx * NC + dc] = lax.ppermute(blocks[dx * NC + dc], "lon", shifts(dx, 0, dc))
    return out


def local(state):
    device = lax.axis_index("lon")
    pos = jnp.stack([device // (NZ * NC), (device // NC) % NZ, device % NC]).astype(jnp.int32)
    wh, wl = twiddle_matrices(1.0 / math.sqrt(NLON))
    swap = split_swap(pos, state)
    swap = lax.ppermute(swap, "lon", shifts(0, 0, 1))
    pieces, parts = split_rest(pos, state)
    pieces = exchange_z_in(pieces, swap)
    parts = exchange_x(parts)
    sent = spread_a(pos, [b.reshape(LON * GROUP, LANES) for b in parts])
    gathered = lax.all_to_all(
        sent, "lon", split_axis=0, concat_axis=0, axis_index_groups=GROUPS, tiled=True
    )
    pieces = spread_x(pos, pieces)
    pieces = exchange_xc(pieces)
    pieces = fft_p(pos, pieces, wh, wl)
    pieces = exchange_z_out(pieces)
    spectrum = fft_a(gathered.reshape(NLON, LANES), wh, wl)
    shares = lax.all_to_all(spectrum, "lon", split_axis=0, concat_axis=0, tiled=True)
    pieces = spread_out(pos, pieces)
    pieces = exchange_xc(pieces)
    out = store_a(shares)
    out = store_p(pos, out, pieces)
    return out.reshape(2, RADIX, FIELDS, 2 * LANES)


def solution(mesh):
    return jax.shard_map(
        local,
        mesh=mesh,
        in_specs=(P("lon", None, "lat"),),
        out_specs=P(None, "lon", None, "lat"),
        check_vma=False,
    )
```

```python
import math

import jax
import jax.numpy as jnp
from jax import lax
from jax.experimental import pallas as pl
from jax.experimental.pallas import tpu as pltpu
from jax.sharding import PartitionSpec as P


NLON = 2048
RADIX = 16
INNER = NLON // RADIX
PEERS = 64
HALF = RADIX // 2
NX, NZ, NC = 4, 8, 2
LON = 32
KEPT = 2 * RADIX
FIELDS = 64
LANES = 128
VMEM = pl.BlockSpec(memory_space=pltpu.VMEM)
HBM = pl.BlockSpec(memory_space=pltpu.HBM)
SMEM = pl.BlockSpec(memory_space=pltpu.SMEM)
PARAMS = pltpu.CompilerParams(vmem_limit_bytes=16 * 1024 * 1024)


def f32(*shape):
    return jax.ShapeDtypeStruct(shape, jnp.float32)


def vmem(*shape):
    return pltpu.VMEM(shape, jnp.float32)


def split_bf16(v):
    high = v.astype(jnp.bfloat16)
    low = (v - high.astype(jnp.float32)).astype(jnp.bfloat16)
    return high, low


def phase(rows, cols):
    turn = (rows * cols) % NLON
    turn = jnp.where(turn >= NLON // 2, turn - NLON, turn)
    return turn.astype(jnp.float32) * (2.0 * math.pi / NLON)


def twiddle_matrices(scale):
    shape = (HALF, 2, PEERS, INNER)
    pair = lax.broadcasted_iota(jnp.int32, shape, 0)
    mirror = lax.broadcasted_iota(jnp.int32, shape, 1)
    outer = lax.broadcasted_iota(jnp.int32, shape, 2)
    inner = lax.broadcasted_iota(jnp.int32, shape, 3)
    first = jnp.where(mirror == 0, pair, jnp.where(pair == 0, HALF, RADIX - pair))
    angle = phase(inner, first + RADIX * outer)
    c = jnp.cos(angle) * scale
    s = jnp.sin(angle) * scale
    real_only = pair == 0
    zero = jnp.zeros_like(c)
    plain = mirror == 0
    re_a = jnp.where(real_only, jnp.where(plain, c, zero), c)
    im_a = jnp.where(real_only, jnp.where(plain, -s, zero), -s)
    re_b = jnp.where(real_only, jnp.where(plain, zero, c), jnp.where(plain, s, -s))
    im_b = jnp.where(real_only, jnp.where(plain, zero, -s), jnp.where(plain, c, -c))
    re = jnp.concatenate([re_a, re_b], axis=-1)
    im = jnp.concatenate([im_a, im_b], axis=-1)
    full = jnp.stack([re, im], axis=2)
    full = full.reshape(HALF, 4 * PEERS, 2 * INNER)
    high = lax.reduce_precision(full, 8, 7)
    high, low = high.astype(jnp.bfloat16), (full - high).astype(jnp.bfloat16)
    return high, low


def fft_real16(x):
    def fft_complex8(z):
        def fft4(a):
            (ar, ai), (br, bi), (cr, ci), (dr, di) = a
            sr, si = ar + cr, ai + ci
            tr, ti = ar - cr, ai - ci
            ur, ui = br + dr, bi + di
            vr, vi = br - dr, bi - di
            return [(sr + ur, si + ui), (tr + vi, ti - vr), (sr - ur, si - ui), (tr - vi, ti + vr)]

        even = fft4(z[0::2])
        odd = fft4(z[1::2])
        h = math.sqrt(0.5)
        out = [None] * 8
        for k in range(4):
            er, ei = even[k]
            pr, pi = odd[k]
            if k == 1:
                pr, pi = (pr + pi) * h, (pi - pr) * h
            elif k == 2:
                pr, pi = pi, -pr
            elif k == 3:
                pr, pi = (pi - pr) * h, -(pr + pi) * h
            out[k] = (er + pr, ei + pi)
            out[k + 4] = (er - pr, ei - pi)
        return out

    z = fft_complex8([(x[2 * i], x[2 * i + 1]) for i in range(8)])
    out = [(z[0][0] + z[0][1], None)]
    for k in range(1, 8):
        zr, zi = z[k]
        wr, wi = z[8 - k]
        er, ei = (zr + wr) * 0.5, (zi - wi) * 0.5
        pr, pi = (zi + wi) * 0.5, (wr - zr) * 0.5
        c, s = math.cos(2 * math.pi * k / 16), math.sin(2 * math.pi * k / 16)
        out.append((er + c * pr + s * pi, ei + c * pi - s * pr))
    out.append((z[0][0] - z[0][1], None))
    return out


PAD_R = PEERS + 8


def natural_row(n2, base):
    return n2 * INNER + base


def grouped_row(n2, base):
    return ((n2 % 4) * 4 + base // LON) * INNER + (n2 // 4) * LON + base % LON


def fft_core(x_ref, wh_ref, wl_ref, y_ref, r_ref, row_of):
    def butterfly(i, carry):
        base = pl.multiple_of(i * 8, 8)
        x = [x_ref[pl.ds(pl.multiple_of(row_of(n2, base), 8), 8), :] for n2 in range(RADIX)]
        y = fft_real16(x)
        for k in range(HALF):
            parts = (y[0][0], y[HALF][0]) if k == 0 else y[k]
            for j, part in enumerate(parts):
                y_ref[k, pl.ds(j * INNER + base, 8), :] = part
        return carry

    lax.fori_loop(0, INNER // 8, butterfly, 0, unroll=4)
    for k in range(HALF):
        yh, yl = split_bf16(y_ref[k])
        two = jnp.dot(wh_ref[k], jnp.concatenate([yh, yl], axis=1), preferred_element_type=jnp.float32)
        r = two[:, :LANES] + two[:, LANES:]
        r = r + jnp.dot(wl_ref[k], yh, preferred_element_type=jnp.float32)
        mirror = HALF if k == 0 else RADIX - k
        for q, row in enumerate((k, RADIX + k, mirror, RADIX + mirror)):
            r_ref[pl.ds(row * PAD_R, PEERS), :] = r[q * PEERS : (q + 1) * PEERS]


PIECES = 4


def send_pieces(body, count, buf_ref, o_ref, sem):
    step = count // PIECES
    copies = []
    for piece in range(PIECES):
        lax.fori_loop(piece * step, (piece + 1) * step, body, 0, unroll=4)
        rows = pl.ds(piece * step, step)
        copy = pltpu.make_async_copy(buf_ref.at[rows], o_ref.at[rows], sem.at[piece])
        copy.start()
        copies.append(copy)
    for copy in copies:
        copy.wait()


FFT_SCRATCH = [
    pltpu.VMEM((HALF, 2 * INNER, LANES), jnp.float32),
    pltpu.VMEM((KEPT * PAD_R, LANES), jnp.float32),
]


def mode_rows(r_ref, k1, eight):
    return r_ref[pl.ds(eight * 8 * PAD_R + k1, 8, stride=PAD_R), :]


def fft_a_kernel(x_ref, wh_ref, wl_ref, o_ref, y_ref, r_ref, buf_ref, sem):
    fft_core(x_ref, wh_ref, wl_ref, y_ref, r_ref, grouped_row)

    def peer(k1, carry):
        for eight in range(KEPT // 8):
            buf_ref[k1, eight * 8 : eight * 8 + 8, :] = mode_rows(r_ref, k1, eight)
        return carry

    send_pieces(peer, PEERS, buf_ref, o_ref, sem)


def fft_a(gathered, wh, wl):
    return pl.pallas_call(
        fft_a_kernel,
        in_specs=[VMEM] * 3,
        out_specs=HBM,
        out_shape=pltpu.HBM((PEERS, KEPT, LANES), jnp.float32),
        scratch_shapes=FFT_SCRATCH
        + [pltpu.VMEM((PEERS, KEPT, LANES), jnp.float32), pltpu.SemaphoreType.DMA((PIECES,))],
        compiler_params=PARAMS,
        name="fft_a",
    )(gathered, wh, wl)


def fft_p_kernel(pos_ref, *refs):
    g_refs, (wh_ref, wl_ref), o_refs = refs[:8], refs[8:10], refs[10:18]
    x_ref, y_ref, r_ref = refs[18:]
    x, z, c = pos_ref[0], pos_ref[1], pos_ref[2]
    for dx in range(NX):
        for dc in range(NC):
            start = ((x + NX - dx) % NX) * (NLON // NX) + ((c + dc) % NC) * LON
            for zz in range(NZ):
                row = pl.multiple_of(start + zz * NC * LON, LON)
                x_ref[pl.ds(row, LON), :] = g_refs[dx * NC + dc][zz * LON : (zz + 1) * LON, :]
    fft_core(x_ref, wh_ref, wl_ref, y_ref, r_ref, natural_row)
    for dz in range(NZ):
        target = (z + dz) % NZ
        for xx in range(NX):
            for cc in range(NC):
                k1 = xx * NZ * NC + target * NC + cc
                for eight in range(KEPT // 8):
                    row = (xx * NC + cc) * KEPT + eight * 8
                    o_refs[dz][row : row + 8, :] = mode_rows(r_ref, k1, eight)


def fft_p(pos, blocks, wh, wl):
    return pl.pallas_call(
        fft_p_kernel,
        in_specs=[SMEM] + [VMEM] * 10,
        out_specs=[VMEM] * NZ,
        out_shape=[vmem(NX * NC * KEPT, LANES)] * NZ,
        scratch_shapes=[pltpu.VMEM((NLON, LANES), jnp.float32)] + FFT_SCRATCH,
        compiler_params=PARAMS,
        name="fft_p",
    )(pos, *blocks, wh, wl)


GROUP = NZ * NC


def split_kernel(pos_ref, s_ref, *refs):
    o_refs, sem = refs[: NZ + NX], refs[NZ + NX]
    x, z = pos_ref[0], pos_ref[1]
    copies = []
    for dz in range(NZ):
        field = pl.multiple_of(((z + dz) % NZ) * 8, 8)
        source = s_ref.at[:, pl.ds(field, 8), pl.ds(0, LANES)]
        copies.append(pltpu.make_async_copy(source, o_refs[dz], sem.at[dz]))
    for dx in range(NX):
        field = pl.multiple_of(((x + dx) % NX) * GROUP, GROUP)
        source = s_ref.at[:, pl.ds(field, GROUP), pl.ds(LANES, LANES)]
        copies.append(pltpu.make_async_copy(source, o_refs[NZ + dx], sem.at[NZ + dx]))
    for copy in copies:
        copy.start()
    for copy in copies:
        copy.wait()


def split(pos, state):
    out = pl.pallas_call(
        split_kernel,
        in_specs=[SMEM, HBM],
        out_specs=[VMEM] * (NZ + NX),
        out_shape=[vmem(LON, 8, LANES)] * NZ + [vmem(LON, GROUP, LANES)] * NX,
        scratch_shapes=[pltpu.SemaphoreType.DMA((NZ + NX,))],
        compiler_params=PARAMS,
        name="split",
    )(pos, pltpu.with_memory_space_constraint(state, pltpu.HBM))
    return out[:NZ], out[NZ:]


def spread_x_kernel(pos_ref, *refs):
    b_refs, o_refs = refs[:NZ], refs[NZ:]
    x, z, c = pos_ref[0], pos_ref[1], pos_ref[2]
    for dx in range(NX):
        for dc in range(NC):
            field = ((x + dx) % NX) * NC + (c + dc) % NC
            for dz in range(NZ):
                row = pl.multiple_of(((z + NZ - dz) % NZ) * LON, LON)
                o_refs[dx * NC + dc][pl.ds(row, LON), :] = b_refs[dz][pl.ds(field, LON, stride=8), :]


def spread_x(pos, blocks):
    return pl.pallas_call(
        spread_x_kernel,
        in_specs=[SMEM] + [VMEM] * NZ,
        out_specs=[VMEM] * (NX * NC),
        out_shape=[vmem(NZ * LON, LANES)] * (NX * NC),
        compiler_params=PARAMS,
        name="spread_x",
    )(pos, *blocks)


def spread_out_kernel(pos_ref, *refs):
    h_refs, o_refs = refs[:NZ], refs[NZ:]
    x, z, c = pos_ref[0], pos_ref[1], pos_ref[2]
    for dx in range(NX):
        for dc in range(NC):
            source = pl.multiple_of((((x + dx) % NX) * NC + (c + dc) % NC) * KEPT, KEPT)
            for dz in range(NZ):
                row = pl.multiple_of(((z + NZ - dz) % NZ) * KEPT, KEPT)
                o_refs[dx * NC + dc][pl.ds(row, KEPT), :] = h_refs[dz][pl.ds(source, KEPT), :]


def spread_out(pos, blocks):
    return pl.pallas_call(
        spread_out_kernel,
        in_specs=[SMEM] + [VMEM] * NZ,
        out_specs=[VMEM] * (NX * NC),
        out_shape=[vmem(NZ * KEPT, LANES)] * (NX * NC),
        compiler_params=PARAMS,
        name="spread_out",
    )(pos, *blocks)


def spread_a_kernel(pos_ref, *refs):
    b_refs, o_ref, buf_ref, sem = refs[:NX], refs[NX], refs[NX + 1], refs[NX + 2]
    x = pos_ref[0]

    def field(f, carry):
        for dx in range(NX):
            row = pl.multiple_of(((x + NX - dx) % NX) * LON, LON)
            buf_ref[f, pl.ds(row, LON), :] = b_refs[dx][pl.ds(f, LON, stride=GROUP), :]
        return carry

    send_pieces(field, GROUP, buf_ref, o_ref, sem)


def spread_a(pos, blocks):
    return pl.pallas_call(
        spread_a_kernel,
        in_specs=[SMEM] + [VMEM] * NX,
        out_specs=HBM,
        out_shape=pltpu.HBM((GROUP, NX * LON, LANES), jnp.float32),
        scratch_shapes=[
            pltpu.VMEM((GROUP, NX * LON, LANES), jnp.float32),
            pltpu.SemaphoreType.DMA((PIECES,)),
        ],
        compiler_params=PARAMS,
        name="spread_a",
    )(pos, *blocks)


PAD_K = KEPT + 8


def store_half(x_ref, buf_ref, o_ref, sem, lane):
    copies = []
    step = KEPT // PIECES
    for piece in range(PIECES):
        for kept in range(piece * step, (piece + 1) * step):
            for eight in range(FIELDS // 8):
                buf_ref[kept, eight * 8 : eight * 8 + 8, :] = x_ref[pl.ds(eight * 8 * PAD_K + kept, 8, stride=PAD_K), :]
        copy = pltpu.make_async_copy(
            buf_ref.at[pl.ds(piece * step, step)],
            o_ref.at[pl.ds(piece * step, step), :, pl.ds(lane, LANES)],
            sem.at[piece],
        )
        copy.start()
        copies.append(copy)
    for copy in copies:
        copy.wait()


STORE_SCRATCH = [
    pltpu.VMEM((FIELDS * PAD_K, LANES), jnp.float32),
    pltpu.VMEM((KEPT, FIELDS, LANES), jnp.float32),
    pltpu.SemaphoreType.DMA((PIECES,)),
]


def store_p_kernel(pos_ref, prior_ref, *refs):
    del prior_ref
    q_refs, o_ref = refs[:8], refs[8]
    x_ref, buf_ref, sem = refs[9:]
    x, c = pos_ref[0], pos_ref[2]
    for dx in range(NX):
        for dc in range(NC):
            base = ((x + NX - dx) % NX) * NC + (c + dc) % NC
            for zz in range(NZ):
                row = pl.multiple_of((base + zz * NX * NC) * PAD_K, 8)
                x_ref[pl.ds(row, KEPT), :] = q_refs[dx * NC + dc][zz * KEPT : (zz + 1) * KEPT, :]
    store_half(x_ref, buf_ref, o_ref, sem, 0)


def store_p(pos, prior, blocks):
    return pl.pallas_call(
        store_p_kernel,
        in_specs=[SMEM, HBM] + [VMEM] * 8,
        out_specs=HBM,
        out_shape=f32(KEPT, FIELDS, 2 * LANES),
        scratch_shapes=STORE_SCRATCH,
        input_output_aliases={1: 0},
        compiler_params=PARAMS,
        name="store_p",
    )(pos, prior, *blocks)


def store_a_kernel(q_ref, o_ref, x_ref, buf_ref, sem):
    def field(f, carry):
        x_ref[pl.ds(pl.multiple_of(f * PAD_K, 8), KEPT), :] = q_ref[f]
        return carry

    lax.fori_loop(0, FIELDS, field, 0, unroll=8)
    store_half(x_ref, buf_ref, o_ref, sem, LANES)


def store_a(shares):
    return pl.pallas_call(
        store_a_kernel,
        in_specs=[VMEM],
        out_specs=HBM,
        out_shape=f32(KEPT, FIELDS, 2 * LANES),
        scratch_shapes=STORE_SCRATCH,
        compiler_params=PARAMS,
        name="store_a",
    )(shares)


def shifts(dx, dz, dc):
    def at(x, z, c):
        return (x % NX) * NZ * NC + (z % NZ) * NC + c % NC

    return [
        (at(x, z, c), at(x + dx, z + dz, c + dc)) for x in range(NX) for z in range(NZ) for c in range(NC)
    ]


Z_ORDER = (1, 7, 4, 3, 5, 2, 6)


def exchange_z(blocks):
    out = [None] * NZ
    out[0] = blocks[0]
    for dz in Z_ORDER:
        out[dz] = lax.ppermute(blocks[dz], "lon", shifts(0, dz, 0))
    return out


AX_ORDER = (1, 3, 2)
GROUPS = [[x * GROUP + g for g in range(GROUP)] for x in range(NX)]


def exchange_x(blocks):
    out = [None] * NX
    out[0] = blocks[0]
    for dx in AX_ORDER:
        out[dx] = lax.ppermute(blocks[dx], "lon", shifts(dx, 0, 0))
    return out


X_ORDER = ((1, 0), (3, 0), (2, 0), (2, 1), (1, 1), (3, 1), (0, 1))


def exchange_xc(blocks):
    out = [None] * (NX * NC)
    out[0] = blocks[0]
    for dx, dc in X_ORDER:
        out[dx * NC + dc] = lax.ppermute(blocks[dx * NC + dc], "lon", shifts(dx, 0, dc))
    return out


def local(state):
    device = lax.axis_index("lon")
    pos = jnp.stack([device // (NZ * NC), (device // NC) % NZ, device % NC]).astype(jnp.int32)
    wh, wl = twiddle_matrices(1.0 / math.sqrt(NLON))
    pieces, parts = split(pos, state)
    pieces = exchange_z(pieces)
    parts = exchange_x(parts)
    sent = spread_a(pos, [b.reshape(LON * GROUP, LANES) for b in parts])
    gathered = lax.all_to_all(
        sent, "lon", split_axis=0, concat_axis=0, axis_index_groups=GROUPS, tiled=True
    )
    pieces = spread_x(pos, [b.reshape(LON * 8, LANES) for b in pieces])
    pieces = exchange_xc(pieces)
    pieces = fft_p(pos, pieces, wh, wl)
    pieces = exchange_z(pieces)
    spectrum = fft_a(gathered.reshape(NLON, LANES), wh, wl)
    shares = lax.all_to_all(spectrum, "lon", split_axis=0, concat_axis=0, tiled=True)
    pieces = spread_out(pos, pieces)
    pieces = exchange_xc(pieces)
    out = store_a(shares)
    out = store_p(pos, out, pieces)
    return out.reshape(2, RADIX, FIELDS, 2 * LANES)


def solution(mesh):
    return jax.shard_map(
        local,
        mesh=mesh,
        in_specs=(P("lon", None, "lat"),),
        out_specs=P(None, "lon", None, "lat"),
        check_vma=False,
    )
```

```python
import math

import jax
import jax.numpy as jnp
from jax import lax
from jax.experimental import pallas as pl
from jax.experimental.pallas import tpu as pltpu
from jax.sharding import PartitionSpec as P


NLON = 2048
RADIX = 16
INNER = NLON // RADIX
PEERS = 64
HALF = RADIX // 2
NX, NZ, NC = 4, 8, 2
LON = 32
KEPT = 2 * RADIX
FIELDS = 64
LANES = 128
VMEM = pl.BlockSpec(memory_space=pltpu.VMEM)
HBM = pl.BlockSpec(memory_space=pltpu.HBM)
SMEM = pl.BlockSpec(memory_space=pltpu.SMEM)
PARAMS = pltpu.CompilerParams(vmem_limit_bytes=16 * 1024 * 1024)


def f32(*shape):
    return jax.ShapeDtypeStruct(shape, jnp.float32)


def vmem(*shape):
    return pltpu.VMEM(shape, jnp.float32)


def split_bf16(v):
    high = v.astype(jnp.bfloat16)
    low = (v - high.astype(jnp.float32)).astype(jnp.bfloat16)
    return high, low


def phase(rows, cols):
    turn = (rows * cols) % NLON
    turn = jnp.where(turn >= NLON // 2, turn - NLON, turn)
    return turn.astype(jnp.float32) * (2.0 * math.pi / NLON)


def twiddle_matrices(scale):
    shape = (HALF, 2, PEERS, INNER)
    pair = lax.broadcasted_iota(jnp.int32, shape, 0)
    mirror = lax.broadcasted_iota(jnp.int32, shape, 1)
    outer = lax.broadcasted_iota(jnp.int32, shape, 2)
    inner = lax.broadcasted_iota(jnp.int32, shape, 3)
    first = jnp.where(mirror == 0, pair, jnp.where(pair == 0, HALF, RADIX - pair))
    angle = phase(inner, first + RADIX * outer)
    c = jnp.cos(angle) * scale
    s = jnp.sin(angle) * scale
    real_only = pair == 0
    zero = jnp.zeros_like(c)
    plain = mirror == 0
    re_a = jnp.where(real_only, jnp.where(plain, c, zero), c)
    im_a = jnp.where(real_only, jnp.where(plain, -s, zero), -s)
    re_b = jnp.where(real_only, jnp.where(plain, zero, c), jnp.where(plain, s, -s))
    im_b = jnp.where(real_only, jnp.where(plain, zero, -s), jnp.where(plain, c, -c))
    re = jnp.concatenate([re_a, re_b], axis=-1)
    im = jnp.concatenate([im_a, im_b], axis=-1)
    full = jnp.stack([re, im], axis=2)
    full = full.reshape(HALF, 4 * PEERS, 2 * INNER)
    high = lax.reduce_precision(full, 8, 7)
    high, low = high.astype(jnp.bfloat16), (full - high).astype(jnp.bfloat16)
    return high, low


def fft_real16(x):
    def fft_complex8(z):
        def fft4(a):
            (ar, ai), (br, bi), (cr, ci), (dr, di) = a
            sr, si = ar + cr, ai + ci
            tr, ti = ar - cr, ai - ci
            ur, ui = br + dr, bi + di
            vr, vi = br - dr, bi - di
            return [(sr + ur, si + ui), (tr + vi, ti - vr), (sr - ur, si - ui), (tr - vi, ti + vr)]

        even = fft4(z[0::2])
        odd = fft4(z[1::2])
        h = math.sqrt(0.5)
        out = [None] * 8
        for k in range(4):
            er, ei = even[k]
            pr, pi = odd[k]
            if k == 1:
                pr, pi = (pr + pi) * h, (pi - pr) * h
            elif k == 2:
                pr, pi = pi, -pr
            elif k == 3:
                pr, pi = (pi - pr) * h, -(pr + pi) * h
            out[k] = (er + pr, ei + pi)
            out[k + 4] = (er - pr, ei - pi)
        return out

    z = fft_complex8([(x[2 * i], x[2 * i + 1]) for i in range(8)])
    out = [(z[0][0] + z[0][1], None)]
    for k in range(1, 8):
        zr, zi = z[k]
        wr, wi = z[8 - k]
        er, ei = (zr + wr) * 0.5, (zi - wi) * 0.5
        pr, pi = (zi + wi) * 0.5, (wr - zr) * 0.5
        c, s = math.cos(2 * math.pi * k / 16), math.sin(2 * math.pi * k / 16)
        out.append((er + c * pr + s * pi, ei + c * pi - s * pr))
    out.append((z[0][0] - z[0][1], None))
    return out


PAD_R = PEERS + 8


def natural_row(n2, base):
    return n2 * INNER + base


def grouped_row(n2, base):
    return ((n2 % 4) * 4 + base // LON) * INNER + (n2 // 4) * LON + base % LON


def fft_core(x_ref, wh_ref, wl_ref, y_ref, r_ref, row_of):
    def butterfly(i, carry):
        base = pl.multiple_of(i * 8, 8)
        x = [x_ref[pl.ds(pl.multiple_of(row_of(n2, base), 8), 8), :] for n2 in range(RADIX)]
        y = fft_real16(x)
        for k in range(HALF):
            parts = (y[0][0], y[HALF][0]) if k == 0 else y[k]
            for j, part in enumerate(parts):
                y_ref[k, pl.ds(j * INNER + base, 8), :] = part
        return carry

    lax.fori_loop(0, INNER // 8, butterfly, 0, unroll=4)
    for k in range(HALF):
        yh, yl = split_bf16(y_ref[k])
        two = jnp.dot(wh_ref[k], jnp.concatenate([yh, yl], axis=1), preferred_element_type=jnp.float32)
        r = two[:, :LANES] + two[:, LANES:]
        r = r + jnp.dot(wl_ref[k], yh, preferred_element_type=jnp.float32)
        mirror = HALF if k == 0 else RADIX - k
        for q, row in enumerate((k, RADIX + k, mirror, RADIX + mirror)):
            r_ref[pl.ds(row * PAD_R, PEERS), :] = r[q * PEERS : (q + 1) * PEERS]


PIECES = 4


def send_pieces(body, count, buf_ref, o_ref, sem):
    step = count // PIECES
    copies = []
    for piece in range(PIECES):
        lax.fori_loop(piece * step, (piece + 1) * step, body, 0, unroll=4)
        rows = pl.ds(piece * step, step)
        copy = pltpu.make_async_copy(buf_ref.at[rows], o_ref.at[rows], sem.at[piece])
        copy.start()
        copies.append(copy)
    for copy in copies:
        copy.wait()


FFT_SCRATCH = [
    pltpu.VMEM((HALF, 2 * INNER, LANES), jnp.float32),
    pltpu.VMEM((KEPT * PAD_R, LANES), jnp.float32),
]


def mode_rows(r_ref, k1, eight):
    return r_ref[pl.ds(eight * 8 * PAD_R + k1, 8, stride=PAD_R), :]


def fft_a_kernel(x_ref, wh_ref, wl_ref, o_ref, y_ref, r_ref, buf_ref, sem):
    fft_core(x_ref, wh_ref, wl_ref, y_ref, r_ref, grouped_row)

    def peer(k1, carry):
        for eight in range(KEPT // 8):
            buf_ref[k1, eight * 8 : eight * 8 + 8, :] = mode_rows(r_ref, k1, eight)
        return carry

    send_pieces(peer, PEERS, buf_ref, o_ref, sem)


def fft_a(gathered, wh, wl):
    return pl.pallas_call(
        fft_a_kernel,
        in_specs=[VMEM] * 3,
        out_specs=HBM,
        out_shape=pltpu.HBM((PEERS, KEPT, LANES), jnp.float32),
        scratch_shapes=FFT_SCRATCH
        + [pltpu.VMEM((PEERS, KEPT, LANES), jnp.float32), pltpu.SemaphoreType.DMA((PIECES,))],
        compiler_params=PARAMS,
        name="fft_a",
    )(gathered, wh, wl)


def fft_p_kernel(pos_ref, *refs):
    g_refs, (wh_ref, wl_ref), o_refs = refs[:8], refs[8:10], refs[10:18]
    x_ref, y_ref, r_ref = refs[18:]
    x, z, c = pos_ref[0], pos_ref[1], pos_ref[2]
    for dx in range(NX):
        for dc in range(NC):
            start = ((x + NX - dx) % NX) * (NLON // NX) + ((c + dc) % NC) * LON
            for zz in range(NZ):
                row = pl.multiple_of(start + zz * NC * LON, LON)
                x_ref[pl.ds(row, LON), :] = g_refs[dx * NC + dc][zz * LON : (zz + 1) * LON, :]
    fft_core(x_ref, wh_ref, wl_ref, y_ref, r_ref, natural_row)
    for dz in range(NZ):
        target = (z + dz) % NZ
        for xx in range(NX):
            for cc in range(NC):
                k1 = xx * NZ * NC + target * NC + cc
                for eight in range(KEPT // 8):
                    row = (xx * NC + cc) * KEPT + eight * 8
                    o_refs[dz][row : row + 8, :] = mode_rows(r_ref, k1, eight)


def fft_p(pos, blocks, wh, wl):
    return pl.pallas_call(
        fft_p_kernel,
        in_specs=[SMEM] + [VMEM] * 10,
        out_specs=[VMEM] * NZ,
        out_shape=[vmem(NX * NC * KEPT, LANES)] * NZ,
        scratch_shapes=[pltpu.VMEM((NLON, LANES), jnp.float32)] + FFT_SCRATCH,
        compiler_params=PARAMS,
        name="fft_p",
    )(pos, *blocks, wh, wl)


GROUP = NZ * NC


def start_and_wait(pairs, sem):
    copies = [pltpu.make_async_copy(source, target, sem.at[i]) for i, (source, target) in enumerate(pairs)]
    for copy in copies:
        copy.start()
    for copy in copies:
        copy.wait()


def split_z_kernel(pos_ref, s_ref, *refs):
    pairs = []
    for dz in range(NZ):
        field = pl.multiple_of(((pos_ref[1] + dz) % NZ) * 8, 8)
        pairs.append((s_ref.at[:, pl.ds(field, 8), pl.ds(0, LANES)], refs[dz]))
    start_and_wait(pairs, refs[NZ])


def split_x_kernel(pos_ref, s_ref, *refs):
    pairs = []
    for dx in range(NX):
        field = pl.multiple_of(((pos_ref[0] + dx) % NX) * GROUP, GROUP)
        pairs.append((s_ref.at[:, pl.ds(field, GROUP), pl.ds(LANES, LANES)], refs[dx]))
    start_and_wait(pairs, refs[NX])


def split(pos, state, kernel, count, fields):
    return pl.pallas_call(
        kernel,
        in_specs=[SMEM, HBM],
        out_specs=[VMEM] * count,
        out_shape=[vmem(LON, fields, LANES)] * count,
        scratch_shapes=[pltpu.SemaphoreType.DMA((count,))],
        compiler_params=PARAMS,
    )(pos, pltpu.with_memory_space_constraint(state, pltpu.HBM))


def spread_x_kernel(pos_ref, *refs):
    b_refs, o_refs = refs[:NZ], refs[NZ:]
    x, z, c = pos_ref[0], pos_ref[1], pos_ref[2]
    for dx in range(NX):
        for dc in range(NC):
            field = ((x + dx) % NX) * NC + (c + dc) % NC
            for dz in range(NZ):
                row = pl.multiple_of(((z + NZ - dz) % NZ) * LON, LON)
                o_refs[dx * NC + dc][pl.ds(row, LON), :] = b_refs[dz][pl.ds(field, LON, stride=8), :]


def spread_x(pos, blocks):
    return pl.pallas_call(
        spread_x_kernel,
        in_specs=[SMEM] + [VMEM] * NZ,
        out_specs=[VMEM] * (NX * NC),
        out_shape=[vmem(NZ * LON, LANES)] * (NX * NC),
        compiler_params=PARAMS,
        name="spread_x",
    )(pos, *blocks)


def spread_out_kernel(pos_ref, *refs):
    h_refs, o_refs = refs[:NZ], refs[NZ:]
    x, z, c = pos_ref[0], pos_ref[1], pos_ref[2]
    for dx in range(NX):
        for dc in range(NC):
            source = pl.multiple_of((((x + dx) % NX) * NC + (c + dc) % NC) * KEPT, KEPT)
            for dz in range(NZ):
                row = pl.multiple_of(((z + NZ - dz) % NZ) * KEPT, KEPT)
                o_refs[dx * NC + dc][pl.ds(row, KEPT), :] = h_refs[dz][pl.ds(source, KEPT), :]


def spread_out(pos, blocks):
    return pl.pallas_call(
        spread_out_kernel,
        in_specs=[SMEM] + [VMEM] * NZ,
        out_specs=[VMEM] * (NX * NC),
        out_shape=[vmem(NZ * KEPT, LANES)] * (NX * NC),
        compiler_params=PARAMS,
        name="spread_out",
    )(pos, *blocks)


def spread_a_kernel(pos_ref, *refs):
    b_refs, o_ref, buf_ref, sem = refs[:NX], refs[NX], refs[NX + 1], refs[NX + 2]
    x = pos_ref[0]

    def field(f, carry):
        for dx in range(NX):
            row = pl.multiple_of(((x + NX - dx) % NX) * LON, LON)
            buf_ref[f, pl.ds(row, LON), :] = b_refs[dx][pl.ds(f, LON, stride=GROUP), :]
        return carry

    send_pieces(field, GROUP, buf_ref, o_ref, sem)


def spread_a(pos, blocks):
    return pl.pallas_call(
        spread_a_kernel,
        in_specs=[SMEM] + [VMEM] * NX,
        out_specs=HBM,
        out_shape=pltpu.HBM((GROUP, NX * LON, LANES), jnp.float32),
        scratch_shapes=[
            pltpu.VMEM((GROUP, NX * LON, LANES), jnp.float32),
            pltpu.SemaphoreType.DMA((PIECES,)),
        ],
        compiler_params=PARAMS,
        name="spread_a",
    )(pos, *blocks)


PAD_K = KEPT + 8


def store_half(x_ref, buf_ref, o_ref, sem, lane):
    copies = []
    step = KEPT // PIECES
    for piece in range(PIECES):
        for kept in range(piece * step, (piece + 1) * step):
            for eight in range(FIELDS // 8):
                buf_ref[kept, eight * 8 : eight * 8 + 8, :] = x_ref[pl.ds(eight * 8 * PAD_K + kept, 8, stride=PAD_K), :]
        copy = pltpu.make_async_copy(
            buf_ref.at[pl.ds(piece * step, step)],
            o_ref.at[pl.ds(piece * step, step), :, pl.ds(lane, LANES)],
            sem.at[piece],
        )
        copy.start()
        copies.append(copy)
    for copy in copies:
        copy.wait()


STORE_SCRATCH = [
    pltpu.VMEM((FIELDS * PAD_K, LANES), jnp.float32),
    pltpu.VMEM((KEPT, FIELDS, LANES), jnp.float32),
    pltpu.SemaphoreType.DMA((PIECES,)),
]


def store_p_kernel(pos_ref, *refs):
    q_refs, o_ref = refs[:8], refs[8]
    x_ref, buf_ref, sem = refs[9:]
    x, c = pos_ref[0], pos_ref[2]
    for dx in range(NX):
        for dc in range(NC):
            base = ((x + NX - dx) % NX) * NC + (c + dc) % NC
            for zz in range(NZ):
                row = pl.multiple_of((base + zz * NX * NC) * PAD_K, 8)
                x_ref[pl.ds(row, KEPT), :] = q_refs[dx * NC + dc][zz * KEPT : (zz + 1) * KEPT, :]
    store_half(x_ref, buf_ref, o_ref, sem, 0)


def store_p(pos, blocks):
    return pl.pallas_call(
        store_p_kernel,
        in_specs=[SMEM] + [VMEM] * 8,
        out_specs=HBM,
        out_shape=f32(KEPT, FIELDS, 2 * LANES),
        scratch_shapes=STORE_SCRATCH,
        compiler_params=PARAMS,
        name="store_p",
    )(pos, *blocks)


def store_a_kernel(prior_ref, q_ref, o_ref, x_ref, buf_ref, sem):
    del prior_ref

    def field(f, carry):
        x_ref[pl.ds(pl.multiple_of(f * PAD_K, 8), KEPT), :] = q_ref[f]
        return carry

    lax.fori_loop(0, FIELDS, field, 0, unroll=8)
    store_half(x_ref, buf_ref, o_ref, sem, LANES)


def store_a(prior, shares):
    return pl.pallas_call(
        store_a_kernel,
        in_specs=[HBM, VMEM],
        out_specs=HBM,
        out_shape=f32(KEPT, FIELDS, 2 * LANES),
        scratch_shapes=STORE_SCRATCH,
        input_output_aliases={0: 0},
        compiler_params=PARAMS,
        name="store_a",
    )(prior, shares)


def shifts(dx, dz, dc):
    def at(x, z, c):
        return (x % NX) * NZ * NC + (z % NZ) * NC + c % NC

    return [
        (at(x, z, c), at(x + dx, z + dz, c + dc)) for x in range(NX) for z in range(NZ) for c in range(NC)
    ]


Z_ORDER = (1, 7, 4, 3, 5, 2, 6)


def exchange_z(blocks):
    out = [None] * NZ
    out[0] = blocks[0]
    for dz in Z_ORDER:
        out[dz] = lax.ppermute(blocks[dz], "lon", shifts(0, dz, 0))
    return out


AX_ORDER = (1, 3, 2)
GROUPS = [[x * GROUP + g for g in range(GROUP)] for x in range(NX)]


def exchange_x(blocks):
    out = [None] * NX
    out[0] = blocks[0]
    for dx in AX_ORDER:
        out[dx] = lax.ppermute(blocks[dx], "lon", shifts(dx, 0, 0))
    return out


X_ORDER = ((1, 0), (3, 0), (2, 0), (2, 1), (1, 1), (3, 1), (0, 1))


def exchange_xc(blocks):
    out = [None] * (NX * NC)
    out[0] = blocks[0]
    for dx, dc in X_ORDER:
        out[dx * NC + dc] = lax.ppermute(blocks[dx * NC + dc], "lon", shifts(dx, 0, dc))
    return out


def local(state):
    device = lax.axis_index("lon")
    pos = jnp.stack([device // (NZ * NC), (device // NC) % NZ, device % NC]).astype(jnp.int32)
    wh, wl = twiddle_matrices(1.0 / math.sqrt(NLON))
    pieces = split(pos, state, split_z_kernel, NZ, 8)
    pieces = exchange_z(pieces)
    parts = split(pos, state, split_x_kernel, NX, GROUP)
    parts = exchange_x(parts)
    sent = spread_a(pos, [b.reshape(LON * GROUP, LANES) for b in parts])
    gathered = lax.all_to_all(
        sent, "lon", split_axis=0, concat_axis=0, axis_index_groups=GROUPS, tiled=True
    )
    pieces = spread_x(pos, [b.reshape(LON * 8, LANES) for b in pieces])
    pieces = exchange_xc(pieces)
    pieces = fft_p(pos, pieces, wh, wl)
    pieces = exchange_z(pieces)
    spectrum = fft_a(gathered.reshape(NLON, LANES), wh, wl)
    shares = lax.all_to_all(spectrum, "lon", split_axis=0, concat_axis=0, tiled=True)
    pieces = spread_out(pos, pieces)
    pieces = exchange_xc(pieces)
    out = store_p(pos, pieces)
    out = store_a(out, shares)
    return out.reshape(2, RADIX, FIELDS, 2 * LANES)


def solution(mesh):
    return jax.shard_map(
        local,
        mesh=mesh,
        in_specs=(P("lon", None, "lat"),),
        out_specs=P(None, "lon", None, "lat"),
        check_vma=False,
    )
```

```python
import math

import jax
import jax.numpy as jnp
from jax import lax
from jax.experimental import pallas as pl
from jax.experimental.pallas import tpu as pltpu
from jax.sharding import PartitionSpec as P


NLON = 2048
RADIX = 16
INNER = NLON // RADIX
PEERS = 64
HALF = RADIX // 2
NX, NZ, NC = 4, 8, 2
LON = 32
KEPT = 2 * RADIX
FIELDS = 64
LANES = 128
VMEM = pl.BlockSpec(memory_space=pltpu.VMEM)
HBM = pl.BlockSpec(memory_space=pltpu.HBM)
SMEM = pl.BlockSpec(memory_space=pltpu.SMEM)
PARAMS = pltpu.CompilerParams(vmem_limit_bytes=16 * 1024 * 1024)


def f32(*shape):
    return jax.ShapeDtypeStruct(shape, jnp.float32)


def vmem(*shape):
    return pltpu.VMEM(shape, jnp.float32)


def split_bf16(v):
    high = v.astype(jnp.bfloat16)
    low = (v - high.astype(jnp.float32)).astype(jnp.bfloat16)
    return high, low


def phase(rows, cols):
    turn = (rows * cols) % NLON
    turn = jnp.where(turn >= NLON // 2, turn - NLON, turn)
    return turn.astype(jnp.float32) * (2.0 * math.pi / NLON)


def twiddle_matrices(scale):
    shape = (HALF, 2, PEERS, INNER)
    pair = lax.broadcasted_iota(jnp.int32, shape, 0)
    mirror = lax.broadcasted_iota(jnp.int32, shape, 1)
    outer = lax.broadcasted_iota(jnp.int32, shape, 2)
    inner = lax.broadcasted_iota(jnp.int32, shape, 3)
    first = jnp.where(mirror == 0, pair, jnp.where(pair == 0, HALF, RADIX - pair))
    angle = phase(inner, first + RADIX * outer)
    c = jnp.cos(angle) * scale
    s = jnp.sin(angle) * scale
    real_only = pair == 0
    zero = jnp.zeros_like(c)
    plain = mirror == 0
    re_a = jnp.where(real_only, jnp.where(plain, c, zero), c)
    im_a = jnp.where(real_only, jnp.where(plain, -s, zero), -s)
    re_b = jnp.where(real_only, jnp.where(plain, zero, c), jnp.where(plain, s, -s))
    im_b = jnp.where(real_only, jnp.where(plain, zero, -s), jnp.where(plain, c, -c))
    re = jnp.concatenate([re_a, re_b], axis=-1)
    im = jnp.concatenate([im_a, im_b], axis=-1)
    full = jnp.stack([re, im], axis=2)
    full = full.reshape(HALF, 4 * PEERS, 2 * INNER)
    high = lax.reduce_precision(full, 8, 7)
    high, low = high.astype(jnp.bfloat16), (full - high).astype(jnp.bfloat16)
    return high, low


def fft_real16(x):
    def fft_complex8(z):
        def fft4(a):
            (ar, ai), (br, bi), (cr, ci), (dr, di) = a
            sr, si = ar + cr, ai + ci
            tr, ti = ar - cr, ai - ci
            ur, ui = br + dr, bi + di
            vr, vi = br - dr, bi - di
            return [(sr + ur, si + ui), (tr + vi, ti - vr), (sr - ur, si - ui), (tr - vi, ti + vr)]

        even = fft4(z[0::2])
        odd = fft4(z[1::2])
        h = math.sqrt(0.5)
        out = [None] * 8
        for k in range(4):
            er, ei = even[k]
            pr, pi = odd[k]
            if k == 1:
                pr, pi = (pr + pi) * h, (pi - pr) * h
            elif k == 2:
                pr, pi = pi, -pr
            elif k == 3:
                pr, pi = (pi - pr) * h, -(pr + pi) * h
            out[k] = (er + pr, ei + pi)
            out[k + 4] = (er - pr, ei - pi)
        return out

    z = fft_complex8([(x[2 * i], x[2 * i + 1]) for i in range(8)])
    out = [(z[0][0] + z[0][1], None)]
    for k in range(1, 8):
        zr, zi = z[k]
        wr, wi = z[8 - k]
        er, ei = (zr + wr) * 0.5, (zi - wi) * 0.5
        pr, pi = (zi + wi) * 0.5, (wr - zr) * 0.5
        c, s = math.cos(2 * math.pi * k / 16), math.sin(2 * math.pi * k / 16)
        out.append((er + c * pr + s * pi, ei + c * pi - s * pr))
    out.append((z[0][0] - z[0][1], None))
    return out


PAD_R = PEERS + 8


def natural_row(n2, base):
    return n2 * INNER + base


def grouped_row(n2, base):
    return ((n2 % 4) * 4 + base // LON) * INNER + (n2 // 4) * LON + base % LON


def fft_core(x_ref, wh_ref, wl_ref, y_ref, r_ref, row_of):
    def butterfly(i, carry):
        base = pl.multiple_of(i * 8, 8)
        x = [x_ref[pl.ds(pl.multiple_of(row_of(n2, base), 8), 8), :] for n2 in range(RADIX)]
        y = fft_real16(x)
        for k in range(HALF):
            parts = (y[0][0], y[HALF][0]) if k == 0 else y[k]
            for j, part in enumerate(parts):
                y_ref[k, pl.ds(j * INNER + base, 8), :] = part
        return carry

    lax.fori_loop(0, INNER // 8, butterfly, 0, unroll=4)
    for k in range(HALF):
        yh, yl = split_bf16(y_ref[k])
        two = jnp.dot(wh_ref[k], jnp.concatenate([yh, yl], axis=1), preferred_element_type=jnp.float32)
        r = two[:, :LANES] + two[:, LANES:]
        r = r + jnp.dot(wl_ref[k], yh, preferred_element_type=jnp.float32)
        mirror = HALF if k == 0 else RADIX - k
        for q, row in enumerate((k, RADIX + k, mirror, RADIX + mirror)):
            r_ref[pl.ds(row * PAD_R, PEERS), :] = r[q * PEERS : (q + 1) * PEERS]


PIECES = 4


def send_pieces(body, count, buf_ref, o_ref, sem):
    step = count // PIECES
    copies = []
    for piece in range(PIECES):
        lax.fori_loop(piece * step, (piece + 1) * step, body, 0, unroll=4)
        rows = pl.ds(piece * step, step)
        copy = pltpu.make_async_copy(buf_ref.at[rows], o_ref.at[rows], sem.at[piece])
        copy.start()
        copies.append(copy)
    for copy in copies:
        copy.wait()


FFT_SCRATCH = [
    pltpu.VMEM((HALF, 2 * INNER, LANES), jnp.float32),
    pltpu.VMEM((KEPT * PAD_R, LANES), jnp.float32),
]


def mode_rows(r_ref, k1, eight):
    return r_ref[pl.ds(eight * 8 * PAD_R + k1, 8, stride=PAD_R), :]


def fft_a_kernel(x_ref, wh_ref, wl_ref, o_ref, y_ref, r_ref, buf_ref, sem):
    fft_core(x_ref, wh_ref, wl_ref, y_ref, r_ref, grouped_row)

    def peer(k1, carry):
        for eight in range(KEPT // 8):
            buf_ref[k1, eight * 8 : eight * 8 + 8, :] = mode_rows(r_ref, k1, eight)
        return carry

    send_pieces(peer, PEERS, buf_ref, o_ref, sem)


def fft_a(gathered, wh, wl):
    return pl.pallas_call(
        fft_a_kernel,
        in_specs=[VMEM] * 3,
        out_specs=HBM,
        out_shape=pltpu.HBM((PEERS, KEPT, LANES), jnp.float32),
        scratch_shapes=FFT_SCRATCH
        + [pltpu.VMEM((PEERS, KEPT, LANES), jnp.float32), pltpu.SemaphoreType.DMA((PIECES,))],
        compiler_params=PARAMS,
        name="fft_a",
    )(gathered, wh, wl)


def fft_p_kernel(pos_ref, *refs):
    g_refs, (wh_ref, wl_ref), o_refs = refs[:8], refs[8:10], refs[10:18]
    x_ref, y_ref, r_ref = refs[18:]
    x, z, c = pos_ref[0], pos_ref[1], pos_ref[2]
    for dx in range(NX):
        for dc in range(NC):
            start = ((x + NX - dx) % NX) * (NLON // NX) + ((c + dc) % NC) * LON
            for zz in range(NZ):
                row = pl.multiple_of(start + zz * NC * LON, LON)
                x_ref[pl.ds(row, LON), :] = g_refs[dx * NC + dc][zz * LON : (zz + 1) * LON, :]
    fft_core(x_ref, wh_ref, wl_ref, y_ref, r_ref, natural_row)
    for dz in range(NZ):
        target = (z + dz) % NZ
        for xx in range(NX):
            for cc in range(NC):
                k1 = xx * NZ * NC + target * NC + cc
                for eight in range(KEPT // 8):
                    row = (xx * NC + cc) * KEPT + eight * 8
                    o_refs[dz][row : row + 8, :] = mode_rows(r_ref, k1, eight)


def fft_p(pos, blocks, wh, wl):
    return pl.pallas_call(
        fft_p_kernel,
        in_specs=[SMEM] + [VMEM] * 10,
        out_specs=[VMEM] * NZ,
        out_shape=[vmem(NX * NC * KEPT, LANES)] * NZ,
        scratch_shapes=[pltpu.VMEM((NLON, LANES), jnp.float32)] + FFT_SCRATCH,
        compiler_params=PARAMS,
        name="fft_p",
    )(pos, *blocks, wh, wl)


GROUP = NZ * NC


def split_kernel(pos_ref, s_ref, *refs):
    o_refs, sem = refs[: NZ + NX], refs[NZ + NX]
    x, z = pos_ref[0], pos_ref[1]
    copies = []
    for dz in range(NZ):
        field = pl.multiple_of(((z + dz) % NZ) * 8, 8)
        source = s_ref.at[:, pl.ds(field, 8), pl.ds(0, LANES)]
        copies.append(pltpu.make_async_copy(source, o_refs[dz], sem.at[dz]))
    for dx in range(NX):
        field = pl.multiple_of(((x + dx) % NX) * GROUP, GROUP)
        source = s_ref.at[:, pl.ds(field, GROUP), pl.ds(LANES, LANES)]
        copies.append(pltpu.make_async_copy(source, o_refs[NZ + dx], sem.at[NZ + dx]))
    for copy in copies:
        copy.start()
    for copy in copies:
        copy.wait()


def split(pos, state):
    out = pl.pallas_call(
        split_kernel,
        in_specs=[SMEM, HBM],
        out_specs=[VMEM] * (NZ + NX),
        out_shape=[vmem(LON, 8, LANES)] * NZ + [vmem(LON, GROUP, LANES)] * NX,
        scratch_shapes=[pltpu.SemaphoreType.DMA((NZ + NX,))],
        compiler_params=PARAMS,
        name="split",
    )(pos, pltpu.with_memory_space_constraint(state, pltpu.HBM))
    return out[:NZ], out[NZ:]


def spread_x_kernel(pos_ref, *refs):
    b_refs, o_refs = refs[:NZ], refs[NZ:]
    x, z, c = pos_ref[0], pos_ref[1], pos_ref[2]
    for dx in range(NX):
        for dc in range(NC):
            field = ((x + dx) % NX) * NC + (c + dc) % NC
            for dz in range(NZ):
                row = pl.multiple_of(((z + NZ - dz) % NZ) * LON, LON)
                o_refs[dx * NC + dc][pl.ds(row, LON), :] = b_refs[dz][pl.ds(field, LON, stride=8), :]


def spread_x(pos, blocks):
    return pl.pallas_call(
        spread_x_kernel,
        in_specs=[SMEM] + [VMEM] * NZ,
        out_specs=[VMEM] * (NX * NC),
        out_shape=[vmem(NZ * LON, LANES)] * (NX * NC),
        compiler_params=PARAMS,
        name="spread_x",
    )(pos, *blocks)


def spread_out_kernel(pos_ref, *refs):
    h_refs, o_refs = refs[:NZ], refs[NZ:]
    x, z, c = pos_ref[0], pos_ref[1], pos_ref[2]
    for dx in range(NX):
        for dc in range(NC):
            source = pl.multiple_of((((x + dx) % NX) * NC + (c + dc) % NC) * KEPT, KEPT)
            for dz in range(NZ):
                row = pl.multiple_of(((z + NZ - dz) % NZ) * KEPT, KEPT)
                o_refs[dx * NC + dc][pl.ds(row, KEPT), :] = h_refs[dz][pl.ds(source, KEPT), :]


def spread_out(pos, blocks):
    return pl.pallas_call(
        spread_out_kernel,
        in_specs=[SMEM] + [VMEM] * NZ,
        out_specs=[VMEM] * (NX * NC),
        out_shape=[vmem(NZ * KEPT, LANES)] * (NX * NC),
        compiler_params=PARAMS,
        name="spread_out",
    )(pos, *blocks)


def spread_a_kernel(pos_ref, *refs):
    b_refs, o_ref, buf_ref, sem = refs[:NX], refs[NX], refs[NX + 1], refs[NX + 2]
    x = pos_ref[0]

    def field(f, carry):
        for dx in range(NX):
            row = pl.multiple_of(((x + NX - dx) % NX) * LON, LON)
            buf_ref[f, pl.ds(row, LON), :] = b_refs[dx][pl.ds(f, LON, stride=GROUP), :]
        return carry

    send_pieces(field, GROUP, buf_ref, o_ref, sem)


def spread_a(pos, blocks):
    return pl.pallas_call(
        spread_a_kernel,
        in_specs=[SMEM] + [VMEM] * NX,
        out_specs=HBM,
        out_shape=pltpu.HBM((GROUP, NX * LON, LANES), jnp.float32),
        scratch_shapes=[
            pltpu.VMEM((GROUP, NX * LON, LANES), jnp.float32),
            pltpu.SemaphoreType.DMA((PIECES,)),
        ],
        compiler_params=PARAMS,
        name="spread_a",
    )(pos, *blocks)


PAD_K = KEPT + 8


def store_half(x_ref, buf_ref, o_ref, sem, lane):
    copies = []
    step = KEPT // PIECES
    for piece in range(PIECES):
        for kept in range(piece * step, (piece + 1) * step):
            for eight in range(FIELDS // 8):
                buf_ref[kept, eight * 8 : eight * 8 + 8, :] = x_ref[pl.ds(eight * 8 * PAD_K + kept, 8, stride=PAD_K), :]
        copy = pltpu.make_async_copy(
            buf_ref.at[pl.ds(piece * step, step)],
            o_ref.at[pl.ds(piece * step, step), :, pl.ds(lane, LANES)],
            sem.at[piece],
        )
        copy.start()
        copies.append(copy)
    for copy in copies:
        copy.wait()


STORE_SCRATCH = [
    pltpu.VMEM((FIELDS * PAD_K, LANES), jnp.float32),
    pltpu.VMEM((KEPT, FIELDS, LANES), jnp.float32),
    pltpu.SemaphoreType.DMA((PIECES,)),
]


def store_p_kernel(pos_ref, prior_ref, *refs):
    del prior_ref
    q_refs, o_ref = refs[:8], refs[8]
    x_ref, buf_ref, sem = refs[9:]
    x, c = pos_ref[0], pos_ref[2]
    for dx in range(NX):
        for dc in range(NC):
            base = ((x + NX - dx) % NX) * NC + (c + dc) % NC
            for zz in range(NZ):
                row = pl.multiple_of((base + zz * NX * NC) * PAD_K, 8)
                x_ref[pl.ds(row, KEPT), :] = q_refs[dx * NC + dc][zz * KEPT : (zz + 1) * KEPT, :]
    store_half(x_ref, buf_ref, o_ref, sem, 0)


def store_p(pos, prior, blocks):
    return pl.pallas_call(
        store_p_kernel,
        in_specs=[SMEM, HBM] + [VMEM] * 8,
        out_specs=HBM,
        out_shape=f32(KEPT, FIELDS, 2 * LANES),
        scratch_shapes=STORE_SCRATCH,
        input_output_aliases={1: 0},
        compiler_params=PARAMS,
        name="store_p",
    )(pos, prior, *blocks)


def store_a_kernel(q_ref, o_ref, x_ref, buf_ref, sem):
    def field(f, carry):
        x_ref[pl.ds(pl.multiple_of(f * PAD_K, 8), KEPT), :] = q_ref[f]
        return carry

    lax.fori_loop(0, FIELDS, field, 0, unroll=8)
    store_half(x_ref, buf_ref, o_ref, sem, LANES)


def store_a(shares):
    return pl.pallas_call(
        store_a_kernel,
        in_specs=[VMEM],
        out_specs=HBM,
        out_shape=f32(KEPT, FIELDS, 2 * LANES),
        scratch_shapes=STORE_SCRATCH,
        compiler_params=PARAMS,
        name="store_a",
    )(shares)


def shifts(dx, dz, dc):
    def at(x, z, c):
        return (x % NX) * NZ * NC + (z % NZ) * NC + c % NC

    return [
        (at(x, z, c), at(x + dx, z + dz, c + dc)) for x in range(NX) for z in range(NZ) for c in range(NC)
    ]


Z_IN = (1, 7, 4, 3, 5, 2, 6)
Z_OUT = (1, 7, 2, 6, 3, 5, 4)


def exchange_z(blocks, order):
    out = [None] * NZ
    out[0] = blocks[0]
    for dz in order:
        out[dz] = lax.ppermute(blocks[dz], "lon", shifts(0, dz, 0))
    return out


AX_ORDER = (1, 3, 2)
GROUPS = [[x * GROUP + g for g in range(GROUP)] for x in range(NX)]


def exchange_x(blocks):
    out = [None] * NX
    out[0] = blocks[0]
    for dx in AX_ORDER:
        out[dx] = lax.ppermute(blocks[dx], "lon", shifts(dx, 0, 0))
    return out


X_ORDER = ((1, 0), (3, 0), (2, 0), (2, 1), (1, 1), (3, 1), (0, 1))


def exchange_xc(blocks):
    out = [None] * (NX * NC)
    out[0] = blocks[0]
    for dx, dc in X_ORDER:
        out[dx * NC + dc] = lax.ppermute(blocks[dx * NC + dc], "lon", shifts(dx, 0, dc))
    return out


def local(state):
    device = lax.axis_index("lon")
    pos = jnp.stack([device // (NZ * NC), (device // NC) % NZ, device % NC]).astype(jnp.int32)
    wh, wl = twiddle_matrices(1.0 / math.sqrt(NLON))
    pieces, parts = split(pos, state)
    pieces = exchange_z(pieces, Z_IN)
    parts = exchange_x(parts)
    sent = spread_a(pos, [b.reshape(LON * GROUP, LANES) for b in parts])
    gathered = lax.all_to_all(
        sent, "lon", split_axis=0, concat_axis=0, axis_index_groups=GROUPS, tiled=True
    )
    pieces = spread_x(pos, [b.reshape(LON * 8, LANES) for b in pieces])
    pieces = exchange_xc(pieces)
    pieces = fft_p(pos, pieces, wh, wl)
    pieces = exchange_z(pieces, Z_OUT)
    spectrum = fft_a(gathered.reshape(NLON, LANES), wh, wl)
    shares = lax.all_to_all(spectrum, "lon", split_axis=0, concat_axis=0, tiled=True)
    pieces = spread_out(pos, pieces)
    pieces = exchange_xc(pieces)
    out = store_a(shares)
    out = store_p(pos, out, pieces)
    return out.reshape(2, RADIX, FIELDS, 2 * LANES)


def solution(mesh):
    return jax.shard_map(
        local,
        mesh=mesh,
        in_specs=(P("lon", None, "lat"),),
        out_specs=P(None, "lon", None, "lat"),
        check_vma=False,
    )
```

```python
import math

import jax
import jax.numpy as jnp
from jax import lax
from jax.experimental import pallas as pl
from jax.experimental.pallas import tpu as pltpu
from jax.sharding import PartitionSpec as P


NLON = 2048
RADIX = 16
INNER = NLON // RADIX
PEERS = 64
HALF = RADIX // 2
NX, NZ, NC = 4, 8, 2
LON = 32
KEPT = 2 * RADIX
FIELDS = 64
LANES = 128
VMEM = pl.BlockSpec(memory_space=pltpu.VMEM)
HBM = pl.BlockSpec(memory_space=pltpu.HBM)
SMEM = pl.BlockSpec(memory_space=pltpu.SMEM)
PARAMS = pltpu.CompilerParams(vmem_limit_bytes=16 * 1024 * 1024)


def f32(*shape):
    return jax.ShapeDtypeStruct(shape, jnp.float32)


def vmem(*shape):
    return pltpu.VMEM(shape, jnp.float32)


def split_bf16(v):
    high = v.astype(jnp.bfloat16)
    low = (v - high.astype(jnp.float32)).astype(jnp.bfloat16)
    return high, low


def phase(rows, cols):
    turn = (rows * cols) % NLON
    turn = jnp.where(turn >= NLON // 2, turn - NLON, turn)
    return turn.astype(jnp.float32) * (2.0 * math.pi / NLON)


def twiddle_matrices(scale):
    shape = (HALF, 2, PEERS, INNER)
    pair = lax.broadcasted_iota(jnp.int32, shape, 0)
    mirror = lax.broadcasted_iota(jnp.int32, shape, 1)
    outer = lax.broadcasted_iota(jnp.int32, shape, 2)
    inner = lax.broadcasted_iota(jnp.int32, shape, 3)
    first = jnp.where(mirror == 0, pair, jnp.where(pair == 0, HALF, RADIX - pair))
    angle = phase(inner, first + RADIX * outer)
    c = jnp.cos(angle) * scale
    s = jnp.sin(angle) * scale
    real_only = pair == 0
    zero = jnp.zeros_like(c)
    plain = mirror == 0
    re_a = jnp.where(real_only, jnp.where(plain, c, zero), c)
    im_a = jnp.where(real_only, jnp.where(plain, -s, zero), -s)
    re_b = jnp.where(real_only, jnp.where(plain, zero, c), jnp.where(plain, s, -s))
    im_b = jnp.where(real_only, jnp.where(plain, zero, -s), jnp.where(plain, c, -c))
    re = jnp.concatenate([re_a, re_b], axis=-1)
    im = jnp.concatenate([im_a, im_b], axis=-1)
    full = jnp.stack([re, im], axis=2)
    full = full.reshape(HALF, 4 * PEERS, 2 * INNER)
    high = lax.reduce_precision(full, 8, 7)
    high, low = high.astype(jnp.bfloat16), (full - high).astype(jnp.bfloat16)
    return high, low


def fft_real16(x):
    def fft_complex8(z):
        def fft4(a):
            (ar, ai), (br, bi), (cr, ci), (dr, di) = a
            sr, si = ar + cr, ai + ci
            tr, ti = ar - cr, ai - ci
            ur, ui = br + dr, bi + di
            vr, vi = br - dr, bi - di
            return [(sr + ur, si + ui), (tr + vi, ti - vr), (sr - ur, si - ui), (tr - vi, ti + vr)]

        even = fft4(z[0::2])
        odd = fft4(z[1::2])
        h = math.sqrt(0.5)
        out = [None] * 8
        for k in range(4):
            er, ei = even[k]
            pr, pi = odd[k]
            if k == 1:
                pr, pi = (pr + pi) * h, (pi - pr) * h
            elif k == 2:
                pr, pi = pi, -pr
            elif k == 3:
                pr, pi = (pi - pr) * h, -(pr + pi) * h
            out[k] = (er + pr, ei + pi)
            out[k + 4] = (er - pr, ei - pi)
        return out

    z = fft_complex8([(x[2 * i], x[2 * i + 1]) for i in range(8)])
    out = [(z[0][0] + z[0][1], None)]
    for k in range(1, 8):
        zr, zi = z[k]
        wr, wi = z[8 - k]
        er, ei = (zr + wr) * 0.5, (zi - wi) * 0.5
        pr, pi = (zi + wi) * 0.5, (wr - zr) * 0.5
        c, s = math.cos(2 * math.pi * k / 16), math.sin(2 * math.pi * k / 16)
        out.append((er + c * pr + s * pi, ei + c * pi - s * pr))
    out.append((z[0][0] - z[0][1], None))
    return out


PAD_R = PEERS + 8


def natural_row(n2, base):
    return n2 * INNER + base


def grouped_row(n2, base):
    return ((n2 % 4) * 4 + base // LON) * INNER + (n2 // 4) * LON + base % LON


def fft_core(x_ref, wh_ref, wl_ref, y_ref, r_ref, row_of):
    def butterfly(i, carry):
        base = pl.multiple_of(i * 8, 8)
        x = [x_ref[pl.ds(pl.multiple_of(row_of(n2, base), 8), 8), :] for n2 in range(RADIX)]
        y = fft_real16(x)
        for k in range(HALF):
            parts = (y[0][0], y[HALF][0]) if k == 0 else y[k]
            for j, part in enumerate(parts):
                y_ref[k, pl.ds(j * INNER + base, 8), :] = part
        return carry

    lax.fori_loop(0, INNER // 8, butterfly, 0, unroll=4)
    for k in range(HALF):
        yh, yl = split_bf16(y_ref[k])
        two = jnp.dot(wh_ref[k], jnp.concatenate([yh, yl], axis=1), preferred_element_type=jnp.float32)
        r = two[:, :LANES] + two[:, LANES:]
        r = r + jnp.dot(wl_ref[k], yh, preferred_element_type=jnp.float32)
        mirror = HALF if k == 0 else RADIX - k
        for q, row in enumerate((k, RADIX + k, mirror, RADIX + mirror)):
            r_ref[pl.ds(row * PAD_R, PEERS), :] = r[q * PEERS : (q + 1) * PEERS]


PIECES = 4


def send_pieces(body, count, buf_ref, o_ref, sem):
    step = count // PIECES
    copies = []
    for piece in range(PIECES):
        lax.fori_loop(piece * step, (piece + 1) * step, body, 0, unroll=4)
        rows = pl.ds(piece * step, step)
        copy = pltpu.make_async_copy(buf_ref.at[rows], o_ref.at[rows], sem.at[piece])
        copy.start()
        copies.append(copy)
    for copy in copies:
        copy.wait()


FFT_SCRATCH = [
    pltpu.VMEM((HALF, 2 * INNER, LANES), jnp.float32),
    pltpu.VMEM((KEPT * PAD_R, LANES), jnp.float32),
]


def mode_rows(r_ref, k1, eight):
    return r_ref[pl.ds(eight * 8 * PAD_R + k1, 8, stride=PAD_R), :]


def fft_a_kernel(x_ref, wh_ref, wl_ref, o_ref, y_ref, r_ref, buf_ref, sem):
    fft_core(x_ref, wh_ref, wl_ref, y_ref, r_ref, grouped_row)

    def peer(k1, carry):
        for eight in range(KEPT // 8):
            buf_ref[k1, eight * 8 : eight * 8 + 8, :] = mode_rows(r_ref, k1, eight)
        return carry

    send_pieces(peer, PEERS, buf_ref, o_ref, sem)


def fft_a(gathered, wh, wl):
    return pl.pallas_call(
        fft_a_kernel,
        in_specs=[VMEM] * 3,
        out_specs=HBM,
        out_shape=pltpu.HBM((PEERS, KEPT, LANES), jnp.float32),
        scratch_shapes=FFT_SCRATCH
        + [pltpu.VMEM((PEERS, KEPT, LANES), jnp.float32), pltpu.SemaphoreType.DMA((PIECES,))],
        compiler_params=PARAMS,
        name="fft_a",
    )(gathered, wh, wl)


def fft_p_kernel(pos_ref, *refs):
    g_refs, (wh_ref, wl_ref), o_refs = refs[:8], refs[8:10], refs[10:18]
    x_ref, y_ref, r_ref = refs[18:]
    x, z, c = pos_ref[0], pos_ref[1], pos_ref[2]
    for dx in range(NX):
        for dc in range(NC):
            start = ((x + NX - dx) % NX) * (NLON // NX) + ((c + dc) % NC) * LON
            for zz in range(NZ):
                row = pl.multiple_of(start + zz * NC * LON, LON)
                x_ref[pl.ds(row, LON), :] = g_refs[dx * NC + dc][zz * LON : (zz + 1) * LON, :]
    fft_core(x_ref, wh_ref, wl_ref, y_ref, r_ref, natural_row)
    for dz in range(NZ):
        target = (z + dz) % NZ
        for xx in range(NX):
            for cc in range(NC):
                k1 = xx * NZ * NC + target * NC + cc
                for eight in range(KEPT // 8):
                    row = (xx * NC + cc) * KEPT + eight * 8
                    o_refs[dz][row : row + 8, :] = mode_rows(r_ref, k1, eight)


def fft_p(pos, blocks, wh, wl):
    return pl.pallas_call(
        fft_p_kernel,
        in_specs=[SMEM] + [VMEM] * 10,
        out_specs=[VMEM] * NZ,
        out_shape=[vmem(NX * NC * KEPT, LANES)] * NZ,
        scratch_shapes=[pltpu.VMEM((NLON, LANES), jnp.float32)] + FFT_SCRATCH,
        compiler_params=PARAMS,
        name="fft_p",
    )(pos, *blocks, wh, wl)


GROUP = NZ * NC


def split_kernel(pos_ref, s_ref, *refs):
    o_refs, sem = refs[: NZ + NX], refs[NZ + NX]
    x, z = pos_ref[0], pos_ref[1]
    copies = []
    for dz in range(NZ):
        field = pl.multiple_of(((z + dz) % NZ) * 8, 8)
        source = s_ref.at[:, pl.ds(field, 8), pl.ds(0, LANES)]
        copies.append(pltpu.make_async_copy(source, o_refs[dz], sem.at[dz]))
    for dx in range(NX):
        field = pl.multiple_of(((x + dx) % NX) * GROUP, GROUP)
        source = s_ref.at[:, pl.ds(field, GROUP), pl.ds(LANES, LANES)]
        copies.append(pltpu.make_async_copy(source, o_refs[NZ + dx], sem.at[NZ + dx]))
    for copy in copies:
        copy.start()
    for copy in copies:
        copy.wait()


def split(pos, state):
    out = pl.pallas_call(
        split_kernel,
        in_specs=[SMEM, HBM],
        out_specs=[VMEM] * (NZ + NX),
        out_shape=[vmem(LON, 8, LANES)] * NZ + [vmem(LON, GROUP, LANES)] * NX,
        scratch_shapes=[pltpu.SemaphoreType.DMA((NZ + NX,))],
        compiler_params=PARAMS,
        name="split",
    )(pos, pltpu.with_memory_space_constraint(state, pltpu.HBM))
    return out[:NZ], out[NZ:]


def spread_x_kernel(pos_ref, *refs):
    b_refs, o_refs = refs[:NZ], refs[NZ:]
    x, z, c = pos_ref[0], pos_ref[1], pos_ref[2]
    for dx in range(NX):
        for dc in range(NC):
            field = ((x + dx) % NX) * NC + (c + dc) % NC
            for dz in range(NZ):
                row = pl.multiple_of(((z + NZ - dz) % NZ) * LON, LON)
                o_refs[dx * NC + dc][pl.ds(row, LON), :] = b_refs[dz][pl.ds(field, LON, stride=8), :]


def spread_x(pos, blocks):
    return pl.pallas_call(
        spread_x_kernel,
        in_specs=[SMEM] + [VMEM] * NZ,
        out_specs=[VMEM] * (NX * NC),
        out_shape=[vmem(NZ * LON, LANES)] * (NX * NC),
        compiler_params=PARAMS,
        name="spread_x",
    )(pos, *blocks)


def spread_out_kernel(pos_ref, *refs):
    h_refs, o_refs = refs[:NZ], refs[NZ:]
    x, z, c = pos_ref[0], pos_ref[1], pos_ref[2]
    for dx in range(NX):
        for dc in range(NC):
            source = pl.multiple_of((((x + dx) % NX) * NC + (c + dc) % NC) * KEPT, KEPT)
            for dz in range(NZ):
                row = pl.multiple_of(((z + NZ - dz) % NZ) * KEPT, KEPT)
                o_refs[dx * NC + dc][pl.ds(row, KEPT), :] = h_refs[dz][pl.ds(source, KEPT), :]


def spread_out(pos, blocks):
    return pl.pallas_call(
        spread_out_kernel,
        in_specs=[SMEM] + [VMEM] * NZ,
        out_specs=[VMEM] * (NX * NC),
        out_shape=[vmem(NZ * KEPT, LANES)] * (NX * NC),
        compiler_params=PARAMS,
        name="spread_out",
    )(pos, *blocks)


def spread_a_kernel(pos_ref, *refs):
    b_refs, o_ref, buf_ref, sem = refs[:NX], refs[NX], refs[NX + 1], refs[NX + 2]
    x = pos_ref[0]

    def field(f, carry):
        for dx in range(NX):
            row = pl.multiple_of(((x + NX - dx) % NX) * LON, LON)
            buf_ref[f, pl.ds(row, LON), :] = b_refs[dx][pl.ds(f, LON, stride=GROUP), :]
        return carry

    send_pieces(field, GROUP, buf_ref, o_ref, sem)


def spread_a(pos, blocks):
    return pl.pallas_call(
        spread_a_kernel,
        in_specs=[SMEM] + [VMEM] * NX,
        out_specs=HBM,
        out_shape=pltpu.HBM((GROUP, NX * LON, LANES), jnp.float32),
        scratch_shapes=[
            pltpu.VMEM((GROUP, NX * LON, LANES), jnp.float32),
            pltpu.SemaphoreType.DMA((PIECES,)),
        ],
        compiler_params=PARAMS,
        name="spread_a",
    )(pos, *blocks)


PAD_K = KEPT + 8


def store_block(block, x_ref, buf_ref, o_ref, sem, lane):
    for kept in range(KEPT):
        buf_ref[block, kept] = x_ref[pl.ds(block * 8 * PAD_K + kept, 8, stride=PAD_K), :]
    copy = pltpu.make_async_copy(
        buf_ref.at[block],
        o_ref.at[:, pl.ds(block * 8, 8), pl.ds(lane, LANES)],
        sem.at[block],
    )
    copy.start()
    return copy


STORE_SCRATCH = [
    pltpu.VMEM((FIELDS * PAD_K, LANES), jnp.float32),
    pltpu.VMEM((FIELDS // 8, KEPT, 8, LANES), jnp.float32),
    pltpu.SemaphoreType.DMA((FIELDS // 8,)),
]


def store_p_kernel(pos_ref, prior_ref, *refs):
    del prior_ref
    q_refs, o_ref = refs[:8], refs[8]
    x_ref, buf_ref, sem = refs[9:]
    x, c = pos_ref[0], pos_ref[2]
    copies = []
    for zz in range(NZ):
        for dx in range(NX):
            for dc in range(NC):
                field = zz * 8 + ((x + NX - dx) % NX) * NC + (c + dc) % NC
                row = pl.multiple_of(field * PAD_K, 8)
                x_ref[pl.ds(row, KEPT), :] = q_refs[dx * NC + dc][zz * KEPT : (zz + 1) * KEPT, :]
        copies.append(store_block(zz, x_ref, buf_ref, o_ref, sem, 0))
    for copy in copies:
        copy.wait()


def store_p(pos, prior, blocks):
    return pl.pallas_call(
        store_p_kernel,
        in_specs=[SMEM, HBM] + [VMEM] * 8,
        out_specs=HBM,
        out_shape=f32(KEPT, FIELDS, 2 * LANES),
        scratch_shapes=STORE_SCRATCH,
        input_output_aliases={1: 0},
        compiler_params=PARAMS,
        name="store_p",
    )(pos, prior, *blocks)


def store_a_kernel(q_ref, o_ref, x_ref, buf_ref, sem):
    copies = []
    for block in range(FIELDS // 8):
        for f in range(block * 8, block * 8 + 8):
            x_ref[pl.ds(f * PAD_K, KEPT), :] = q_ref[f]
        copies.append(store_block(block, x_ref, buf_ref, o_ref, sem, LANES))
    for copy in copies:
        copy.wait()


def store_a(shares):
    return pl.pallas_call(
        store_a_kernel,
        in_specs=[VMEM],
        out_specs=HBM,
        out_shape=f32(KEPT, FIELDS, 2 * LANES),
        scratch_shapes=STORE_SCRATCH,
        compiler_params=PARAMS,
        name="store_a",
    )(shares)


def shifts(dx, dz, dc):
    def at(x, z, c):
        return (x % NX) * NZ * NC + (z % NZ) * NC + c % NC

    return [
        (at(x, z, c), at(x + dx, z + dz, c + dc)) for x in range(NX) for z in range(NZ) for c in range(NC)
    ]


Z_ORDER = (1, 7, 4, 3, 5, 2, 6)


def exchange_z(blocks):
    out = [None] * NZ
    out[0] = blocks[0]
    for dz in Z_ORDER:
        out[dz] = lax.ppermute(blocks[dz], "lon", shifts(0, dz, 0))
    return out


AX_ORDER = (1, 3, 2)
GROUPS = [[x * GROUP + g for g in range(GROUP)] for x in range(NX)]


def exchange_x(blocks):
    out = [None] * NX
    out[0] = blocks[0]
    for dx in AX_ORDER:
        out[dx] = lax.ppermute(blocks[dx], "lon", shifts(dx, 0, 0))
    return out


X_ORDER = ((1, 0), (3, 0), (2, 0), (2, 1), (1, 1), (3, 1), (0, 1))


def exchange_xc(blocks):
    out = [None] * (NX * NC)
    out[0] = blocks[0]
    for dx, dc in X_ORDER:
        out[dx * NC + dc] = lax.ppermute(blocks[dx * NC + dc], "lon", shifts(dx, 0, dc))
    return out


def local(state):
    device = lax.axis_index("lon")
    pos = jnp.stack([device // (NZ * NC), (device // NC) % NZ, device % NC]).astype(jnp.int32)
    wh, wl = twiddle_matrices(1.0 / math.sqrt(NLON))
    pieces, parts = split(pos, state)
    pieces = exchange_z(pieces)
    parts = exchange_x(parts)
    sent = spread_a(pos, [b.reshape(LON * GROUP, LANES) for b in parts])
    gathered = lax.all_to_all(
        sent, "lon", split_axis=0, concat_axis=0, axis_index_groups=GROUPS, tiled=True
    )
    pieces = spread_x(pos, [b.reshape(LON * 8, LANES) for b in pieces])
    pieces = exchange_xc(pieces)
    pieces = fft_p(pos, pieces, wh, wl)
    pieces = exchange_z(pieces)
    spectrum = fft_a(gathered.reshape(NLON, LANES), wh, wl)
    shares = lax.all_to_all(spectrum, "lon", split_axis=0, concat_axis=0, tiled=True)
    pieces = spread_out(pos, pieces)
    pieces = exchange_xc(pieces)
    out = store_a(shares)
    out = store_p(pos, out, pieces)
    return out.reshape(2, RADIX, FIELDS, 2 * LANES)


def solution(mesh):
    return jax.shard_map(
        local,
        mesh=mesh,
        in_specs=(P("lon", None, "lat"),),
        out_specs=P(None, "lon", None, "lat"),
        check_vma=False,
    )
```

```python
import math

import jax
import jax.numpy as jnp
from jax import lax
from jax.experimental import pallas as pl
from jax.experimental.pallas import tpu as pltpu
from jax.sharding import PartitionSpec as P


NLON = 2048
RADIX = 16
INNER = NLON // RADIX
PEERS = 64
HALF = RADIX // 2
NX, NZ, NC = 4, 8, 2
LON = 32
KEPT = 2 * RADIX
FIELDS = 64
LANES = 128
VMEM = pl.BlockSpec(memory_space=pltpu.VMEM)
HBM = pl.BlockSpec(memory_space=pltpu.HBM)
SMEM = pl.BlockSpec(memory_space=pltpu.SMEM)
PARAMS = pltpu.CompilerParams(vmem_limit_bytes=16 * 1024 * 1024)


def f32(*shape):
    return jax.ShapeDtypeStruct(shape, jnp.float32)


def vmem(*shape):
    return pltpu.VMEM(shape, jnp.float32)


def split_bf16(v):
    high = v.astype(jnp.bfloat16)
    low = (v - high.astype(jnp.float32)).astype(jnp.bfloat16)
    return high, low


def phase(rows, cols):
    turn = (rows * cols) % NLON
    turn = jnp.where(turn >= NLON // 2, turn - NLON, turn)
    return turn.astype(jnp.float32) * (2.0 * math.pi / NLON)


def twiddle_matrices(scale):
    shape = (HALF, 4, PEERS, INNER)
    pair = lax.broadcasted_iota(jnp.int32, shape, 0)
    kind = lax.broadcasted_iota(jnp.int32, shape, 1)
    outer = lax.broadcasted_iota(jnp.int32, shape, 2)
    inner = lax.broadcasted_iota(jnp.int32, shape, 3)
    first = jnp.where(kind < 2, pair, jnp.where(pair == 0, HALF, RADIX - pair))
    angle = phase(inner, first + RADIX * outer)
    full = jnp.where(kind % 2 == 0, jnp.cos(angle), jnp.sin(angle)) * scale
    full = full.reshape(HALF, 4 * PEERS, INNER)
    high = lax.reduce_precision(full, 8, 7)
    return high.astype(jnp.bfloat16), (full - high).astype(jnp.bfloat16)


def fft_real16(x):
    def fft_complex8(z):
        def fft4(a):
            (ar, ai), (br, bi), (cr, ci), (dr, di) = a
            sr, si = ar + cr, ai + ci
            tr, ti = ar - cr, ai - ci
            ur, ui = br + dr, bi + di
            vr, vi = br - dr, bi - di
            return [(sr + ur, si + ui), (tr + vi, ti - vr), (sr - ur, si - ui), (tr - vi, ti + vr)]

        even = fft4(z[0::2])
        odd = fft4(z[1::2])
        h = math.sqrt(0.5)
        out = [None] * 8
        for k in range(4):
            er, ei = even[k]
            pr, pi = odd[k]
            if k == 1:
                pr, pi = (pr + pi) * h, (pi - pr) * h
            elif k == 2:
                pr, pi = pi, -pr
            elif k == 3:
                pr, pi = (pi - pr) * h, -(pr + pi) * h
            out[k] = (er + pr, ei + pi)
            out[k + 4] = (er - pr, ei - pi)
        return out

    z = fft_complex8([(x[2 * i], x[2 * i + 1]) for i in range(8)])
    out = [(z[0][0] + z[0][1], None)]
    for k in range(1, 8):
        zr, zi = z[k]
        wr, wi = z[8 - k]
        er, ei = (zr + wr) * 0.5, (zi - wi) * 0.5
        pr, pi = (zi + wi) * 0.5, (wr - zr) * 0.5
        c, s = math.cos(2 * math.pi * k / 16), math.sin(2 * math.pi * k / 16)
        out.append((er + c * pr + s * pi, ei + c * pi - s * pr))
    out.append((z[0][0] - z[0][1], None))
    return out


PAD_R = PEERS + 8


def natural_row(n2, base):
    return n2 * INNER + base


def grouped_row(n2, base):
    return ((n2 % 4) * 4 + base // LON) * INNER + (n2 // 4) * LON + base % LON


def fft_core(x_ref, wh_ref, wl_ref, y_ref, r_ref, row_of):
    def butterfly(i, carry):
        base = pl.multiple_of(i * 8, 8)
        x = [x_ref[pl.ds(pl.multiple_of(row_of(n2, base), 8), 8), :] for n2 in range(RADIX)]
        y = fft_real16(x)
        for k in range(HALF):
            parts = (y[0][0], y[HALF][0]) if k == 0 else y[k]
            for j, part in enumerate(parts):
                y_ref[k, pl.ds(j * INNER + base, 8), :] = part
        return carry

    lax.fori_loop(0, INNER // 8, butterfly, 0, unroll=4)
    for k in range(HALF):
        yh, yl = split_bf16(y_ref[k])
        sides = jnp.concatenate([yh[:INNER], yh[INNER:], yl[:INNER], yl[INNER:]], axis=1)
        r = jnp.dot(wh_ref[k], sides, preferred_element_type=jnp.float32)
        r = r[:, : 2 * LANES] + r[:, 2 * LANES :]
        r = r + jnp.dot(wl_ref[k], sides[:, : 2 * LANES], preferred_element_type=jnp.float32)
        (c1, s1, c2, s2), (d1, t1, d2, t2) = (
            [r[q * PEERS : (q + 1) * PEERS, p * LANES : (p + 1) * LANES] for q in range(4)] for p in range(2)
        )
        if k == 0:
            parts = (c1, -s1, d2, -t2)
        else:
            parts = (c1 + t1, d1 - s1, c2 - t2, -d2 - s2)
        mirror = HALF if k == 0 else RADIX - k
        for row, part in zip((k, RADIX + k, mirror, RADIX + mirror), parts):
            r_ref[pl.ds(row * PAD_R, PEERS), :] = part


PIECES = 4


def send_pieces(body, count, buf_ref, o_ref, sem):
    step = count // PIECES
    copies = []
    for piece in range(PIECES):
        lax.fori_loop(piece * step, (piece + 1) * step, body, 0, unroll=4)
        rows = pl.ds(piece * step, step)
        copy = pltpu.make_async_copy(buf_ref.at[rows], o_ref.at[rows], sem.at[piece])
        copy.start()
        copies.append(copy)
    for copy in copies:
        copy.wait()


FFT_SCRATCH = [
    pltpu.VMEM((HALF, 2 * INNER, LANES), jnp.float32),
    pltpu.VMEM((KEPT * PAD_R, LANES), jnp.float32),
]


def mode_rows(r_ref, k1, eight):
    return r_ref[pl.ds(eight * 8 * PAD_R + k1, 8, stride=PAD_R), :]


def fft_a_kernel(x_ref, wh_ref, wl_ref, o_ref, y_ref, r_ref, buf_ref, sem):
    fft_core(x_ref, wh_ref, wl_ref, y_ref, r_ref, grouped_row)

    def peer(k1, carry):
        for eight in range(KEPT // 8):
            buf_ref[k1, eight * 8 : eight * 8 + 8, :] = mode_rows(r_ref, k1, eight)
        return carry

    send_pieces(peer, PEERS, buf_ref, o_ref, sem)


def fft_a(gathered, wh, wl):
    return pl.pallas_call(
        fft_a_kernel,
        in_specs=[VMEM] * 3,
        out_specs=HBM,
        out_shape=pltpu.HBM((PEERS, KEPT, LANES), jnp.float32),
        scratch_shapes=FFT_SCRATCH
        + [pltpu.VMEM((PEERS, KEPT, LANES), jnp.float32), pltpu.SemaphoreType.DMA((PIECES,))],
        compiler_params=PARAMS,
        name="fft_a",
    )(gathered, wh, wl)


def fft_p_kernel(pos_ref, *refs):
    g_refs, (wh_ref, wl_ref), o_refs = refs[:8], refs[8:10], refs[10:18]
    x_ref, y_ref, r_ref = refs[18:]
    x, z, c = pos_ref[0], pos_ref[1], pos_ref[2]
    for dx in range(NX):
        for dc in range(NC):
            start = ((x + NX - dx) % NX) * (NLON // NX) + ((c + dc) % NC) * LON
            for zz in range(NZ):
                row = pl.multiple_of(start + zz * NC * LON, LON)
                x_ref[pl.ds(row, LON), :] = g_refs[dx * NC + dc][zz * LON : (zz + 1) * LON, :]
    fft_core(x_ref, wh_ref, wl_ref, y_ref, r_ref, natural_row)
    for dz in range(NZ):
        target = (z + dz) % NZ
        for xx in range(NX):
            for cc in range(NC):
                k1 = xx * NZ * NC + target * NC + cc
                for eight in range(KEPT // 8):
                    row = (xx * NC + cc) * KEPT + eight * 8
                    o_refs[dz][row : row + 8, :] = mode_rows(r_ref, k1, eight)


def fft_p(pos, blocks, wh, wl):
    return pl.pallas_call(
        fft_p_kernel,
        in_specs=[SMEM] + [VMEM] * 10,
        out_specs=[VMEM] * NZ,
        out_shape=[vmem(NX * NC * KEPT, LANES)] * NZ,
        scratch_shapes=[pltpu.VMEM((NLON, LANES), jnp.float32)] + FFT_SCRATCH,
        compiler_params=PARAMS,
        name="fft_p",
    )(pos, *blocks, wh, wl)


GROUP = NZ * NC


def split_kernel(pos_ref, s_ref, *refs):
    o_refs, sem = refs[: NZ + NX], refs[NZ + NX]
    x, z = pos_ref[0], pos_ref[1]
    copies = []
    for dz in range(NZ):
        field = pl.multiple_of(((z + dz) % NZ) * 8, 8)
        source = s_ref.at[:, pl.ds(field, 8), pl.ds(0, LANES)]
        copies.append(pltpu.make_async_copy(source, o_refs[dz], sem.at[dz]))
    for dx in range(NX):
        field = pl.multiple_of(((x + dx) % NX) * GROUP, GROUP)
        source = s_ref.at[:, pl.ds(field, GROUP), pl.ds(LANES, LANES)]
        copies.append(pltpu.make_async_copy(source, o_refs[NZ + dx], sem.at[NZ + dx]))
    for copy in copies:
        copy.start()
    for copy in copies:
        copy.wait()


def split(pos, state):
    out = pl.pallas_call(
        split_kernel,
        in_specs=[SMEM, HBM],
        out_specs=[VMEM] * (NZ + NX),
        out_shape=[vmem(LON, 8, LANES)] * NZ + [vmem(LON, GROUP, LANES)] * NX,
        scratch_shapes=[pltpu.SemaphoreType.DMA((NZ + NX,))],
        compiler_params=PARAMS,
        name="split",
    )(pos, pltpu.with_memory_space_constraint(state, pltpu.HBM))
    return out[:NZ], out[NZ:]


def spread_x_kernel(pos_ref, *refs):
    b_refs, o_refs = refs[:NZ], refs[NZ:]
    x, z, c = pos_ref[0], pos_ref[1], pos_ref[2]
    for dx in range(NX):
        for dc in range(NC):
            field = ((x + dx) % NX) * NC + (c + dc) % NC
            for dz in range(NZ):
                row = pl.multiple_of(((z + NZ - dz) % NZ) * LON, LON)
                o_refs[dx * NC + dc][pl.ds(row, LON), :] = b_refs[dz][pl.ds(field, LON, stride=8), :]


def spread_x(pos, blocks):
    return pl.pallas_call(
        spread_x_kernel,
        in_specs=[SMEM] + [VMEM] * NZ,
        out_specs=[VMEM] * (NX * NC),
        out_shape=[vmem(NZ * LON, LANES)] * (NX * NC),
        compiler_params=PARAMS,
        name="spread_x",
    )(pos, *blocks)


def spread_out_kernel(pos_ref, *refs):
    h_refs, o_refs = refs[:NZ], refs[NZ:]
    x, z, c = pos_ref[0], pos_ref[1], pos_ref[2]
    for dx in range(NX):
        for dc in range(NC):
            source = pl.multiple_of((((x + dx) % NX) * NC + (c + dc) % NC) * KEPT, KEPT)
            for dz in range(NZ):
                row = pl.multiple_of(((z + NZ - dz) % NZ) * KEPT, KEPT)
                o_refs[dx * NC + dc][pl.ds(row, KEPT), :] = h_refs[dz][pl.ds(source, KEPT), :]


def spread_out(pos, blocks):
    return pl.pallas_call(
        spread_out_kernel,
        in_specs=[SMEM] + [VMEM] * NZ,
        out_specs=[VMEM] * (NX * NC),
        out_shape=[vmem(NZ * KEPT, LANES)] * (NX * NC),
        compiler_params=PARAMS,
        name="spread_out",
    )(pos, *blocks)


def spread_a_kernel(pos_ref, *refs):
    b_refs, o_ref, buf_ref, sem = refs[:NX], refs[NX], refs[NX + 1], refs[NX + 2]
    x = pos_ref[0]

    def field(f, carry):
        for dx in range(NX):
            row = pl.multiple_of(((x + NX - dx) % NX) * LON, LON)
            buf_ref[f, pl.ds(row, LON), :] = b_refs[dx][pl.ds(f, LON, stride=GROUP), :]
        return carry

    send_pieces(field, GROUP, buf_ref, o_ref, sem)


def spread_a(pos, blocks):
    return pl.pallas_call(
        spread_a_kernel,
        in_specs=[SMEM] + [VMEM] * NX,
        out_specs=HBM,
        out_shape=pltpu.HBM((GROUP, NX * LON, LANES), jnp.float32),
        scratch_shapes=[
            pltpu.VMEM((GROUP, NX * LON, LANES), jnp.float32),
            pltpu.SemaphoreType.DMA((PIECES,)),
        ],
        compiler_params=PARAMS,
        name="spread_a",
    )(pos, *blocks)


PAD_K = KEPT + 8


def store_block(block, x_ref, buf_ref, o_ref, sem, lane):
    for kept in range(KEPT):
        buf_ref[block, kept] = x_ref[pl.ds(block * 8 * PAD_K + kept, 8, stride=PAD_K), :]
    copy = pltpu.make_async_copy(
        buf_ref.at[block],
        o_ref.at[:, pl.ds(block * 8, 8), pl.ds(lane, LANES)],
        sem.at[block],
    )
    copy.start()
    return copy


STORE_SCRATCH = [
    pltpu.VMEM((FIELDS * PAD_K, LANES), jnp.float32),
    pltpu.VMEM((FIELDS // 8, KEPT, 8, LANES), jnp.float32),
    pltpu.SemaphoreType.DMA((FIELDS // 8,)),
]


def store_p_kernel(pos_ref, prior_ref, *refs):
    del prior_ref
    q_refs, o_ref = refs[:8], refs[8]
    x_ref, buf_ref, sem = refs[9:]
    x, c = pos_ref[0], pos_ref[2]
    copies = []
    for zz in range(NZ):
        for dx in range(NX):
            for dc in range(NC):
                field = zz * 8 + ((x + NX - dx) % NX) * NC + (c + dc) % NC
                row = pl.multiple_of(field * PAD_K, 8)
                x_ref[pl.ds(row, KEPT), :] = q_refs[dx * NC + dc][zz * KEPT : (zz + 1) * KEPT, :]
        copies.append(store_block(zz, x_ref, buf_ref, o_ref, sem, 0))
    for copy in copies:
        copy.wait()


def store_p(pos, prior, blocks):
    return pl.pallas_call(
        store_p_kernel,
        in_specs=[SMEM, HBM] + [VMEM] * 8,
        out_specs=HBM,
        out_shape=f32(KEPT, FIELDS, 2 * LANES),
        scratch_shapes=STORE_SCRATCH,
        input_output_aliases={1: 0},
        compiler_params=PARAMS,
        name="store_p",
    )(pos, prior, *blocks)


def store_a_kernel(q_ref, o_ref, x_ref, buf_ref, sem):
    copies = []
    for block in range(FIELDS // 8):
        for f in range(block * 8, block * 8 + 8):
            x_ref[pl.ds(f * PAD_K, KEPT), :] = q_ref[f]
        copies.append(store_block(block, x_ref, buf_ref, o_ref, sem, LANES))
    for copy in copies:
        copy.wait()


def store_a(shares):
    return pl.pallas_call(
        store_a_kernel,
        in_specs=[VMEM],
        out_specs=HBM,
        out_shape=f32(KEPT, FIELDS, 2 * LANES),
        scratch_shapes=STORE_SCRATCH,
        compiler_params=PARAMS,
        name="store_a",
    )(shares)


def shifts(dx, dz, dc):
    def at(x, z, c):
        return (x % NX) * NZ * NC + (z % NZ) * NC + c % NC

    return [
        (at(x, z, c), at(x + dx, z + dz, c + dc)) for x in range(NX) for z in range(NZ) for c in range(NC)
    ]


Z_ORDER = (1, 7, 4, 3, 5, 2, 6)


def exchange_z(blocks):
    out = [None] * NZ
    out[0] = blocks[0]
    for dz in Z_ORDER:
        out[dz] = lax.ppermute(blocks[dz], "lon", shifts(0, dz, 0))
    return out


AX_ORDER = (1, 3, 2)
GROUPS = [[x * GROUP + g for g in range(GROUP)] for x in range(NX)]


def exchange_x(blocks):
    out = [None] * NX
    out[0] = blocks[0]
    for dx in AX_ORDER:
        out[dx] = lax.ppermute(blocks[dx], "lon", shifts(dx, 0, 0))
    return out


X_ORDER = ((1, 0), (3, 0), (2, 0), (2, 1), (1, 1), (3, 1), (0, 1))


def exchange_xc(blocks):
    out = [None] * (NX * NC)
    out[0] = blocks[0]
    for dx, dc in X_ORDER:
        out[dx * NC + dc] = lax.ppermute(blocks[dx * NC + dc], "lon", shifts(dx, 0, dc))
    return out


def local(state):
    device = lax.axis_index("lon")
    pos = jnp.stack([device // (NZ * NC), (device // NC) % NZ, device % NC]).astype(jnp.int32)
    wh, wl = twiddle_matrices(1.0 / math.sqrt(NLON))
    pieces, parts = split(pos, state)
    pieces = exchange_z(pieces)
    parts = exchange_x(parts)
    sent = spread_a(pos, [b.reshape(LON * GROUP, LANES) for b in parts])
    gathered = lax.all_to_all(
        sent, "lon", split_axis=0, concat_axis=0, axis_index_groups=GROUPS, tiled=True
    )
    pieces = spread_x(pos, [b.reshape(LON * 8, LANES) for b in pieces])
    pieces = exchange_xc(pieces)
    pieces = fft_p(pos, pieces, wh, wl)
    pieces = exchange_z(pieces)
    spectrum = fft_a(gathered.reshape(NLON, LANES), wh, wl)
    shares = lax.all_to_all(spectrum, "lon", split_axis=0, concat_axis=0, tiled=True)
    pieces = spread_out(pos, pieces)
    pieces = exchange_xc(pieces)
    out = store_a(shares)
    out = store_p(pos, out, pieces)
    return out.reshape(2, RADIX, FIELDS, 2 * LANES)


def solution(mesh):
    return jax.shard_map(
        local,
        mesh=mesh,
        in_specs=(P("lon", None, "lat"),),
        out_specs=P(None, "lon", None, "lat"),
        check_vma=False,
    )
```

```python
import math

import jax
import jax.numpy as jnp
from jax import lax
from jax.experimental import pallas as pl
from jax.experimental.pallas import tpu as pltpu
from jax.sharding import PartitionSpec as P


NLON = 2048
RADIX = 16
INNER = NLON // RADIX
PEERS = 64
HALF = RADIX // 2
NX, NZ, NC = 4, 8, 2
LON = 32
KEPT = 2 * RADIX
FIELDS = 64
LANES = 128
VMEM = pl.BlockSpec(memory_space=pltpu.VMEM)
HBM = pl.BlockSpec(memory_space=pltpu.HBM)
SMEM = pl.BlockSpec(memory_space=pltpu.SMEM)
PARAMS = pltpu.CompilerParams(vmem_limit_bytes=16 * 1024 * 1024)


def f32(*shape):
    return jax.ShapeDtypeStruct(shape, jnp.float32)


def vmem(*shape):
    return pltpu.VMEM(shape, jnp.float32)


def split_bf16(v):
    high = v.astype(jnp.bfloat16)
    low = (v - high.astype(jnp.float32)).astype(jnp.bfloat16)
    return high, low


def phase(rows, cols):
    turn = (rows * cols) % NLON
    turn = jnp.where(turn >= NLON // 2, turn - NLON, turn)
    return turn.astype(jnp.float32) * (2.0 * math.pi / NLON)


def twiddle_matrices(scale):
    shape = (HALF, 2, PEERS, INNER)
    pair = lax.broadcasted_iota(jnp.int32, shape, 0)
    mirror = lax.broadcasted_iota(jnp.int32, shape, 1)
    outer = lax.broadcasted_iota(jnp.int32, shape, 2)
    inner = lax.broadcasted_iota(jnp.int32, shape, 3)
    first = jnp.where(mirror == 0, pair, jnp.where(pair == 0, HALF, RADIX - pair))
    angle = phase(inner, first + RADIX * outer)
    full = jnp.stack([jnp.cos(angle) * scale, jnp.sin(angle) * scale], axis=2)
    full = full.reshape(HALF, 4 * PEERS, INNER)
    high = lax.reduce_precision(full, 8, 7)
    return high.astype(jnp.bfloat16), (full - high).astype(jnp.bfloat16)


def fft_real16(x):
    def fft_complex8(z):
        def fft4(a):
            (ar, ai), (br, bi), (cr, ci), (dr, di) = a
            sr, si = ar + cr, ai + ci
            tr, ti = ar - cr, ai - ci
            ur, ui = br + dr, bi + di
            vr, vi = br - dr, bi - di
            return [(sr + ur, si + ui), (tr + vi, ti - vr), (sr - ur, si - ui), (tr - vi, ti + vr)]

        even = fft4(z[0::2])
        odd = fft4(z[1::2])
        h = math.sqrt(0.5)
        out = [None] * 8
        for k in range(4):
            er, ei = even[k]
            pr, pi = odd[k]
            if k == 1:
                pr, pi = (pr + pi) * h, (pi - pr) * h
            elif k == 2:
                pr, pi = pi, -pr
            elif k == 3:
                pr, pi = (pi - pr) * h, -(pr + pi) * h
            out[k] = (er + pr, ei + pi)
            out[k + 4] = (er - pr, ei - pi)
        return out

    z = fft_complex8([(x[2 * i], x[2 * i + 1]) for i in range(8)])
    out = [(z[0][0] + z[0][1], None)]
    for k in range(1, 8):
        zr, zi = z[k]
        wr, wi = z[8 - k]
        er, ei = (zr + wr) * 0.5, (zi - wi) * 0.5
        pr, pi = (zi + wi) * 0.5, (wr - zr) * 0.5
        c, s = math.cos(2 * math.pi * k / 16), math.sin(2 * math.pi * k / 16)
        out.append((er + c * pr + s * pi, ei + c * pi - s * pr))
    out.append((z[0][0] - z[0][1], None))
    return out


PAD_R = PEERS + 8


def natural_row(n2, base):
    return n2 * INNER + base


def grouped_row(n2, base):
    return ((n2 % 4) * 4 + base // LON) * INNER + (n2 // 4) * LON + base % LON


def fft_core(x_ref, wh_ref, wl_ref, y_ref, r_ref, row_of):
    def butterfly(i, carry):
        base = pl.multiple_of(i * 8, 8)
        x = [x_ref[pl.ds(pl.multiple_of(row_of(n2, base), 8), 8), :] for n2 in range(RADIX)]
        y = fft_real16(x)
        for k in range(HALF):
            parts = (y[0][0], y[HALF][0]) if k == 0 else y[k]
            for j, part in enumerate(parts):
                y_ref[k, pl.ds(j * INNER + base, 8), :] = part
        return carry

    lax.fori_loop(0, INNER // 8, butterfly, 0, unroll=4)
    for k in range(HALF):
        yh, yl = split_bf16(y_ref[k])
        sides = jnp.concatenate([yh[:INNER], yh[INNER:], yl[:INNER], yl[INNER:]], axis=1)
        r = jnp.dot(wh_ref[k], sides, preferred_element_type=jnp.float32)
        r = r[:, : 2 * LANES] + r[:, 2 * LANES :]
        r = r + jnp.dot(wl_ref[k], sides[:, : 2 * LANES], preferred_element_type=jnp.float32)
        (c1, s1, c2, s2), (d1, t1, d2, t2) = (
            [r[q * PEERS : (q + 1) * PEERS, p * LANES : (p + 1) * LANES] for q in range(4)] for p in range(2)
        )
        if k == 0:
            parts = (c1, -s1, d2, -t2)
        else:
            parts = (c1 + t1, d1 - s1, c2 - t2, -d2 - s2)
        mirror = HALF if k == 0 else RADIX - k
        for row, part in zip((k, RADIX + k, mirror, RADIX + mirror), parts):
            r_ref[pl.ds(row * PAD_R, PEERS), :] = part


PIECES = 4


def send_pieces(body, count, buf_ref, o_ref, sem):
    step = count // PIECES
    copies = []
    for piece in range(PIECES):
        lax.fori_loop(piece * step, (piece + 1) * step, body, 0, unroll=4)
        rows = pl.ds(piece * step, step)
        copy = pltpu.make_async_copy(buf_ref.at[rows], o_ref.at[rows], sem.at[piece])
        copy.start()
        copies.append(copy)
    for copy in copies:
        copy.wait()


FFT_SCRATCH = [
    pltpu.VMEM((HALF, 2 * INNER, LANES), jnp.float32),
    pltpu.VMEM((KEPT * PAD_R, LANES), jnp.float32),
]


def mode_rows(r_ref, k1, eight):
    return r_ref[pl.ds(eight * 8 * PAD_R + k1, 8, stride=PAD_R), :]


def fft_a_kernel(x_ref, wh_ref, wl_ref, o_ref, y_ref, r_ref, buf_ref, sem):
    fft_core(x_ref, wh_ref, wl_ref, y_ref, r_ref, grouped_row)

    def peer(k1, carry):
        for eight in range(KEPT // 8):
            buf_ref[k1, eight * 8 : eight * 8 + 8, :] = mode_rows(r_ref, k1, eight)
        return carry

    send_pieces(peer, PEERS, buf_ref, o_ref, sem)


def fft_a(gathered, wh, wl):
    return pl.pallas_call(
        fft_a_kernel,
        in_specs=[VMEM] * 3,
        out_specs=HBM,
        out_shape=pltpu.HBM((PEERS, KEPT, LANES), jnp.float32),
        scratch_shapes=FFT_SCRATCH
        + [pltpu.VMEM((PEERS, KEPT, LANES), jnp.float32), pltpu.SemaphoreType.DMA((PIECES,))],
        compiler_params=PARAMS,
        name="fft_a",
    )(gathered, wh, wl)


def fft_p_kernel(pos_ref, *refs):
    g_refs, (wh_ref, wl_ref), o_refs = refs[:8], refs[8:10], refs[10:18]
    x_ref, y_ref, r_ref = refs[18:]
    x, z, c = pos_ref[0], pos_ref[1], pos_ref[2]
    for dx in range(NX):
        for dc in range(NC):
            start = ((x + NX - dx) % NX) * (NLON // NX) + ((c + dc) % NC) * LON
            for zz in range(NZ):
                row = pl.multiple_of(start + zz * NC * LON, LON)
                x_ref[pl.ds(row, LON), :] = g_refs[dx * NC + dc][zz * LON : (zz + 1) * LON, :]
    fft_core(x_ref, wh_ref, wl_ref, y_ref, r_ref, natural_row)
    for dz in range(NZ):
        target = (z + dz) % NZ
        for xx in range(NX):
            for cc in range(NC):
                k1 = xx * NZ * NC + target * NC + cc
                for eight in range(KEPT // 8):
                    row = (xx * NC + cc) * KEPT + eight * 8
                    o_refs[dz][row : row + 8, :] = mode_rows(r_ref, k1, eight)


def fft_p(pos, blocks, wh, wl):
    return pl.pallas_call(
        fft_p_kernel,
        in_specs=[SMEM] + [VMEM] * 10,
        out_specs=[VMEM] * NZ,
        out_shape=[vmem(NX * NC * KEPT, LANES)] * NZ,
        scratch_shapes=[pltpu.VMEM((NLON, LANES), jnp.float32)] + FFT_SCRATCH,
        compiler_params=PARAMS,
        name="fft_p",
    )(pos, *blocks, wh, wl)


GROUP = NZ * NC


def split_kernel(pos_ref, s_ref, *refs):
    o_refs, sem = refs[: NZ + NX], refs[NZ + NX]
    x, z = pos_ref[0], pos_ref[1]
    copies = []
    for dz in range(NZ):
        field = pl.multiple_of(((z + dz) % NZ) * 8, 8)
        source = s_ref.at[:, pl.ds(field, 8), pl.ds(0, LANES)]
        copies.append(pltpu.make_async_copy(source, o_refs[dz], sem.at[dz]))
    for dx in range(NX):
        field = pl.multiple_of(((x + dx) % NX) * GROUP, GROUP)
        source = s_ref.at[:, pl.ds(field, GROUP), pl.ds(LANES, LANES)]
        copies.append(pltpu.make_async_copy(source, o_refs[NZ + dx], sem.at[NZ + dx]))
    for copy in copies:
        copy.start()
    for copy in copies:
        copy.wait()


def split(pos, state):
    out = pl.pallas_call(
        split_kernel,
        in_specs=[SMEM, HBM],
        out_specs=[VMEM] * (NZ + NX),
        out_shape=[vmem(LON, 8, LANES)] * NZ + [vmem(LON, GROUP, LANES)] * NX,
        scratch_shapes=[pltpu.SemaphoreType.DMA((NZ + NX,))],
        compiler_params=PARAMS,
        name="split",
    )(pos, pltpu.with_memory_space_constraint(state, pltpu.HBM))
    return out[:NZ], out[NZ:]


def spread_x_kernel(pos_ref, *refs):
    b_refs, o_refs = refs[:NZ], refs[NZ:]
    x, z, c = pos_ref[0], pos_ref[1], pos_ref[2]
    for dx in range(NX):
        for dc in range(NC):
            field = ((x + dx) % NX) * NC + (c + dc) % NC
            for dz in range(NZ):
                row = pl.multiple_of(((z + NZ - dz) % NZ) * LON, LON)
                o_refs[dx * NC + dc][pl.ds(row, LON), :] = b_refs[dz][pl.ds(field, LON, stride=8), :]


def spread_x(pos, blocks):
    return pl.pallas_call(
        spread_x_kernel,
        in_specs=[SMEM] + [VMEM] * NZ,
        out_specs=[VMEM] * (NX * NC),
        out_shape=[vmem(NZ * LON, LANES)] * (NX * NC),
        compiler_params=PARAMS,
        name="spread_x",
    )(pos, *blocks)


def spread_out_kernel(pos_ref, *refs):
    h_refs, o_refs = refs[:NZ], refs[NZ:]
    x, z, c = pos_ref[0], pos_ref[1], pos_ref[2]
    for dx in range(NX):
        for dc in range(NC):
            source = pl.multiple_of((((x + dx) % NX) * NC + (c + dc) % NC) * KEPT, KEPT)
            for dz in range(NZ):
                row = pl.multiple_of(((z + NZ - dz) % NZ) * KEPT, KEPT)
                o_refs[dx * NC + dc][pl.ds(row, KEPT), :] = h_refs[dz][pl.ds(source, KEPT), :]


def spread_out(pos, blocks):
    return pl.pallas_call(
        spread_out_kernel,
        in_specs=[SMEM] + [VMEM] * NZ,
        out_specs=[VMEM] * (NX * NC),
        out_shape=[vmem(NZ * KEPT, LANES)] * (NX * NC),
        compiler_params=PARAMS,
        name="spread_out",
    )(pos, *blocks)


def spread_a_kernel(pos_ref, *refs):
    b_refs, o_ref, buf_ref, sem = refs[:NX], refs[NX], refs[NX + 1], refs[NX + 2]
    x = pos_ref[0]

    def field(f, carry):
        for dx in range(NX):
            row = pl.multiple_of(((x + NX - dx) % NX) * LON, LON)
            buf_ref[f, pl.ds(row, LON), :] = b_refs[dx][pl.ds(f, LON, stride=GROUP), :]
        return carry

    send_pieces(field, GROUP, buf_ref, o_ref, sem)


def spread_a(pos, blocks):
    return pl.pallas_call(
        spread_a_kernel,
        in_specs=[SMEM] + [VMEM] * NX,
        out_specs=HBM,
        out_shape=pltpu.HBM((GROUP, NX * LON, LANES), jnp.float32),
        scratch_shapes=[
            pltpu.VMEM((GROUP, NX * LON, LANES), jnp.float32),
            pltpu.SemaphoreType.DMA((PIECES,)),
        ],
        compiler_params=PARAMS,
        name="spread_a",
    )(pos, *blocks)


PAD_K = KEPT + 8


def store_block(block, x_ref, buf_ref, o_ref, sem, lane):
    for kept in range(KEPT):
        buf_ref[block, kept] = x_ref[pl.ds(block * 8 * PAD_K + kept, 8, stride=PAD_K), :]
    copy = pltpu.make_async_copy(
        buf_ref.at[block],
        o_ref.at[:, pl.ds(block * 8, 8), pl.ds(lane, LANES)],
        sem.at[block],
    )
    copy.start()
    return copy


STORE_SCRATCH = [
    pltpu.VMEM((FIELDS * PAD_K, LANES), jnp.float32),
    pltpu.VMEM((FIELDS // 8, KEPT, 8, LANES), jnp.float32),
    pltpu.SemaphoreType.DMA((FIELDS // 8,)),
]


def store_p_kernel(pos_ref, prior_ref, *refs):
    del prior_ref
    q_refs, o_ref = refs[:8], refs[8]
    x_ref, buf_ref, sem = refs[9:]
    x, c = pos_ref[0], pos_ref[2]
    copies = []
    for zz in range(NZ):
        for dx in range(NX):
            for dc in range(NC):
                field = zz * 8 + ((x + NX - dx) % NX) * NC + (c + dc) % NC
                row = pl.multiple_of(field * PAD_K, 8)
                x_ref[pl.ds(row, KEPT), :] = q_refs[dx * NC + dc][zz * KEPT : (zz + 1) * KEPT, :]
        copies.append(store_block(zz, x_ref, buf_ref, o_ref, sem, 0))
    for copy in copies:
        copy.wait()


def store_p(pos, prior, blocks):
    return pl.pallas_call(
        store_p_kernel,
        in_specs=[SMEM, HBM] + [VMEM] * 8,
        out_specs=HBM,
        out_shape=f32(KEPT, FIELDS, 2 * LANES),
        scratch_shapes=STORE_SCRATCH,
        input_output_aliases={1: 0},
        compiler_params=PARAMS,
        name="store_p",
    )(pos, prior, *blocks)


def store_a_kernel(q_ref, o_ref, x_ref, buf_ref, sem):
    copies = []
    for block in range(FIELDS // 8):
        for f in range(block * 8, block * 8 + 8):
            x_ref[pl.ds(f * PAD_K, KEPT), :] = q_ref[f]
        copies.append(store_block(block, x_ref, buf_ref, o_ref, sem, LANES))
    for copy in copies:
        copy.wait()


def store_a(shares):
    return pl.pallas_call(
        store_a_kernel,
        in_specs=[VMEM],
        out_specs=HBM,
        out_shape=f32(KEPT, FIELDS, 2 * LANES),
        scratch_shapes=STORE_SCRATCH,
        compiler_params=PARAMS,
        name="store_a",
    )(shares)


def shifts(dx, dz, dc):
    def at(x, z, c):
        return (x % NX) * NZ * NC + (z % NZ) * NC + c % NC

    return [
        (at(x, z, c), at(x + dx, z + dz, c + dc)) for x in range(NX) for z in range(NZ) for c in range(NC)
    ]


Z_ORDER = (1, 7, 4, 3, 5, 2, 6)


def exchange_z(blocks):
    out = [None] * NZ
    out[0] = blocks[0]
    for dz in Z_ORDER:
        out[dz] = lax.ppermute(blocks[dz], "lon", shifts(0, dz, 0))
    return out


AX_ORDER = (1, 3, 2)
GROUPS = [[x * GROUP + g for g in range(GROUP)] for x in range(NX)]


def exchange_x(blocks):
    out = [None] * NX
    out[0] = blocks[0]
    for dx in AX_ORDER:
        out[dx] = lax.ppermute(blocks[dx], "lon", shifts(dx, 0, 0))
    return out


X_ORDER = ((1, 0), (3, 0), (2, 0), (2, 1), (1, 1), (3, 1), (0, 1))


def exchange_xc(blocks):
    out = [None] * (NX * NC)
    out[0] = blocks[0]
    for dx, dc in X_ORDER:
        out[dx * NC + dc] = lax.ppermute(blocks[dx * NC + dc], "lon", shifts(dx, 0, dc))
    return out


def local(state):
    device = lax.axis_index("lon")
    pos = jnp.stack([device // (NZ * NC), (device // NC) % NZ, device % NC]).astype(jnp.int32)
    wh, wl = twiddle_matrices(1.0 / math.sqrt(NLON))
    pieces, parts = split(pos, state)
    pieces = exchange_z(pieces)
    parts = exchange_x(parts)
    sent = spread_a(pos, [b.reshape(LON * GROUP, LANES) for b in parts])
    gathered = lax.all_to_all(
        sent, "lon", split_axis=0, concat_axis=0, axis_index_groups=GROUPS, tiled=True
    )
    pieces = spread_x(pos, [b.reshape(LON * 8, LANES) for b in pieces])
    pieces = exchange_xc(pieces)
    pieces = fft_p(pos, pieces, wh, wl)
    pieces = exchange_z(pieces)
    spectrum = fft_a(gathered.reshape(NLON, LANES), wh, wl)
    shares = lax.all_to_all(spectrum, "lon", split_axis=0, concat_axis=0, tiled=True)
    pieces = spread_out(pos, pieces)
    pieces = exchange_xc(pieces)
    out = store_a(shares)
    out = store_p(pos, out, pieces)
    return out.reshape(2, RADIX, FIELDS, 2 * LANES)


def solution(mesh):
    return jax.shard_map(
        local,
        mesh=mesh,
        in_specs=(P("lon", None, "lat"),),
        out_specs=P(None, "lon", None, "lat"),
        check_vma=False,
    )
```

```python
import math

import jax
import jax.numpy as jnp
from jax import lax
from jax.experimental import pallas as pl
from jax.experimental.pallas import tpu as pltpu
from jax.sharding import PartitionSpec as P


NLON = 2048
RADIX = 16
INNER = NLON // RADIX
PEERS = 64
HALF = RADIX // 2
NX, NZ, NC = 4, 8, 2
LON = 32
KEPT = 2 * RADIX
FIELDS = 64
LANES = 128
VMEM = pl.BlockSpec(memory_space=pltpu.VMEM)
HBM = pl.BlockSpec(memory_space=pltpu.HBM)
SMEM = pl.BlockSpec(memory_space=pltpu.SMEM)
PARAMS = pltpu.CompilerParams(vmem_limit_bytes=16 * 1024 * 1024)


def f32(*shape):
    return jax.ShapeDtypeStruct(shape, jnp.float32)


def vmem(*shape):
    return pltpu.VMEM(shape, jnp.float32)


def split_bf16(v):
    high = v.astype(jnp.bfloat16)
    low = (v - high.astype(jnp.float32)).astype(jnp.bfloat16)
    return high, low


def phase(rows, cols):
    turn = (rows * cols) % NLON
    turn = jnp.where(turn >= NLON // 2, turn - NLON, turn)
    return turn.astype(jnp.float32) * (2.0 * math.pi / NLON)


def twiddle_matrices(scale):
    shape = (HALF, 2, PEERS, INNER)
    pair = lax.broadcasted_iota(jnp.int32, shape, 0)
    mirror = lax.broadcasted_iota(jnp.int32, shape, 1)
    outer = lax.broadcasted_iota(jnp.int32, shape, 2)
    inner = lax.broadcasted_iota(jnp.int32, shape, 3)
    first = jnp.where(mirror == 0, pair, jnp.where(pair == 0, HALF, RADIX - pair))
    angle = phase(inner, first + RADIX * outer)
    c = jnp.cos(angle) * scale
    s = jnp.sin(angle) * scale
    real_only = pair == 0
    zero = jnp.zeros_like(c)
    plain = mirror == 0
    re_a = jnp.where(real_only, jnp.where(plain, c, zero), c)
    im_a = jnp.where(real_only, jnp.where(plain, -s, zero), -s)
    re_b = jnp.where(real_only, jnp.where(plain, zero, c), jnp.where(plain, s, -s))
    im_b = jnp.where(real_only, jnp.where(plain, zero, -s), jnp.where(plain, c, -c))
    re = jnp.concatenate([re_a, re_b], axis=-1)
    im = jnp.concatenate([im_a, im_b], axis=-1)
    full = jnp.stack([re, im], axis=2)
    full = full.reshape(HALF, 4 * PEERS, 2 * INNER)
    high = lax.reduce_precision(full, 8, 7)
    high, low = high.astype(jnp.bfloat16), (full - high).astype(jnp.bfloat16)
    return high, low


def fft_real16(x):
    def fft_complex8(z):
        def fft4(a):
            (ar, ai), (br, bi), (cr, ci), (dr, di) = a
            sr, si = ar + cr, ai + ci
            tr, ti = ar - cr, ai - ci
            ur, ui = br + dr, bi + di
            vr, vi = br - dr, bi - di
            return [(sr + ur, si + ui), (tr + vi, ti - vr), (sr - ur, si - ui), (tr - vi, ti + vr)]

        even = fft4(z[0::2])
        odd = fft4(z[1::2])
        h = math.sqrt(0.5)
        out = [None] * 8
        for k in range(4):
            er, ei = even[k]
            pr, pi = odd[k]
            if k == 1:
                pr, pi = (pr + pi) * h, (pi - pr) * h
            elif k == 2:
                pr, pi = pi, -pr
            elif k == 3:
                pr, pi = (pi - pr) * h, -(pr + pi) * h
            out[k] = (er + pr, ei + pi)
            out[k + 4] = (er - pr, ei - pi)
        return out

    z = fft_complex8([(x[2 * i], x[2 * i + 1]) for i in range(8)])
    out = [(z[0][0] + z[0][1], None)]
    for k in range(1, 8):
        zr, zi = z[k]
        wr, wi = z[8 - k]
        er, ei = (zr + wr) * 0.5, (zi - wi) * 0.5
        pr, pi = (zi + wi) * 0.5, (wr - zr) * 0.5
        c, s = math.cos(2 * math.pi * k / 16), math.sin(2 * math.pi * k / 16)
        out.append((er + c * pr + s * pi, ei + c * pi - s * pr))
    out.append((z[0][0] - z[0][1], None))
    return out


PAD_R = PEERS + 8


def natural_row(n2, base):
    return n2 * INNER + base


def grouped_row(n2, base):
    return ((n2 % 4) * 4 + base // LON) * INNER + (n2 // 4) * LON + base % LON


def fft_core(x_ref, wh_ref, wl_ref, y_ref, r_ref, row_of):
    def butterfly(i, carry):
        base = pl.multiple_of(i * 8, 8)
        x = [x_ref[pl.ds(pl.multiple_of(row_of(n2, base), 8), 8), :] for n2 in range(RADIX)]
        y = fft_real16(x)
        for k in range(HALF):
            parts = (y[0][0], y[HALF][0]) if k == 0 else y[k]
            for j, part in enumerate(parts):
                y_ref[k, pl.ds(j * INNER + base, 8), :] = part
        return carry

    lax.fori_loop(0, INNER // 8, butterfly, 0, unroll=4)
    for k in range(HALF):
        yh, yl = split_bf16(y_ref[k])
        two = jnp.dot(wh_ref[k], jnp.concatenate([yh, yl], axis=1), preferred_element_type=jnp.float32)
        r = two[:, :LANES] + two[:, LANES:]
        r = r + jnp.dot(wl_ref[k], yh, preferred_element_type=jnp.float32)
        mirror = HALF if k == 0 else RADIX - k
        for q, row in enumerate((k, RADIX + k, mirror, RADIX + mirror)):
            r_ref[pl.ds(row * PAD_R, PEERS), :] = r[q * PEERS : (q + 1) * PEERS]


PIECES = 4


def send_pieces(body, count, buf_ref, o_ref, sem):
    step = count // PIECES
    copies = []
    for piece in range(PIECES):
        lax.fori_loop(piece * step, (piece + 1) * step, body, 0, unroll=4)
        rows = pl.ds(piece * step, step)
        copy = pltpu.make_async_copy(buf_ref.at[rows], o_ref.at[rows], sem.at[piece])
        copy.start()
        copies.append(copy)
    for copy in copies:
        copy.wait()


FFT_SCRATCH = [
    pltpu.VMEM((HALF, 2 * INNER, LANES), jnp.float32),
    pltpu.VMEM((KEPT * PAD_R, LANES), jnp.float32),
]


def mode_rows(r_ref, k1, eight):
    return r_ref[pl.ds(eight * 8 * PAD_R + k1, 8, stride=PAD_R), :]


def fft_a_kernel(x_ref, wh_ref, wl_ref, o_ref, y_ref, r_ref, buf_ref, sem):
    fft_core(x_ref, wh_ref, wl_ref, y_ref, r_ref, grouped_row)

    def peer(k1, carry):
        for eight in range(KEPT // 8):
            buf_ref[k1, eight * 8 : eight * 8 + 8, :] = mode_rows(r_ref, k1, eight)
        return carry

    send_pieces(peer, PEERS, buf_ref, o_ref, sem)


def fft_a(gathered, wh, wl):
    return pl.pallas_call(
        fft_a_kernel,
        in_specs=[VMEM] * 3,
        out_specs=HBM,
        out_shape=pltpu.HBM((PEERS, KEPT, LANES), jnp.float32),
        scratch_shapes=FFT_SCRATCH
        + [pltpu.VMEM((PEERS, KEPT, LANES), jnp.float32), pltpu.SemaphoreType.DMA((PIECES,))],
        compiler_params=PARAMS,
        name="fft_a",
    )(gathered, wh, wl)


def fft_p_kernel(pos_ref, *refs):
    g_refs, (wh_ref, wl_ref), o_refs = refs[:8], refs[8:10], refs[10:18]
    x_ref, y_ref, r_ref = refs[18:]
    x, z, c = pos_ref[0], pos_ref[1], pos_ref[2]
    for dx in range(NX):
        for dc in range(NC):
            start = ((x + NX - dx) % NX) * (NLON // NX) + ((c + dc) % NC) * LON
            for zz in range(NZ):
                row = pl.multiple_of(start + zz * NC * LON, LON)
                x_ref[pl.ds(row, LON), :] = g_refs[dx * NC + dc][zz * LON : (zz + 1) * LON, :]
    fft_core(x_ref, wh_ref, wl_ref, y_ref, r_ref, natural_row)
    for dz in range(NZ):
        target = (z + dz) % NZ
        for xx in range(NX):
            for cc in range(NC):
                k1 = xx * NZ * NC + target * NC + cc
                for eight in range(KEPT // 8):
                    row = (xx * NC + cc) * KEPT + eight * 8
                    o_refs[dz][row : row + 8, :] = mode_rows(r_ref, k1, eight)


def fft_p(pos, blocks, wh, wl):
    return pl.pallas_call(
        fft_p_kernel,
        in_specs=[SMEM] + [VMEM] * 10,
        out_specs=[VMEM] * NZ,
        out_shape=[vmem(NX * NC * KEPT, LANES)] * NZ,
        scratch_shapes=[pltpu.VMEM((NLON, LANES), jnp.float32)] + FFT_SCRATCH,
        compiler_params=PARAMS,
        name="fft_p",
    )(pos, *blocks, wh, wl)


GROUP = NZ * NC


def split_kernel(pos_ref, s_ref, *refs):
    o_refs, sem = refs[: NZ + NX], refs[NZ + NX]
    x, z = pos_ref[0], pos_ref[1]
    copies = []
    for dz in range(NZ):
        field = pl.multiple_of(((z + dz) % NZ) * 8, 8)
        source = s_ref.at[:, pl.ds(field, 8), pl.ds(0, LANES)]
        copies.append(pltpu.make_async_copy(source, o_refs[dz], sem.at[dz]))
    for dx in range(NX):
        field = pl.multiple_of(((x + dx) % NX) * GROUP, GROUP)
        source = s_ref.at[:, pl.ds(field, GROUP), pl.ds(LANES, LANES)]
        copies.append(pltpu.make_async_copy(source, o_refs[NZ + dx], sem.at[NZ + dx]))
    for copy in copies:
        copy.start()
    for copy in copies:
        copy.wait()


def split(pos, state):
    out = pl.pallas_call(
        split_kernel,
        in_specs=[SMEM, HBM],
        out_specs=[VMEM] * (NZ + NX),
        out_shape=[vmem(LON, 8, LANES)] * NZ + [vmem(LON, GROUP, LANES)] * NX,
        scratch_shapes=[pltpu.SemaphoreType.DMA((NZ + NX,))],
        compiler_params=PARAMS,
        name="split",
    )(pos, pltpu.with_memory_space_constraint(state, pltpu.HBM))
    return out[:NZ], out[NZ:]


def spread_x_kernel(pos_ref, *refs):
    b_refs, o_refs = refs[:NZ], refs[NZ:]
    x, z, c = pos_ref[0], pos_ref[1], pos_ref[2]
    for dx in range(NX):
        for dc in range(NC):
            field = ((x + dx) % NX) * NC + (c + dc) % NC
            for dz in range(NZ):
                row = pl.multiple_of(((z + NZ - dz) % NZ) * LON, LON)
                o_refs[dx * NC + dc][pl.ds(row, LON), :] = b_refs[dz][pl.ds(field, LON, stride=8), :]


def spread_x(pos, blocks):
    return pl.pallas_call(
        spread_x_kernel,
        in_specs=[SMEM] + [VMEM] * NZ,
        out_specs=[VMEM] * (NX * NC),
        out_shape=[vmem(NZ * LON, LANES)] * (NX * NC),
        compiler_params=PARAMS,
        name="spread_x",
    )(pos, *blocks)


def spread_out_kernel(pos_ref, *refs):
    h_refs, o_refs = refs[:NZ], refs[NZ:]
    x, z, c = pos_ref[0], pos_ref[1], pos_ref[2]
    for dx in range(NX):
        for dc in range(NC):
            source = pl.multiple_of((((x + dx) % NX) * NC + (c + dc) % NC) * KEPT, KEPT)
            for dz in range(NZ):
                row = pl.multiple_of(((z + NZ - dz) % NZ) * KEPT, KEPT)
                o_refs[dx * NC + dc][pl.ds(row, KEPT), :] = h_refs[dz][pl.ds(source, KEPT), :]


def spread_out(pos, blocks):
    return pl.pallas_call(
        spread_out_kernel,
        in_specs=[SMEM] + [VMEM] * NZ,
        out_specs=[VMEM] * (NX * NC),
        out_shape=[vmem(NZ * KEPT, LANES)] * (NX * NC),
        compiler_params=PARAMS,
        name="spread_out",
    )(pos, *blocks)


def spread_a_kernel(pos_ref, *refs):
    b_refs, o_ref, buf_ref, sem = refs[:NX], refs[NX], refs[NX + 1], refs[NX + 2]
    x = pos_ref[0]

    def field(f, carry):
        for dx in range(NX):
            row = pl.multiple_of(((x + NX - dx) % NX) * LON, LON)
            buf_ref[f, pl.ds(row, LON), :] = b_refs[dx][pl.ds(f, LON, stride=GROUP), :]
        return carry

    send_pieces(field, GROUP, buf_ref, o_ref, sem)


def spread_a(pos, blocks):
    return pl.pallas_call(
        spread_a_kernel,
        in_specs=[SMEM] + [VMEM] * NX,
        out_specs=HBM,
        out_shape=pltpu.HBM((GROUP, NX * LON, LANES), jnp.float32),
        scratch_shapes=[
            pltpu.VMEM((GROUP, NX * LON, LANES), jnp.float32),
            pltpu.SemaphoreType.DMA((PIECES,)),
        ],
        compiler_params=PARAMS,
        name="spread_a",
    )(pos, *blocks)


PAD_K = KEPT + 8


def store_block(block, x_ref, buf_ref, o_ref, sem, lane):
    for kept in range(KEPT):
        buf_ref[block, kept] = x_ref[pl.ds(block * 8 * PAD_K + kept, 8, stride=PAD_K), :]
    copy = pltpu.make_async_copy(
        buf_ref.at[block],
        o_ref.at[:, pl.ds(block * 8, 8), pl.ds(lane, LANES)],
        sem.at[block],
    )
    copy.start()
    return copy


STORE_SCRATCH = [
    pltpu.VMEM((FIELDS * PAD_K, LANES), jnp.float32),
    pltpu.VMEM((FIELDS // 8, KEPT, 8, LANES), jnp.float32),
    pltpu.SemaphoreType.DMA((FIELDS // 8,)),
]


def store_p_kernel(pos_ref, prior_ref, *refs):
    del prior_ref
    q_refs, o_ref = refs[:8], refs[8]
    x_ref, buf_ref, sem = refs[9:]
    x, c = pos_ref[0], pos_ref[2]
    copies = []
    for zz in range(NZ):
        for dx in range(NX):
            for dc in range(NC):
                field = zz * 8 + ((x + NX - dx) % NX) * NC + (c + dc) % NC
                row = pl.multiple_of(field * PAD_K, 8)
                x_ref[pl.ds(row, KEPT), :] = q_refs[dx * NC + dc][zz * KEPT : (zz + 1) * KEPT, :]
        copies.append(store_block(zz, x_ref, buf_ref, o_ref, sem, 0))
    for copy in copies:
        copy.wait()


def store_p(pos, prior, blocks):
    return pl.pallas_call(
        store_p_kernel,
        in_specs=[SMEM, HBM] + [VMEM] * 8,
        out_specs=HBM,
        out_shape=f32(KEPT, FIELDS, 2 * LANES),
        scratch_shapes=STORE_SCRATCH,
        input_output_aliases={1: 0},
        compiler_params=PARAMS,
        name="store_p",
    )(pos, prior, *blocks)


def store_a_kernel(q_ref, o_ref, x_ref, buf_ref, sem):
    copies = []
    for block in range(FIELDS // 8):
        for f in range(block * 8, block * 8 + 8):
            x_ref[pl.ds(f * PAD_K, KEPT), :] = q_ref[f]
        copies.append(store_block(block, x_ref, buf_ref, o_ref, sem, LANES))
    for copy in copies:
        copy.wait()


def store_a(shares):
    return pl.pallas_call(
        store_a_kernel,
        in_specs=[VMEM],
        out_specs=HBM,
        out_shape=f32(KEPT, FIELDS, 2 * LANES),
        scratch_shapes=STORE_SCRATCH,
        compiler_params=PARAMS,
        name="store_a",
    )(shares)


def shifts(dx, dz, dc):
    def at(x, z, c):
        return (x % NX) * NZ * NC + (z % NZ) * NC + c % NC

    return [
        (at(x, z, c), at(x + dx, z + dz, c + dc)) for x in range(NX) for z in range(NZ) for c in range(NC)
    ]


Z_ORDER = (1, 7, 4, 3, 5, 2, 6)


def exchange_z(blocks):
    out = [None] * NZ
    out[0] = blocks[0]
    for dz in Z_ORDER:
        out[dz] = lax.ppermute(blocks[dz], "lon", shifts(0, dz, 0))
    return out


AX_ORDER = (1, 3, 2)
GROUPS = [[x * GROUP + g for g in range(GROUP)] for x in range(NX)]


def exchange_x(blocks):
    out = [None] * NX
    out[0] = blocks[0]
    for dx in AX_ORDER:
        out[dx] = lax.ppermute(blocks[dx], "lon", shifts(dx, 0, 0))
    return out


X_ORDER = ((1, 0), (3, 0), (2, 0), (2, 1), (1, 1), (3, 1), (0, 1))
X_OUT = ((2, 0), (2, 1), (1, 0), (3, 0), (1, 1), (3, 1), (0, 1))


def exchange_xc(blocks, order):
    out = [None] * (NX * NC)
    out[0] = blocks[0]
    for dx, dc in order:
        out[dx * NC + dc] = lax.ppermute(blocks[dx * NC + dc], "lon", shifts(dx, 0, dc))
    return out


def local(state):
    device = lax.axis_index("lon")
    pos = jnp.stack([device // (NZ * NC), (device // NC) % NZ, device % NC]).astype(jnp.int32)
    wh, wl = twiddle_matrices(1.0 / math.sqrt(NLON))
    pieces, parts = split(pos, state)
    pieces = exchange_z(pieces)
    parts = exchange_x(parts)
    sent = spread_a(pos, [b.reshape(LON * GROUP, LANES) for b in parts])
    gathered = lax.all_to_all(
        sent, "lon", split_axis=0, concat_axis=0, axis_index_groups=GROUPS, tiled=True
    )
    pieces = spread_x(pos, [b.reshape(LON * 8, LANES) for b in pieces])
    pieces = exchange_xc(pieces, X_ORDER)
    pieces = fft_p(pos, pieces, wh, wl)
    pieces = exchange_z(pieces)
    spectrum = fft_a(gathered.reshape(NLON, LANES), wh, wl)
    shares = lax.all_to_all(spectrum, "lon", split_axis=0, concat_axis=0, tiled=True)
    pieces = spread_out(pos, pieces)
    pieces = exchange_xc(pieces, X_OUT)
    out = store_a(shares)
    out = store_p(pos, out, pieces)
    return out.reshape(2, RADIX, FIELDS, 2 * LANES)


def solution(mesh):
    return jax.shard_map(
        local,
        mesh=mesh,
        in_specs=(P("lon", None, "lat"),),
        out_specs=P(None, "lon", None, "lat"),
        check_vma=False,
    )
```
